32 devices in a mesh: seg: 32 (over z, y, x, core).
Axes of the slice: x: 2, y: 2, z: 4, core: 2. Of those that a mesh axis runs over, the one named last changes fastest.
Arguments:
- cam_jac: bfloat16 [18, 512, 512], P(None, 'seg'), may hold values from -0.25 to 0.25
- point_jac: bfloat16 [6, 512, 512], P(None, 'seg'), may hold values from -6 to 6
- obs_point: int32 [512, 512], P('seg'), may hold values from 0 to 1791, as said below
- obs_count: int32 [512], P('seg'), may hold values from 64 to 512, as said below
- back_list: int32 [32, 384], P('seg'), may hold values from 0 to 1023, as said below
- front_list: int32 [32, 384], P('seg'), may hold values from 0 to 1023, as said below
- point_damp: float32 [32768], P('seg'), may hold values from 0.5 to 4
- cam_damp: float32 [512], P('seg'), may hold values from 0.1 to 1
- right_side: float32 [9, 512], P(None, 'seg'), may hold values from -25 to 25
- start_guess: float32 [9, 512], P(None, 'seg'), may hold values from -3 to 3
Outputs:
- camera_step: float32 [9, 512], P(None, 'seg')
- residual: float32 [9, 512], P(None, 'seg')
The draws below stay inside these ranges and needn't reach their ends.
Inputs may be any that keep to these rules, and one draw needn't show every extreme that they name: `obs_point`: entries below 1024 name the segment's own points; an entry e from 1024 to 1407 names entry e - 1024 of the previous segment's back_list, and a larger one entry e - 1408 of the next segment's front_list. Keyframes of the first segment name no back slot, those of the last segment no front slot. `obs_count`: slots at or past a keyframe's count are padding. Every segment has a keyframe whose slots are all used. `back_list`: each row holds 384 distinct own points of the segment; no point stands on both lists of its segment. `front_list`: each row holds 384 distinct own points of the segment; no point stands on both lists of its segment.
All inputs are finite; a program needn't handle non-finite values.
Results may differ from the reference program's by a relative error of at most 0.0005.
Values sent between devices are 32-bit elements; how exact they have to be, the bound alone decides.
A program may use at most 64 MiB of HBM per device.

```python
import math
import jax
import jax.numpy as jnp
from jax import lax

CAM_DEV = 16
OBS_CAM = 512
P_DEV = 1024
ITERS = 2
BORDER = 384
SEGMENTS = 32
CAMERAS = 512
POINTS = 32768


def border_lists(key):
    seg_keys = jax.random.split(jax.random.fold_in(key, 11), SEGMENTS)
    orders = jax.vmap(lambda seg_key: jax.random.permutation(seg_key, P_DEV))(seg_keys)
    return (orders[:, :BORDER].astype(jnp.int32), orders[:, BORDER:2 * BORDER].astype(jnp.int32))


def draw_back_list(key, part):
    return border_lists(key)[0]


def draw_front_list(key, part):
    return border_lists(key)[1]


def draw_obs_point(key, part):
    side_key, own_key, slot_key = jax.random.split(jax.random.fold_in(key, 3), 3)
    side_pick = jax.random.randint(side_key, (CAMERAS, OBS_CAM), 0, 4)
    segment = (jnp.arange(CAMERAS, dtype=jnp.int32) // CAM_DEV)[:, None]
    own_pick = jax.random.randint(own_key, (CAMERAS, OBS_CAM), 0, P_DEV)
    slot_pick = jax.random.randint(slot_key, (CAMERAS, OBS_CAM), 0, BORDER)
    back_side = (side_pick == 0) & (segment > 0)
    front_side = (side_pick == 1) & (segment < SEGMENTS - 1)
    result = jnp.where(back_side, P_DEV + slot_pick, jnp.where(front_side, P_DEV + BORDER + slot_pick, own_pick))
    return result.astype(jnp.int32)


def draw_obs_count(key, part):
    high_key, count_key, full_key = jax.random.split(jax.random.fold_in(key, 5), 3)
    high_cap = jax.random.randint(high_key, (SEGMENTS,), OBS_CAM // 2, OBS_CAM + 1)
    high_rows = jnp.repeat(high_cap, CAM_DEV)
    low_rows = high_rows // 4
    counts = jax.random.randint(count_key, (CAMERAS,), low_rows, high_rows + 1)
    full_pos = jnp.repeat(jax.random.randint(full_key, (SEGMENTS,), 0, CAM_DEV), CAM_DEV)
    marked = jnp.arange(CAMERAS, dtype=jnp.int32) % CAM_DEV == full_pos
    return jnp.where(marked, OBS_CAM, counts).astype(jnp.int32)


def draw_right_side(key, part):
    first_key = jax.random.fold_in(jax.random.fold_in(key, 9), 0)
    position = jnp.arange(CAMERAS, dtype=jnp.float32) / CAMERAS
    random_part = jnp.clip(jax.random.normal(first_key, (9, CAMERAS), jnp.float32), -6.0, 6.0)
    rising = 3.0 ** position
    return (random_part * rising[None, :]).astype(jnp.float32)


def steps_of(key, extent, pieces, low, top_value):
    def one(dim, shards_of):
        steps = jax.random.uniform(jax.random.fold_in(jax.random.fold_in(key, 6), dim), (shards_of,), jnp.float32, low / len(pieces), top_value / len(pieces))
        return jnp.repeat(jnp.exp(steps), extent[dim] // shards_of).reshape((-1,) + (1,) * (len(extent) - dim - 1))

    gain = one(*pieces[0])
    for cut in pieces[1:]:
        gain = gain * one(*cut)
    return gain


def scatter_about(rng, shape, width, most, pieces=(), kind=jnp.bfloat16):
    values = width * jax.random.normal(rng, shape, jnp.float32)
    if pieces:
        values = values * steps_of(rng, shape, pieces, -0.22, 0.18)
    return jnp.clip(values, -most, most).astype(kind)


def setup_inputs(seed: int = 0) -> dict:
    arg_keys = jax.random.split(jax.random.key(seed), 11)
    cam_jac = scatter_about(arg_keys[0], (18, CAMERAS, OBS_CAM), OBS_CAM ** -0.5, 0.25, ((1, 32),))
    point_jac = scatter_about(arg_keys[1], (6, CAMERAS, OBS_CAM), 1.0, 6.0, ((1, 32),))
    obs_point = draw_obs_point(jax.random.fold_in(arg_keys[10], 71), 0)
    obs_count = draw_obs_count(jax.random.fold_in(arg_keys[10], 71), 0)
    back_list = draw_back_list(jax.random.fold_in(arg_keys[10], 71), 0)
    front_list = draw_front_list(jax.random.fold_in(arg_keys[10], 71), 0)
    point_damp = jnp.clip(jnp.exp(math.log(4.0) - 2.0794415 * jax.random.uniform(arg_keys[6], (POINTS,), jnp.float32) ** steps_of(arg_keys[6], (POINTS,), ((0, 32),), -0.2, 0.2)), 0.5, 4.0)
    cam_damp = jnp.clip(jnp.exp(math.log(1.0) - 2.3025851 * jax.random.uniform(arg_keys[7], (CAMERAS,), jnp.float32) ** steps_of(arg_keys[7], (CAMERAS,), ((0, 32),), -0.2, 0.2)), 0.1, 1.0)
    right_side = draw_right_side(jax.random.fold_in(arg_keys[10], 71), 0)
    start_guess = scatter_about(arg_keys[9], (9, CAMERAS), 0.5, 3.0, ((1, 32),), jnp.float32)
    return {"cam_jac": cam_jac, "point_jac": point_jac, "obs_point": obs_point, "obs_count": obs_count, "back_list": back_list, "front_list": front_list, "point_damp": point_damp, "cam_damp": cam_damp, "right_side": right_side, "start_guess": start_guess}


ENTRY_PAIRS = ((0, 0), (0, 1), (0, 2), (1, 1), (1, 2), (2, 2))


def slot_weights(obs_count, slot_total):
    positions = lax.broadcasted_iota(jnp.int32, (obs_count.shape[0], slot_total), 1)
    return (positions < obs_count[:, None]).astype(jnp.float32)


def global_points(obs_point, back_list, front_list):
    segment = (jnp.arange(obs_point.shape[0], dtype=jnp.int32) // CAM_DEV)[:, None]
    prev_seg = jnp.clip(segment - 1, 0, SEGMENTS - 1)
    next_seg = jnp.clip(segment + 1, 0, SEGMENTS - 1)
    back_slot = jnp.clip(obs_point - P_DEV, 0, BORDER - 1)
    front_slot = jnp.clip(obs_point - P_DEV - BORDER, 0, BORDER - 1)
    own_global = segment * P_DEV + obs_point
    from_back = prev_seg * P_DEV + back_list[prev_seg, back_slot]
    from_front = next_seg * P_DEV + front_list[next_seg, front_slot]
    result = jnp.where(obs_point < P_DEV, own_global, jnp.where(obs_point < P_DEV + BORDER, from_back, from_front))
    return result.astype(jnp.int32).reshape(-1)


def symmetric_inverse(entries):
    cofactors = [entries[3] * entries[5] - entries[4] * entries[4],
                 entries[2] * entries[4] - entries[1] * entries[5],
                 entries[1] * entries[4] - entries[2] * entries[3],
                 entries[0] * entries[5] - entries[2] * entries[2],
                 entries[1] * entries[2] - entries[0] * entries[4],
                 entries[0] * entries[3] - entries[1] * entries[1]]
    determinant = entries[0] * cofactors[0] + entries[1] * cofactors[1] + entries[2] * cofactors[2]
    return [member / determinant for member in cofactors]


def apply_inverse(inverse, point_sums):
    return [inverse[0] * point_sums[0] + inverse[1] * point_sums[1] + inverse[2] * point_sums[2],
            inverse[1] * point_sums[0] + inverse[3] * point_sums[1] + inverse[4] * point_sums[2],
            inverse[2] * point_sums[0] + inverse[4] * point_sums[1] + inverse[5] * point_sums[2]]


def camera_rows(cam_jac, vector, weights):
    error_rows = []
    for row_index in range(2):
        running = cam_jac[9 * row_index].astype(jnp.float32) * vector[0][:, None]
        for column in range(1, 9):
            running = running + cam_jac[9 * row_index + column].astype(jnp.float32) * vector[column][:, None]
        error_rows.append(running * weights)
    return error_rows


def schur_apply(vector, cam_jac, point_jac, weights, owners, inverse, cam_damp):
    errors = camera_rows(cam_jac, vector, weights)
    point_sums = []
    for column in range(3):
        product = errors[0] * point_jac[column].astype(jnp.float32) + errors[1] * point_jac[3 + column].astype(jnp.float32)
        point_sums.append(jax.ops.segment_sum(product.reshape(-1), owners, num_segments=POINTS))
    values = apply_inverse(inverse, point_sums)
    picked = [member[owners].reshape(weights.shape) for member in values]
    adjusted = []
    for row_index in range(2):
        back_term = picked[0] * point_jac[3 * row_index].astype(jnp.float32)
        back_term = back_term + picked[1] * point_jac[3 * row_index + 1].astype(jnp.float32)
        back_term = back_term + picked[2] * point_jac[3 * row_index + 2].astype(jnp.float32)
        adjusted.append(errors[row_index] - weights * back_term)
    result = []
    for column in range(9):
        running = jnp.sum(cam_jac[column].astype(jnp.float32) * adjusted[0] + cam_jac[9 + column].astype(jnp.float32) * adjusted[1], axis=1)
        result.append(cam_damp * vector[column] + running)
    return jnp.stack(result)


def reference(cam_jac, point_jac, obs_point, obs_count, back_list, front_list, point_damp, cam_damp, right_side, start_guess):
    weights = slot_weights(obs_count, obs_point.shape[1])
    owners = global_points(obs_point, back_list, front_list)
    entries = []
    for lead_index, tail_index in ENTRY_PAIRS:
        product = point_jac[lead_index].astype(jnp.float32) * point_jac[tail_index].astype(jnp.float32)
        product = product + point_jac[3 + lead_index].astype(jnp.float32) * point_jac[3 + tail_index].astype(jnp.float32)
        running = jax.ops.segment_sum((product * weights).reshape(-1), owners, num_segments=POINTS)
        if lead_index == tail_index:
            running = running + point_damp
        entries.append(running)
    inverse = symmetric_inverse(entries)
    diagonal = []
    for column in range(9):
        first_sq = cam_jac[column].astype(jnp.float32) ** 2 + cam_jac[9 + column].astype(jnp.float32) ** 2
        diagonal.append(jnp.sum(first_sq * weights, axis=1) + cam_damp)
    precond = 1.0 / jnp.stack(diagonal)

    def operator(vector):
        return schur_apply(vector, cam_jac, point_jac, weights, owners, inverse, cam_damp)

    solution = start_guess
    residual = right_side - operator(solution)
    scaled = precond * residual
    direction = scaled
    inner_now = jnp.sum(residual * scaled)
    for iteration in range(ITERS):
        image = operator(direction)
        step_size = inner_now / jnp.sum(direction * image)
        solution = solution + step_size * direction
        residual = residual - step_size * image
        if iteration + 1 < ITERS:
            scaled = precond * residual
            inner_next = jnp.sum(residual * scaled)
            direction = scaled + (inner_next / inner_now) * direction
            inner_now = inner_next
    return solution, residual
```

```python
import functools

import jax
import jax.numpy as jnp
from jax import lax
from jax.experimental import pallas as pl
from jax.experimental.pallas import tpu as pltpu
from jax.sharding import PartitionSpec as P

ENTRY_PAIRS = ((0, 0), (0, 1), (0, 2), (1, 1), (1, 2), (2, 2))
F32, BF16, I32 = jnp.float32, jnp.bfloat16, jnp.int32
MESH = pl.DeviceIdType.MESH
LANES = 128
WIDE = 256
GROUP = 8
SPLITS = 2
FIRST_ROWS = (0, 9, 12)
SQUARES = tuple((lead, tail) for lead in range(9) for tail in range(lead, 9))
LOAD_ORDER = (
    "back_list",
    "front_list",
    "obs_count",
    "obs_point",
    "cam_damp",
    "start_guess",
    "right_side",
    "point_damp",
    "point_jac",
    "cam_jac",
)


def splits_of(value):
    terms = []
    for step in range(SPLITS):
        term = value.astype(BF16).astype(F32)
        terms.append(term)
        value = value - term
    return terms


def iota(shape, dim):
    return lax.broadcasted_iota(I32, shape, dim)


def dot_nt(left, right):
    return lax.dot_general(left, right, (((1,), (1,)), ((), ())), preferred_element_type=F32)


def symmetric_inverse(entries):
    cofactors = [
        entries[3] * entries[5] - entries[4] * entries[4],
        entries[2] * entries[4] - entries[1] * entries[5],
        entries[1] * entries[4] - entries[2] * entries[3],
        entries[0] * entries[5] - entries[2] * entries[2],
        entries[1] * entries[2] - entries[0] * entries[4],
        entries[0] * entries[3] - entries[1] * entries[1],
    ]
    determinant = entries[0] * cofactors[0] + entries[1] * cofactors[1] + entries[2] * cofactors[2]
    determinant = jnp.where(determinant > 0.0, determinant, 1.0)
    return [member / determinant for member in cofactors]


def apply_inverse(inverse, sums):
    return [
        inverse[0] * sums[0] + inverse[1] * sums[1] + inverse[2] * sums[2],
        inverse[1] * sums[0] + inverse[3] * sums[1] + inverse[4] * sums[2],
        inverse[2] * sums[0] + inverse[4] * sums[1] + inverse[5] * sums[2],
    ]


def kernel(
    n,
    cam_jac_hbm,
    point_jac_hbm,
    obs_point_hbm,
    obs_count_hbm,
    back_list_hbm,
    front_list_hbm,
    point_damp_hbm,
    cam_damp_hbm,
    right_side_hbm,
    start_guess_hbm,
    step_out,
    residual_out,
    group_of,
    lane_of,
    wide_jac,
    first_terms,
    terms,
    coupling,
    partial,
    vector_rows,
    squares,
    to_next,
    to_prev,
    from_prev,
    from_next,
    dots_out,
    dots_in,
    next_send,
    next_recv,
    prev_send,
    prev_recv,
    dots_send,
    dots_recv,
    cam_jac,
    point_jac,
    obs_point,
    obs_count,
    back_list,
    front_list,
    point_damp,
    cam_damp,
    right_side,
    start_guess,
    load_sem,
):
    cams, slots = obs_point.shape
    points = point_damp.shape[1]
    border = back_list.shape[1]
    edge = border // LANES
    own_groups = points // WIDE
    halves = WIDE // LANES
    me = lax.axis_index("seg")

    loads = {
        "cam_jac": pltpu.make_async_copy(cam_jac_hbm, cam_jac, load_sem.at[0]),
        "point_jac": pltpu.make_async_copy(point_jac_hbm, point_jac, load_sem.at[1]),
        "obs_point": pltpu.make_async_copy(obs_point_hbm, obs_point, load_sem.at[2]),
        "obs_count": pltpu.make_async_copy(obs_count_hbm, obs_count, load_sem.at[3]),
        "back_list": pltpu.make_async_copy(back_list_hbm, back_list, load_sem.at[4]),
        "front_list": pltpu.make_async_copy(front_list_hbm, front_list, load_sem.at[5]),
        "point_damp": pltpu.make_async_copy(point_damp_hbm, point_damp, load_sem.at[6]),
        "cam_damp": pltpu.make_async_copy(cam_damp_hbm, cam_damp, load_sem.at[7]),
        "right_side": pltpu.make_async_copy(right_side_hbm, right_side, load_sem.at[8]),
        "start_guess": pltpu.make_async_copy(start_guess_hbm, start_guess, load_sem.at[9]),
    }
    for name in LOAD_ORDER:
        loads[name].start()

    barrier = pltpu.get_barrier_semaphore()

    def greet(offset, carry):
        pl.semaphore_signal(
            barrier, inc=1, device_id=(lax.rem(me + offset, n),), device_id_type=MESH
        )
        return carry

    from_prev[...] = jnp.zeros_like(from_prev)
    from_next[...] = jnp.zeros_like(from_next)
    lax.fori_loop(1, n, greet, 0)

    loads["back_list"].wait()
    loads["front_list"].wait()
    listed = jnp.concatenate([back_list[...], front_list[...]], axis=1)
    total = 2 * border
    place = iota((1, total), 1)
    in_front = place >= border
    place = jnp.where(in_front, place - border, place)
    list_group = jnp.where(in_front, edge, 0) + lax.shift_right_logical(place, 7)
    list_lane = jnp.where(in_front, LANES, 0) + (place & (LANES - 1))
    row = iota((2 * own_groups, total), 0)
    code = jnp.where(row < own_groups, list_group + 1, list_lane)
    wanted = jnp.where(row < own_groups, row, row - own_groups)
    code = jnp.where(lax.shift_right_logical(listed, 8) == wanted, code, 0)
    hot = jnp.where(iota((WIDE, total), 0) == (listed & (WIDE - 1)), 1.0, 0.0).astype(BF16)
    table = dot_nt(code.astype(F32).astype(BF16), hot)
    table_group = table[:own_groups]
    table_lane = table[own_groups:]
    other = jnp.where(table_group == 0.0, 1.0, 0.0)
    before = jnp.where(iota((WIDE, WIDE), 0) < iota((WIDE, WIDE), 1), 1.0, 0.0).astype(BF16)
    rank = jnp.dot(other.astype(BF16), before, preferred_element_type=F32)
    counts = jnp.sum(other, axis=1, keepdims=True)
    table_row = iota((own_groups, WIDE), 0)
    for index in range(own_groups - 1):
        rank = rank + jnp.where(table_row > index, counts[index : index + 1], 0.0)
    rank = rank.astype(I32)
    is_other = other > 0.0
    table_group = jnp.where(
        is_other, (2 * edge + lax.shift_right_logical(rank, 8)).astype(F32), table_group - 1.0
    )
    table_lane = jnp.where(is_other, (rank & (WIDE - 1)).astype(F32), table_lane)

    eye = iota((cams, cams), 0) == iota((cams, cams), 1)

    def column(line):
        wide = jnp.broadcast_to(line, (cams, cams))
        return jnp.sum(jnp.where(eye, wide, jnp.zeros_like(wide)), axis=1, keepdims=True)

    def line(wide):
        return jnp.sum(jnp.where(eye, wide[:, :cams], 0.0), axis=0, keepdims=True)

    loads["obs_count"].wait()
    loads["obs_point"].wait()
    used_count = column(obs_count[...].astype(F32)).astype(I32)
    used = iota((cams, slots), 1) < used_count

    code_table = (table_group * WIDE + table_lane).astype(I32)
    rows_of_table = [
        jnp.broadcast_to(
            code_table[index // halves : index // halves + 1, part * LANES : (part + 1) * LANES],
            (GROUP, LANES),
        )
        for index in range(own_groups * halves)
        for part in (index % halves,)
    ]
    for top in range(0, cams, GROUP):
        for left in range(0, slots, LANES):
            spot = (slice(top, top + GROUP), slice(left, left + LANES))
            ids = obs_point[spot]
            back_slot = ids - points
            front_slot = back_slot - border
            in_back = ids < points + border
            side = jnp.where(
                in_back,
                lax.shift_right_logical(back_slot, 7) * WIDE + LANES + (back_slot & (LANES - 1)),
                (edge + lax.shift_right_logical(front_slot, 7)) * WIDE + (front_slot & (LANES - 1)),
            )
            id_row = lax.shift_right_logical(ids, 7)
            id_lane = ids & (LANES - 1)
            for index, row in enumerate(rows_of_table):
                found = jnp.take_along_axis(row, id_lane, axis=1, mode="promise_in_bounds")
                side = jnp.where(id_row == index, found, side)
            group_of[spot] = jnp.where(used[spot], lax.shift_right_logical(side, 8), -1)
            lane_of[spot] = side & (WIDE - 1)

    wide_row = iota((WIDE, slots), 0)
    group_row = iota((GROUP, slots), 0)

    def scatter(source, count, cam):
        mask = group_row == group_of[cam : cam + 1]
        blocks = [
            jnp.where(mask, jnp.broadcast_to(source[index, cam : cam + 1], (GROUP, slots)), 0.0)
            for index in range(SPLITS * count)
        ]
        hot = jnp.where(wide_row == lane_of[cam : cam + 1], 1.0, 0.0).astype(BF16)
        return dot_nt(jnp.concatenate(blocks, axis=0).astype(BF16), hot)

    def joined(sums, index):
        whole = sums[(SPLITS * index + SPLITS - 1) * GROUP : (SPLITS * index + SPLITS) * GROUP]
        for step in reversed(range(SPLITS - 1)):
            first = (SPLITS * index + step) * GROUP
            whole = whole + sums[first : first + GROUP]
        return whole

    def neighbour(where, turn, size):
        spot = FIRST_ROWS[turn]
        if where == "next":
            return pltpu.make_async_remote_copy(
                src_ref=to_next.at[pl.ds(spot, size)],
                dst_ref=from_prev.at[pl.ds(spot, size)],
                send_sem=next_send.at[turn],
                recv_sem=next_recv.at[turn],
                device_id=(lax.rem(me + 1, n),),
                device_id_type=MESH,
            )
        return pltpu.make_async_remote_copy(
            src_ref=to_prev.at[pl.ds(spot, size)],
            dst_ref=from_next.at[pl.ds(spot, size)],
            send_sem=prev_send.at[turn],
            recv_sem=prev_recv.at[turn],
            device_id=(lax.rem(me + n - 1, n),),
            device_id_type=MESH,
        )

    has_next = me < n - 1
    has_prev = me > 0

    def send(sums, turn):
        spot = FIRST_ROWS[turn]
        for index, member in enumerate(sums):
            to_next[spot + index] = member[:, :LANES]
            to_prev[spot + index] = member[:, LANES:]

        @pl.when(has_next)
        def _():
            neighbour("next", turn, len(sums)).start()

        @pl.when(has_prev)
        def _():
            neighbour("prev", turn, len(sums)).start()

    edge_row = iota((GROUP, LANES), 0) < 2 * edge

    def receive(sums, turn):
        spot = FIRST_ROWS[turn]
        @pl.when(has_next)
        def _():
            copy = neighbour("next", turn, len(sums))
            copy.wait_send()
            neighbour("prev", turn, len(sums)).wait_recv()

        @pl.when(has_prev)
        def _():
            copy = neighbour("prev", turn, len(sums))
            copy.wait_send()
            neighbour("next", turn, len(sums)).wait_recv()

        return [
            jnp.concatenate(
                [
                    member[:, :LANES] + jnp.where(edge_row, from_next[spot + index], 0.0),
                    member[:, LANES:] + jnp.where(edge_row, from_prev[spot + index], 0.0),
                ],
                axis=1,
            )
            for index, member in enumerate(sums)
        ]

    def pjac(index):
        return point_jac[index].astype(F32)

    def spread_out(col):
        return jnp.broadcast_to(col, (cams, LANES))

    def point_product(vector):
        for entry in range(9):
            vector_rows[entry] = vector[entry]
        running = [[None] * halves for index in range(3)]
        for cam in range(cams):
            for entry in range(9):
                scale = jnp.broadcast_to(vector_rows[entry, cam : cam + 1], (GROUP, LANES))
                for index in range(3):
                    for part in range(halves):
                        block = coupling[
                            cam * 27 + index * 9 + entry, :, part * LANES : (part + 1) * LANES
                        ]
                        term = block * scale
                        before = running[index][part]
                        running[index][part] = term if before is None else before + term
        return [jnp.concatenate(parts, axis=1) for parts in running]

    def camera_product(values):
        for cam in range(cams):
            for entry in range(9):
                whole = None
                for index in range(3):
                    for part in range(halves):
                        lanes = slice(part * LANES, (part + 1) * LANES)
                        term = coupling[cam * 27 + index * 9 + entry, :, lanes] * values[index][:, lanes]
                        whole = term if whole is None else whole + term
                partial[entry, cam * GROUP : (cam + 1) * GROUP] = whole
        result = []
        for entry in range(9):
            whole = partial[entry, pl.ds(0, cams, stride=GROUP)]
            for row in range(1, GROUP):
                whole = whole + partial[entry, pl.ds(row, cams, stride=GROUP)]
            result.append(spread_out(jnp.sum(whole, axis=1, keepdims=True)))
        return result

    def square_product(vector):
        result = [None] * 9
        for index, (lead, tail) in enumerate(SQUARES):
            block = squares[index]
            for here, there in {(lead, tail), (tail, lead)}:
                term = block * vector[there]
                result[here] = term if result[here] is None else result[here] + term
        return result

    def dot_of(left, right):
        running = left[0] * right[0]
        for entry in range(1, 9):
            running = running + left[entry] * right[entry]
        return jnp.sum(running, axis=0, keepdims=True)

    dot_lane = iota((1, LANES), 1)
    part_row = iota((GROUP, WIDE), 0)
    part_left = iota((GROUP, WIDE), 1) < LANES
    own_row = jnp.where(part_left, part_row, part_row - edge)
    is_own = jnp.where(part_left, edge - 1 - own_row, own_row) >= 0
    is_own = is_own | (part_row >= 2 * edge)

    def point_dot(left, right):
        running = left[0] * right[0]
        for index in range(1, 3):
            running = running + left[index] * right[index]
        running = jnp.where(is_own, running, 0.0)
        running = running[:, :LANES] + running[:, LANES:]
        running = jnp.sum(running, axis=0, keepdims=True)
        return jnp.broadcast_to(jnp.sum(running, axis=1, keepdims=True), (1, LANES))

    def dots_copy(offset):
        return pltpu.make_async_remote_copy(
            src_ref=dots_out,
            dst_ref=dots_in.at[offset - 1],
            send_sem=dots_send,
            recv_sem=dots_recv,
            device_id=(lax.rem(me + offset, n),),
            device_id_type=MESH,
        )

    def start_dots(offset, carry):
        dots_copy(offset).start()
        return carry

    for name in LOAD_ORDER[4:]:
        loads[name].wait()
    damp = column(cam_damp[...])
    start_col = [column(start_guess[entry : entry + 1]) for entry in range(9)]
    right = [spread_out(column(right_side[entry : entry + 1])) for entry in range(9)]
    start = [spread_out(member) for member in start_col]

    for index in range(18):
        wide_jac[index] = jnp.where(used, cam_jac[index].astype(F32), 0.0)
    errors = []
    for side in range(2):
        running = wide_jac[9 * side] * start_col[0]
        for entry in range(1, 9):
            running = running + wide_jac[9 * side + entry] * start_col[entry]
        errors.append(running)
    blocks = [
        pjac(lead) * pjac(tail) + pjac(3 + lead) * pjac(3 + tail) for lead, tail in ENTRY_PAIRS
    ]
    blocks = blocks + [
        errors[0] * pjac(entry) + errors[1] * pjac(3 + entry) for entry in range(3)
    ]
    for index, block in enumerate(blocks):
        for step, term in enumerate(splits_of(block)):
            first_terms[SPLITS * index + step] = term
    whole = scatter(first_terms, 9, 0)
    for cam in range(1, cams):
        whole = whole + scatter(first_terms, 9, cam)
    sums = [joined(whole, index) for index in range(9)]

    damping = jnp.zeros((SPLITS * GROUP, WIDE), F32)
    damp_row = iota((GROUP, WIDE), 0)
    square_row = iota((WIDE, WIDE), 0)
    for index in range(own_groups):
        here = point_damp[:, index * WIDE : (index + 1) * WIDE]
        mask = damp_row == table_group[index : index + 1].astype(I32)
        block = jnp.concatenate([jnp.where(mask, term, 0.0) for term in splits_of(here)], axis=0)
        hot = jnp.where(
            square_row == table_lane[index : index + 1].astype(I32), 1.0, 0.0
        ).astype(BF16)
        damping = damping + dot_nt(block.astype(BF16), hot)
    moved = damping[(SPLITS - 1) * GROUP :]
    for step in reversed(range(SPLITS - 1)):
        moved = moved + damping[step * GROUP : (step + 1) * GROUP]
    for index, (lead, tail) in enumerate(ENTRY_PAIRS):
        if lead == tail:
            sums[index] = sums[index] + moved

    pl.semaphore_wait(barrier, n - 1)
    send(sums, 0)

    for top in range(0, cams, GROUP):
        for left in range(0, slots, LANES):
            spot = (slice(top, top + GROUP), slice(left, left + LANES))
            camera = [wide_jac[(index, *spot)] for index in range(18)]
            for index in range(3):
                one = point_jac[(index, slice(None), spot[1])].astype(F32)[spot[0]]
                two = point_jac[(3 + index, slice(None), spot[1])].astype(F32)[spot[0]]
                for entry in range(9):
                    product = one * camera[entry] + two * camera[9 + entry]
                    for step, term in enumerate(splits_of(product)):
                        terms[(SPLITS * (index * 9 + entry) + step, *spot)] = term
    for cam in range(cams):
        whole = scatter(terms, 27, cam)
        for index in range(27):
            coupling[cam * 27 + index] = joined(whole, index)

    precond = []
    for index, (lead, tail) in enumerate(SQUARES):
        running = None
        for left in range(0, slots, LANES):
            lanes = slice(left, left + LANES)
            term = (
                wide_jac[lead, :, lanes] * wide_jac[tail, :, lanes]
                + wide_jac[9 + lead, :, lanes] * wide_jac[9 + tail, :, lanes]
            )
            running = term if running is None else running + term
        total = jnp.sum(running, axis=1, keepdims=True)
        if lead == tail:
            total = total + damp
            precond.append(spread_out(1.0 / total))
        squares[index] = spread_out(total)
    image = square_product(start)

    sums = receive(sums, 0)
    inverse = symmetric_inverse(sums[:6])
    back = camera_product(apply_inverse(inverse, sums[6:]))
    residual = [right[entry] - (image[entry] - back[entry]) for entry in range(9)]
    direction = [precond[entry] * residual[entry] for entry in range(9)]

    sums = point_product(direction)
    send(sums, 1)
    square_direction = square_product(direction)
    sums = receive(sums, 1)
    values = apply_inverse(inverse, sums)
    back = camera_product(values)
    image = [square_direction[entry] - back[entry] for entry in range(9)]
    ahead = [precond[entry] * image[entry] for entry in range(9)]

    sums_ahead = point_product(ahead)
    send(sums_ahead, 2)
    square_ahead = square_product(ahead)
    inner = dot_of(residual, direction)
    curve = dot_of(direction, image)
    weight = dot_of(image, ahead)
    shift = dot_of(residual, ahead) / jnp.where(weight > 0.0, weight, 1.0)
    shift = jnp.clip(shift, -1e6, 1e6)
    rest = [direction[entry] - shift * ahead[entry] for entry in range(9)]
    left_over = [residual[entry] - shift * image[entry] for entry in range(9)]
    square_rest = [square_direction[entry] - shift * square_ahead[entry] for entry in range(9)]
    members = [
        inner,
        curve,
        dot_of(left_over, rest),
        dot_of(rest, square_rest),
        dot_of(rest, image),
        2.0 * dot_of(left_over, ahead),
        2.0 * dot_of(rest, square_ahead),
        weight,
        weight,
        dot_of(ahead, square_ahead),
    ]
    packed = jnp.zeros((1, LANES), F32)
    for index, member in enumerate(members):
        packed = jnp.where(dot_lane == index, member, packed)
    dots_out[1] = shift
    sums_ahead = receive(sums_ahead, 2)
    values_ahead = apply_inverse(inverse, sums_ahead)
    wide_shift = jnp.concatenate([shift] * halves, axis=1)
    sums_rest = [sums[index] - wide_shift * sums_ahead[index] for index in range(3)]
    values_rest = [values[index] - wide_shift * values_ahead[index] for index in range(3)]
    packed = packed - jnp.where(dot_lane == 3, point_dot(sums_rest, values_rest), 0.0)
    packed = packed - jnp.where(dot_lane == 6, 2.0 * point_dot(sums_rest, values_ahead), 0.0)
    packed = packed - jnp.where(dot_lane == 9, point_dot(sums_ahead, values_ahead), 0.0)
    dots_out[0] = packed
    lax.fori_loop(1, n, start_dots, 0)

    back = camera_product(values_ahead)
    further = [square_ahead[entry] - back[entry] for entry in range(9)]

    pltpu.make_async_copy(dots_in, dots_in, dots_recv).wait()
    pltpu.make_async_copy(dots_in, dots_in, dots_send).wait()

    def picked(row, low, high):
        inside = (dot_lane >= low) & (dot_lane < high)
        return jnp.sum(jnp.where(inside, row, 0.0), axis=1, keepdims=True)

    whole = packed + jnp.sum(dots_in[:, 0], axis=0)
    inner = picked(whole, 0, 1)
    curve = picked(whole, 1, 2)
    step = inner / curve

    def moved_by(row, about):
        gap = about - step
        row = jnp.where(dot_lane >= 5, row * gap, row)
        return jnp.where(dot_lane >= 8, row * gap, row)

    whole = moved_by(packed, shift)
    for offset in range(1, n):
        whole = whole + moved_by(dots_in[offset - 1, 0], dots_in[offset - 1, 1])
    one = (dot_lane == 2) | (dot_lane == 5) | (dot_lane == 8)
    two = (dot_lane == 3) | (dot_lane == 6) | (dot_lane == 9)
    three = (dot_lane == 4) | (dot_lane == 7)
    inner_next = jnp.sum(jnp.where(one, whole, 0.0), axis=1, keepdims=True)
    own_curve = jnp.sum(jnp.where(two, whole, 0.0), axis=1, keepdims=True)
    cross = jnp.sum(jnp.where(three, whole, 0.0), axis=1, keepdims=True)
    ratio = inner_next / inner
    curve = own_curve + ratio * (2.0 * cross + ratio * curve)
    second = inner_next / curve
    for entry in range(9):
        scaled = direction[entry] - step * ahead[entry]
        fresh = scaled + ratio * direction[entry]
        seen = image[entry] - step * further[entry] + ratio * image[entry]
        solved = start[entry] + step * direction[entry] + second * fresh
        left = residual[entry] - step * image[entry] - second * seen
        step_out[entry : entry + 1] = line(solved)
        residual_out[entry : entry + 1] = line(left)


def solution(mesh):
    n = mesh.shape["seg"]

    def shards(
        cam_jac,
        point_jac,
        obs_point,
        obs_count,
        back_list,
        front_list,
        point_damp,
        cam_damp,
        right_side,
        start_guess,
    ):
        cams, slots = obs_point.shape
        operands = (
            cam_jac,
            point_jac,
            obs_point,
            obs_count.reshape(1, -1),
            back_list,
            front_list,
            point_damp.reshape(1, -1),
            cam_damp.reshape(1, -1),
            right_side,
            start_guess,
        )
        vector = jax.ShapeDtypeStruct(right_side.shape, F32)
        return pl.pallas_call(
            functools.partial(kernel, n),
            out_shape=(vector, vector),
            in_specs=[pl.BlockSpec(memory_space=pltpu.HBM)] * 10,
            out_specs=(pl.BlockSpec(memory_space=pltpu.VMEM),) * 2,
            scratch_shapes=[
                pltpu.VMEM((cams, slots), I32),
                pltpu.VMEM((cams, slots), I32),
                pltpu.VMEM((18, cams, slots), F32),
                pltpu.VMEM((SPLITS * 9, cams, slots), F32),
                pltpu.VMEM((SPLITS * 27, cams, slots), F32),
                pltpu.VMEM((cams * 27, GROUP, WIDE), F32),
                pltpu.VMEM((9, cams * GROUP, LANES), F32),
                pltpu.VMEM((9, cams, LANES), F32),
                pltpu.VMEM((len(SQUARES), cams, LANES), F32),
                pltpu.VMEM((15, GROUP, LANES), F32),
                pltpu.VMEM((15, GROUP, LANES), F32),
                pltpu.VMEM((15, GROUP, LANES), F32),
                pltpu.VMEM((15, GROUP, LANES), F32),
                pltpu.VMEM((2, 1, LANES), F32),
                pltpu.VMEM((n - 1, 2, 1, LANES), F32),
                pltpu.SemaphoreType.DMA((3,)),
                pltpu.SemaphoreType.DMA((3,)),
                pltpu.SemaphoreType.DMA((3,)),
                pltpu.SemaphoreType.DMA((3,)),
                pltpu.SemaphoreType.DMA,
                pltpu.SemaphoreType.DMA,
                *[pltpu.VMEM(member.shape, member.dtype) for member in operands],
                pltpu.SemaphoreType.DMA((len(operands),)),
            ],
            compiler_params=pltpu.CompilerParams(
                collective_id=0, has_side_effects=True, vmem_limit_bytes=56 * 1024 * 1024
            ),
            name="schur_cg",
        )(*operands)

    return jax.shard_map(
        shards,
        mesh=mesh,
        in_specs=(
            P(None, "seg", None),
            P(None, "seg", None),
            P("seg", None),
            P("seg"),
            P("seg", None),
            P("seg", None),
            P("seg"),
            P("seg"),
            P(None, "seg"),
            P(None, "seg"),
        ),
        out_specs=(P(None, "seg"), P(None, "seg")),
        check_vma=False,
    )
```

```python
import functools

import jax
import jax.numpy as jnp
from jax import lax
from jax.experimental import pallas as pl
from jax.experimental.pallas import tpu as pltpu
from jax.sharding import PartitionSpec as P

ENTRY_PAIRS = ((0, 0), (0, 1), (0, 2), (1, 1), (1, 2), (2, 2))
F32, BF16, I32 = jnp.float32, jnp.bfloat16, jnp.int32
MESH = pl.DeviceIdType.MESH
LANES = 128
WIDE = 256
GROUP = 8
SPLITS = 2
FIRST_ROWS = (0, 9, 12)
SQUARES = tuple((lead, tail) for lead in range(9) for tail in range(lead, 9))
LOAD_ORDER = (
    "back_list",
    "front_list",
    "obs_count",
    "obs_point",
    "cam_damp",
    "start_guess",
    "right_side",
    "point_damp",
    "point_jac",
    "cam_jac",
)


def splits_of(value):
    terms = []
    for step in range(SPLITS):
        term = value.astype(BF16).astype(F32)
        terms.append(term)
        value = value - term
    return terms


def iota(shape, dim):
    return lax.broadcasted_iota(I32, shape, dim)


def dot_nt(left, right):
    return lax.dot_general(left, right, (((1,), (1,)), ((), ())), preferred_element_type=F32)


def symmetric_inverse(entries):
    cofactors = [
        entries[3] * entries[5] - entries[4] * entries[4],
        entries[2] * entries[4] - entries[1] * entries[5],
        entries[1] * entries[4] - entries[2] * entries[3],
        entries[0] * entries[5] - entries[2] * entries[2],
        entries[1] * entries[2] - entries[0] * entries[4],
        entries[0] * entries[3] - entries[1] * entries[1],
    ]
    determinant = entries[0] * cofactors[0] + entries[1] * cofactors[1] + entries[2] * cofactors[2]
    determinant = jnp.where(determinant > 0.0, determinant, 1.0)
    return [member / determinant for member in cofactors]


def apply_inverse(inverse, sums):
    return [
        inverse[0] * sums[0] + inverse[1] * sums[1] + inverse[2] * sums[2],
        inverse[1] * sums[0] + inverse[3] * sums[1] + inverse[4] * sums[2],
        inverse[2] * sums[0] + inverse[4] * sums[1] + inverse[5] * sums[2],
    ]


def kernel(
    n,
    cam_jac_hbm,
    point_jac_hbm,
    obs_point_hbm,
    obs_count_hbm,
    back_list_hbm,
    front_list_hbm,
    point_damp_hbm,
    cam_damp_hbm,
    right_side_hbm,
    start_guess_hbm,
    packed_out,
    group_of,
    lane_of,
    wide_jac,
    first_terms,
    terms,
    coupling,
    partial,
    vector_rows,
    squares,
    to_next,
    to_prev,
    from_prev,
    from_next,
    dots_out,
    dots_in,
    next_send,
    next_recv,
    prev_send,
    prev_recv,
    dots_send,
    dots_recv,
    told,
    cam_jac,
    point_jac,
    obs_point,
    obs_count,
    back_list,
    front_list,
    point_damp,
    cam_damp,
    right_side,
    start_guess,
    load_sem,
):
    cams, slots = obs_point.shape
    points = point_damp.shape[1]
    border = back_list.shape[1]
    edge = border // LANES
    own_groups = points // WIDE
    halves = WIDE // LANES
    me = lax.axis_index("seg")

    loads = {
        "cam_jac": pltpu.make_async_copy(cam_jac_hbm, cam_jac, load_sem.at[0]),
        "point_jac": pltpu.make_async_copy(point_jac_hbm, point_jac, load_sem.at[1]),
        "obs_point": pltpu.make_async_copy(obs_point_hbm, obs_point, load_sem.at[2]),
        "obs_count": pltpu.make_async_copy(obs_count_hbm, obs_count, load_sem.at[3]),
        "back_list": pltpu.make_async_copy(back_list_hbm, back_list, load_sem.at[4]),
        "front_list": pltpu.make_async_copy(front_list_hbm, front_list, load_sem.at[5]),
        "point_damp": pltpu.make_async_copy(point_damp_hbm, point_damp, load_sem.at[6]),
        "cam_damp": pltpu.make_async_copy(cam_damp_hbm, cam_damp, load_sem.at[7]),
        "right_side": pltpu.make_async_copy(right_side_hbm, right_side, load_sem.at[8]),
        "start_guess": pltpu.make_async_copy(start_guess_hbm, start_guess, load_sem.at[9]),
    }
    for name in LOAD_ORDER:
        loads[name].start()

    barrier = pltpu.get_barrier_semaphore()

    from_prev[...] = jnp.zeros_like(from_prev)
    from_next[...] = jnp.zeros_like(from_next)

    reaches = []
    while 2 ** len(reaches) < n:
        reaches.insert(0, 2 ** len(reaches))
    has_next = me < n - 1
    has_prev = me > 0
    for reach in reaches:
        pl.semaphore_signal(
            barrier, inc=1, device_id=(lax.rem(me + n - reach, n),), device_id_type=MESH
        )

    @pl.when(has_next)
    def _():
        pl.semaphore_signal(barrier, inc=1, device_id=(me + 1,), device_id_type=MESH)

    def tell(turn):
        pl.semaphore_signal(
            told.at[turn],
            inc=1,
            device_id=(lax.rem(me + reaches[turn], n),),
            device_id_type=MESH,
        )

    def hear(turn):
        pl.semaphore_wait(told.at[turn], 1)
        if turn + 1 < len(reaches):
            tell(turn + 1)


    loads["back_list"].wait()
    loads["front_list"].wait()
    listed = jnp.concatenate([back_list[...], front_list[...]], axis=1)
    total = 2 * border
    place = iota((1, total), 1)
    in_front = place >= border
    place = jnp.where(in_front, place - border, place)
    list_group = jnp.where(in_front, edge, 0) + lax.shift_right_logical(place, 7)
    list_lane = jnp.where(in_front, LANES, 0) + (place & (LANES - 1))
    row = iota((2 * own_groups, total), 0)
    code = jnp.where(row < own_groups, list_group + 1, list_lane)
    wanted = jnp.where(row < own_groups, row, row - own_groups)
    code = jnp.where(lax.shift_right_logical(listed, 8) == wanted, code, 0)
    hot = jnp.where(iota((WIDE, total), 0) == (listed & (WIDE - 1)), 1.0, 0.0).astype(BF16)
    table = dot_nt(code.astype(F32).astype(BF16), hot)
    table_group = table[:own_groups]
    table_lane = table[own_groups:]
    other = jnp.where(table_group == 0.0, 1.0, 0.0)
    before = jnp.where(iota((WIDE, WIDE), 0) < iota((WIDE, WIDE), 1), 1.0, 0.0).astype(BF16)
    rank = jnp.dot(other.astype(BF16), before, preferred_element_type=F32)
    counts = jnp.sum(other, axis=1, keepdims=True)
    table_row = iota((own_groups, WIDE), 0)
    for index in range(own_groups - 1):
        rank = rank + jnp.where(table_row > index, counts[index : index + 1], 0.0)
    rank = rank.astype(I32)
    is_other = other > 0.0
    table_group = jnp.where(
        is_other, (2 * edge + lax.shift_right_logical(rank, 8)).astype(F32), table_group - 1.0
    )
    table_lane = jnp.where(is_other, (rank & (WIDE - 1)).astype(F32), table_lane)

    eye = iota((cams, cams), 0) == iota((cams, cams), 1)

    def column(line):
        wide = jnp.broadcast_to(line, (cams, cams))
        return jnp.sum(jnp.where(eye, wide, jnp.zeros_like(wide)), axis=1, keepdims=True)

    def line(wide):
        return jnp.sum(jnp.where(eye, wide[:, :cams], 0.0), axis=0, keepdims=True)

    loads["obs_count"].wait()
    loads["obs_point"].wait()
    used_count = column(obs_count[...].astype(F32)).astype(I32)
    used = iota((cams, slots), 1) < used_count

    code_table = (table_group * WIDE + table_lane).astype(I32)
    rows_of_table = [
        jnp.broadcast_to(
            code_table[index // halves : index // halves + 1, part * LANES : (part + 1) * LANES],
            (GROUP, LANES),
        )
        for index in range(own_groups * halves)
        for part in (index % halves,)
    ]
    for top in range(0, cams, GROUP):
        for left in range(0, slots, LANES):
            spot = (slice(top, top + GROUP), slice(left, left + LANES))
            ids = obs_point[spot]
            back_slot = ids - points
            front_slot = back_slot - border
            in_back = ids < points + border
            side = jnp.where(
                in_back,
                lax.shift_right_logical(back_slot, 7) * WIDE + LANES + (back_slot & (LANES - 1)),
                (edge + lax.shift_right_logical(front_slot, 7)) * WIDE + (front_slot & (LANES - 1)),
            )
            id_row = lax.shift_right_logical(ids, 7)
            id_lane = ids & (LANES - 1)
            for index, row in enumerate(rows_of_table):
                found = jnp.take_along_axis(row, id_lane, axis=1, mode="promise_in_bounds")
                side = jnp.where(id_row == index, found, side)
            group_of[spot] = jnp.where(used[spot], lax.shift_right_logical(side, 8), -1)
            lane_of[spot] = side & (WIDE - 1)

    pair_rows = [
        (iota((2 * GROUP, slots), 0) + first).astype(jnp.int16)
        for first in range(0, WIDE, 2 * GROUP)
    ]
    unit = jnp.ones((2 * GROUP, slots), BF16)
    nil = jnp.zeros((2 * GROUP, slots), BF16)
    group_row = iota((GROUP, slots), 0)

    def scatter(source, count, cam):
        mask = group_row == group_of[cam : cam + 1]
        blocks = [
            jnp.where(mask, jnp.broadcast_to(source[index, cam : cam + 1], (GROUP, slots)), 0.0)
            for index in range(SPLITS * count)
        ]
        lanes = jnp.broadcast_to(lane_of[cam : cam + 1], (2 * GROUP, slots)).astype(jnp.int16)
        hot = jnp.concatenate(
            [jnp.where(row == lanes, unit, nil) for row in pair_rows], axis=0
        )
        return dot_nt(jnp.concatenate(blocks, axis=0).astype(BF16), hot)

    def joined(sums, index):
        whole = sums[(SPLITS * index + SPLITS - 1) * GROUP : (SPLITS * index + SPLITS) * GROUP]
        for step in reversed(range(SPLITS - 1)):
            first = (SPLITS * index + step) * GROUP
            whole = whole + sums[first : first + GROUP]
        return whole

    def neighbour(where, turn, size):
        spot = FIRST_ROWS[turn]
        if where == "next":
            return pltpu.make_async_remote_copy(
                src_ref=to_next.at[pl.ds(spot, size)],
                dst_ref=from_prev.at[pl.ds(spot, size)],
                send_sem=next_send.at[turn],
                recv_sem=next_recv.at[turn],
                device_id=(lax.rem(me + 1, n),),
                device_id_type=MESH,
            )
        return pltpu.make_async_remote_copy(
            src_ref=to_prev.at[pl.ds(spot, size)],
            dst_ref=from_next.at[pl.ds(spot, size)],
            send_sem=prev_send.at[turn],
            recv_sem=prev_recv.at[turn],
            device_id=(lax.rem(me + n - 1, n),),
            device_id_type=MESH,
        )

    def send(sums, turn):
        spot = FIRST_ROWS[turn]
        for index, member in enumerate(sums):
            to_next[spot + index] = member[:, :LANES]
            to_prev[spot + index] = member[:, LANES:]

        @pl.when(has_next)
        def _():
            neighbour("next", turn, len(sums)).start()

        @pl.when(has_prev)
        def _():
            neighbour("prev", turn, len(sums)).start()

    edge_row = iota((GROUP, LANES), 0) < 2 * edge

    def receive(sums, turn):
        spot = FIRST_ROWS[turn]
        @pl.when(has_next)
        def _():
            copy = neighbour("next", turn, len(sums))
            copy.wait_send()
            neighbour("prev", turn, len(sums)).wait_recv()

        @pl.when(has_prev)
        def _():
            copy = neighbour("prev", turn, len(sums))
            copy.wait_send()
            neighbour("next", turn, len(sums)).wait_recv()

        return [
            jnp.concatenate(
                [
                    member[:, :LANES] + jnp.where(edge_row, from_next[spot + index], 0.0),
                    member[:, LANES:] + jnp.where(edge_row, from_prev[spot + index], 0.0),
                ],
                axis=1,
            )
            for index, member in enumerate(sums)
        ]

    def pjac(index):
        return point_jac[index].astype(F32)

    def spread_out(col):
        return jnp.broadcast_to(col, (cams, LANES))

    def point_product(vector):
        for entry in range(9):
            vector_rows[entry] = vector[entry]
        running = [[None] * halves for index in range(3)]
        for cam in range(cams):
            for entry in range(9):
                scale = jnp.broadcast_to(vector_rows[entry, cam : cam + 1], (GROUP, LANES))
                for index in range(3):
                    for part in range(halves):
                        block = coupling[
                            cam * 27 + index * 9 + entry, :, part * LANES : (part + 1) * LANES
                        ]
                        term = block * scale
                        before = running[index][part]
                        running[index][part] = term if before is None else before + term
        return [jnp.concatenate(parts, axis=1) for parts in running]

    def camera_product(values):
        for cam in range(cams):
            for entry in range(9):
                whole = None
                for index in range(3):
                    for part in range(halves):
                        lanes = slice(part * LANES, (part + 1) * LANES)
                        term = coupling[cam * 27 + index * 9 + entry, :, lanes] * values[index][:, lanes]
                        whole = term if whole is None else whole + term
                partial[entry, cam * GROUP : (cam + 1) * GROUP] = whole
        result = []
        for entry in range(9):
            whole = partial[entry, pl.ds(0, cams, stride=GROUP)]
            for row in range(1, GROUP):
                whole = whole + partial[entry, pl.ds(row, cams, stride=GROUP)]
            result.append(spread_out(jnp.sum(whole, axis=1, keepdims=True)))
        return result

    def square_product(vector):
        result = [None] * 9
        for index, (lead, tail) in enumerate(SQUARES):
            block = squares[index]
            for here, there in {(lead, tail), (tail, lead)}:
                term = block * vector[there]
                result[here] = term if result[here] is None else result[here] + term
        return result

    def dot_of(left, right):
        running = left[0] * right[0]
        for entry in range(1, 9):
            running = running + left[entry] * right[entry]
        return jnp.sum(running, axis=0, keepdims=True)

    dot_lane = iota((1, LANES), 1)
    part_row = iota((GROUP, WIDE), 0)
    part_left = iota((GROUP, WIDE), 1) < LANES
    own_row = jnp.where(part_left, part_row, part_row - edge)
    is_own = jnp.where(part_left, edge - 1 - own_row, own_row) >= 0
    is_own = is_own | (part_row >= 2 * edge)

    def point_dot(left, right):
        running = left[0] * right[0]
        for index in range(1, 3):
            running = running + left[index] * right[index]
        running = jnp.where(is_own, running, 0.0)
        running = running[:, :LANES] + running[:, LANES:]
        running = jnp.sum(running, axis=0, keepdims=True)
        return jnp.broadcast_to(jnp.sum(running, axis=1, keepdims=True), (1, LANES))

    def dots_copy(offset):
        return pltpu.make_async_remote_copy(
            src_ref=dots_out,
            dst_ref=dots_in.at[offset - 1],
            send_sem=dots_send,
            recv_sem=dots_recv,
            device_id=(lax.rem(me + offset, n),),
            device_id_type=MESH,
        )

    def start_dots(offset, carry):
        dots_copy(offset).start()
        return carry

    for name in LOAD_ORDER[4:]:
        loads[name].wait()
    damp = column(cam_damp[...])
    start_col = [column(start_guess[entry : entry + 1]) for entry in range(9)]
    right = [spread_out(column(right_side[entry : entry + 1])) for entry in range(9)]
    start = [spread_out(member) for member in start_col]

    for index in range(18):
        wide_jac[index] = jnp.where(used, cam_jac[index].astype(F32), 0.0)
    errors = []
    for side in range(2):
        running = wide_jac[9 * side] * start_col[0]
        for entry in range(1, 9):
            running = running + wide_jac[9 * side + entry] * start_col[entry]
        errors.append(running)
    blocks = [
        pjac(lead) * pjac(tail) + pjac(3 + lead) * pjac(3 + tail) for lead, tail in ENTRY_PAIRS
    ]
    blocks = blocks + [
        errors[0] * pjac(entry) + errors[1] * pjac(3 + entry) for entry in range(3)
    ]
    for index, block in enumerate(blocks):
        for step, term in enumerate(splits_of(block)):
            first_terms[SPLITS * index + step] = term
    chains = [scatter(first_terms, 9, 0), scatter(first_terms, 9, 1)]
    for cam in range(2, cams):
        chains[cam % 2] = chains[cam % 2] + scatter(first_terms, 9, cam)
    for index in range(9):
        coupling[index] = joined(chains[0], index)
    whole = chains[1]
    sums = [joined(whole, index) + coupling[index] for index in range(9)]

    damping = jnp.zeros((SPLITS * GROUP, WIDE), F32)
    damp_row = iota((GROUP, WIDE), 0)
    square_row = iota((WIDE, WIDE), 0)
    for index in range(own_groups):
        here = point_damp[:, index * WIDE : (index + 1) * WIDE]
        mask = damp_row == table_group[index : index + 1].astype(I32)
        block = jnp.concatenate([jnp.where(mask, term, 0.0) for term in splits_of(here)], axis=0)
        hot = jnp.where(
            square_row == table_lane[index : index + 1].astype(I32), 1.0, 0.0
        ).astype(BF16)
        damping = damping + dot_nt(block.astype(BF16), hot)
    moved = damping[(SPLITS - 1) * GROUP :]
    for step in reversed(range(SPLITS - 1)):
        moved = moved + damping[step * GROUP : (step + 1) * GROUP]
    for index, (lead, tail) in enumerate(ENTRY_PAIRS):
        if lead == tail:
            sums[index] = sums[index] + moved

    pl.semaphore_wait(barrier, len(reaches) + jnp.where(has_prev, 1, 0))
    tell(0)
    send(sums, 0)

    for top in range(0, cams, GROUP):
        for left in range(0, slots, LANES):
            spot = (slice(top, top + GROUP), slice(left, left + LANES))
            camera = [wide_jac[(index, *spot)] for index in range(18)]
            for index in range(3):
                one = point_jac[(index, slice(None), spot[1])].astype(F32)[spot[0]]
                two = point_jac[(3 + index, slice(None), spot[1])].astype(F32)[spot[0]]
                for entry in range(9):
                    product = one * camera[entry] + two * camera[9 + entry]
                    for step, term in enumerate(splits_of(product)):
                        terms[(SPLITS * (index * 9 + entry) + step, *spot)] = term
    for cam in range(cams):
        whole = scatter(terms, 27, cam)
        for index in range(27):
            coupling[cam * 27 + index] = joined(whole, index)

    precond = []
    for index, (lead, tail) in enumerate(SQUARES):
        running = None
        for left in range(0, slots, LANES):
            lanes = slice(left, left + LANES)
            term = (
                wide_jac[lead, :, lanes] * wide_jac[tail, :, lanes]
                + wide_jac[9 + lead, :, lanes] * wide_jac[9 + tail, :, lanes]
            )
            running = term if running is None else running + term
        total = jnp.sum(running, axis=1, keepdims=True)
        if lead == tail:
            total = total + damp
            precond.append(spread_out(1.0 / total))
        squares[index] = spread_out(total)
    image = square_product(start)

    hear(0)
    sums = receive(sums, 0)
    inverse = symmetric_inverse(sums[:6])
    back = camera_product(apply_inverse(inverse, sums[6:]))
    residual = [right[entry] - (image[entry] - back[entry]) for entry in range(9)]
    direction = [precond[entry] * residual[entry] for entry in range(9)]

    sums = point_product(direction)
    send(sums, 1)
    hear(1)
    square_direction = square_product(direction)
    hear(2)
    sums = receive(sums, 1)
    values = apply_inverse(inverse, sums)
    back = camera_product(values)
    image = [square_direction[entry] - back[entry] for entry in range(9)]
    ahead = [precond[entry] * image[entry] for entry in range(9)]

    sums_ahead = point_product(ahead)
    send(sums_ahead, 2)
    hear(3)
    square_ahead = square_product(ahead)
    inner = dot_of(residual, direction)
    curve = dot_of(direction, image)
    weight = dot_of(image, ahead)
    shift = dot_of(residual, ahead) / jnp.where(weight > 0.0, weight, 1.0)
    shift = jnp.clip(shift, -1e6, 1e6)
    rest = [direction[entry] - shift * ahead[entry] for entry in range(9)]
    left_over = [residual[entry] - shift * image[entry] for entry in range(9)]
    square_rest = [square_direction[entry] - shift * square_ahead[entry] for entry in range(9)]
    members = [
        inner,
        curve,
        dot_of(left_over, rest),
        dot_of(rest, square_rest),
        dot_of(rest, image),
        2.0 * dot_of(left_over, ahead),
        2.0 * dot_of(rest, square_ahead),
        weight,
        weight,
        dot_of(ahead, square_ahead),
    ]
    packed = jnp.zeros((1, LANES), F32)
    for index, member in enumerate(members):
        packed = jnp.where(dot_lane == index, member, packed)
    dots_out[1] = shift
    for turn in range(4, len(reaches)):
        hear(turn)
    sums_ahead = receive(sums_ahead, 2)
    values_ahead = apply_inverse(inverse, sums_ahead)
    wide_shift = jnp.concatenate([shift] * halves, axis=1)
    sums_rest = [sums[index] - wide_shift * sums_ahead[index] for index in range(3)]
    values_rest = [values[index] - wide_shift * values_ahead[index] for index in range(3)]
    packed = packed - jnp.where(dot_lane == 3, point_dot(sums_rest, values_rest), 0.0)
    packed = packed - jnp.where(dot_lane == 6, 2.0 * point_dot(sums_rest, values_ahead), 0.0)
    packed = packed - jnp.where(dot_lane == 9, point_dot(sums_ahead, values_ahead), 0.0)
    dots_out[0] = packed
    lax.fori_loop(1, n, start_dots, 0)

    back = camera_product(values_ahead)
    further = [square_ahead[entry] - back[entry] for entry in range(9)]

    pltpu.make_async_copy(dots_in, dots_in, dots_recv).wait()
    pltpu.make_async_copy(dots_in, dots_in, dots_send).wait()

    def picked(row, low, high):
        inside = (dot_lane >= low) & (dot_lane < high)
        return jnp.sum(jnp.where(inside, row, 0.0), axis=1, keepdims=True)

    whole = packed + jnp.sum(dots_in[:, 0], axis=0)
    inner = picked(whole, 0, 1)
    curve = picked(whole, 1, 2)
    step = inner / curve

    def moved_by(row, about):
        gap = about - step
        row = jnp.where(dot_lane >= 5, row * gap, row)
        return jnp.where(dot_lane >= 8, row * gap, row)

    whole = moved_by(packed, shift)
    for offset in range(1, n):
        whole = whole + moved_by(dots_in[offset - 1, 0], dots_in[offset - 1, 1])
    one = (dot_lane == 2) | (dot_lane == 5) | (dot_lane == 8)
    two = (dot_lane == 3) | (dot_lane == 6) | (dot_lane == 9)
    three = (dot_lane == 4) | (dot_lane == 7)
    inner_next = jnp.sum(jnp.where(one, whole, 0.0), axis=1, keepdims=True)
    own_curve = jnp.sum(jnp.where(two, whole, 0.0), axis=1, keepdims=True)
    cross = jnp.sum(jnp.where(three, whole, 0.0), axis=1, keepdims=True)
    ratio = inner_next / inner
    curve = own_curve + ratio * (2.0 * cross + ratio * curve)
    second = inner_next / curve
    for entry in range(9):
        scaled = direction[entry] - step * ahead[entry]
        fresh = scaled + ratio * direction[entry]
        seen = image[entry] - step * further[entry] + ratio * image[entry]
        solved = start[entry] + step * direction[entry] + second * fresh
        left = residual[entry] - step * image[entry] - second * seen
        packed_out[entry : entry + 1] = line(solved)
        packed_out[16 + entry : 17 + entry] = line(left)


def solution(mesh):
    n = mesh.shape["seg"]

    def shards(
        cam_jac,
        point_jac,
        obs_point,
        obs_count,
        back_list,
        front_list,
        point_damp,
        cam_damp,
        right_side,
        start_guess,
    ):
        cams, slots = obs_point.shape
        operands = (
            cam_jac,
            point_jac,
            obs_point,
            obs_count.reshape(1, -1),
            back_list,
            front_list,
            point_damp.reshape(1, -1),
            cam_damp.reshape(1, -1),
            right_side,
            start_guess,
        )
        vector = jax.ShapeDtypeStruct(right_side.shape, F32)
        found = pl.pallas_call(
            functools.partial(kernel, n),
            out_shape=pltpu.VMEM((32, right_side.shape[1]), F32),
            in_specs=[pl.BlockSpec(memory_space=pltpu.HBM)] * 10,
            out_specs=pl.BlockSpec(memory_space=pltpu.VMEM),
            scratch_shapes=[
                pltpu.VMEM((cams, slots), I32),
                pltpu.VMEM((cams, slots), I32),
                pltpu.VMEM((18, cams, slots), F32),
                pltpu.VMEM((SPLITS * 9, cams, slots), F32),
                pltpu.VMEM((SPLITS * 27, cams, slots), F32),
                pltpu.VMEM((cams * 27, GROUP, WIDE), F32),
                pltpu.VMEM((9, cams * GROUP, LANES), F32),
                pltpu.VMEM((9, cams, LANES), F32),
                pltpu.VMEM((len(SQUARES), cams, LANES), F32),
                pltpu.VMEM((15, GROUP, LANES), F32),
                pltpu.VMEM((15, GROUP, LANES), F32),
                pltpu.VMEM((15, GROUP, LANES), F32),
                pltpu.VMEM((15, GROUP, LANES), F32),
                pltpu.VMEM((2, 1, LANES), F32),
                pltpu.VMEM((n - 1, 2, 1, LANES), F32),
                pltpu.SemaphoreType.DMA((3,)),
                pltpu.SemaphoreType.DMA((3,)),
                pltpu.SemaphoreType.DMA((3,)),
                pltpu.SemaphoreType.DMA((3,)),
                pltpu.SemaphoreType.DMA,
                pltpu.SemaphoreType.DMA,
                pltpu.SemaphoreType.REGULAR((max(1, (n - 1).bit_length()),)),
                *[pltpu.VMEM(member.shape, member.dtype) for member in operands],
                pltpu.SemaphoreType.DMA((len(operands),)),
            ],
            compiler_params=pltpu.CompilerParams(
                collective_id=0, has_side_effects=True, vmem_limit_bytes=56 * 1024 * 1024
            ),
            name="schur_cg",
        )(*operands)
        return found[:9], found[16:25]

    return jax.shard_map(
        shards,
        mesh=mesh,
        in_specs=(
            P(None, "seg", None),
            P(None, "seg", None),
            P("seg", None),
            P("seg"),
            P("seg", None),
            P("seg", None),
            P("seg"),
            P("seg"),
            P(None, "seg"),
            P(None, "seg"),
        ),
        out_specs=(P(None, "seg"), P(None, "seg")),
        check_vma=False,
    )
```

```python
import functools

import jax
import jax.numpy as jnp
from jax import lax
from jax.experimental import pallas as pl
from jax.experimental.pallas import tpu as pltpu
from jax.sharding import PartitionSpec as P

ENTRY_PAIRS = ((0, 0), (0, 1), (0, 2), (1, 1), (1, 2), (2, 2))
F32, BF16, I32 = jnp.float32, jnp.bfloat16, jnp.int32
MESH = pl.DeviceIdType.MESH
LANES = 128
WIDE = 256
GROUP = 8
SPLITS = 2
FIRST_ROWS = (0, 9, 12)
SQUARES = tuple((lead, tail) for lead in range(9) for tail in range(lead, 9))
LOAD_ORDER = (
    "obs_count",
    "obs_point",
    "start_guess",
    "point_jac",
    "cam_jac",
    "back_list",
    "front_list",
    "point_damp",
    "cam_damp",
    "right_side",
)


def splits_of(value):
    terms = []
    for step in range(SPLITS):
        term = value.astype(BF16).astype(F32)
        terms.append(term)
        value = value - term
    return terms


def iota(shape, dim):
    return lax.broadcasted_iota(I32, shape, dim)


def dot_nt(left, right):
    return lax.dot_general(left, right, (((1,), (1,)), ((), ())), preferred_element_type=F32)


def symmetric_inverse(entries):
    cofactors = [
        entries[3] * entries[5] - entries[4] * entries[4],
        entries[2] * entries[4] - entries[1] * entries[5],
        entries[1] * entries[4] - entries[2] * entries[3],
        entries[0] * entries[5] - entries[2] * entries[2],
        entries[1] * entries[2] - entries[0] * entries[4],
        entries[0] * entries[3] - entries[1] * entries[1],
    ]
    determinant = entries[0] * cofactors[0] + entries[1] * cofactors[1] + entries[2] * cofactors[2]
    determinant = jnp.where(determinant > 0.0, determinant, 1.0)
    return [member / determinant for member in cofactors]


def apply_inverse(inverse, sums):
    return [
        inverse[0] * sums[0] + inverse[1] * sums[1] + inverse[2] * sums[2],
        inverse[1] * sums[0] + inverse[3] * sums[1] + inverse[4] * sums[2],
        inverse[2] * sums[0] + inverse[4] * sums[1] + inverse[5] * sums[2],
    ]


def kernel(
    n,
    cam_jac_hbm,
    point_jac_hbm,
    obs_point_hbm,
    obs_count_hbm,
    back_list_hbm,
    front_list_hbm,
    point_damp_hbm,
    cam_damp_hbm,
    right_side_hbm,
    start_guess_hbm,
    packed_out,
    group_of,
    lane_of,
    wide_jac,
    first_terms,
    terms,
    coupling,
    partial,
    vector_rows,
    squares,
    to_next,
    to_prev,
    from_prev,
    from_next,
    dots_out,
    dots_in,
    next_send,
    next_recv,
    prev_send,
    prev_recv,
    dots_send,
    dots_recv,
    told,
    cam_jac,
    point_jac,
    obs_point,
    obs_count,
    back_list,
    front_list,
    point_damp,
    cam_damp,
    right_side,
    start_guess,
    load_sem,
):
    cams, slots = obs_point.shape
    points = point_damp.shape[1]
    border = back_list.shape[1]
    edge = border // LANES
    halves = WIDE // LANES
    me = lax.axis_index("seg")

    loads = {
        "cam_jac": pltpu.make_async_copy(cam_jac_hbm, cam_jac, load_sem.at[0]),
        "point_jac": pltpu.make_async_copy(point_jac_hbm, point_jac, load_sem.at[1]),
        "obs_point": pltpu.make_async_copy(obs_point_hbm, obs_point, load_sem.at[2]),
        "obs_count": pltpu.make_async_copy(obs_count_hbm, obs_count, load_sem.at[3]),
        "back_list": pltpu.make_async_copy(back_list_hbm, back_list, load_sem.at[4]),
        "front_list": pltpu.make_async_copy(front_list_hbm, front_list, load_sem.at[5]),
        "point_damp": pltpu.make_async_copy(point_damp_hbm, point_damp, load_sem.at[6]),
        "cam_damp": pltpu.make_async_copy(cam_damp_hbm, cam_damp, load_sem.at[7]),
        "right_side": pltpu.make_async_copy(right_side_hbm, right_side, load_sem.at[8]),
        "start_guess": pltpu.make_async_copy(start_guess_hbm, start_guess, load_sem.at[9]),
    }
    for name in LOAD_ORDER:
        loads[name].start()

    barrier = pltpu.get_barrier_semaphore()

    from_prev[...] = jnp.zeros_like(from_prev)
    from_next[...] = jnp.zeros_like(from_next)

    reaches = []
    while 2 ** len(reaches) < n:
        reaches.insert(0, 2 ** len(reaches))
    has_next = me < n - 1
    has_prev = me > 0
    for reach in reaches:
        pl.semaphore_signal(
            barrier, inc=1, device_id=(lax.rem(me + n - reach, n),), device_id_type=MESH
        )

    @pl.when(has_next)
    def _():
        pl.semaphore_signal(barrier, inc=1, device_id=(me + 1,), device_id_type=MESH)

    def tell(turn):
        pl.semaphore_signal(
            told.at[turn],
            inc=1,
            device_id=(lax.rem(me + reaches[turn], n),),
            device_id_type=MESH,
        )

    def hear(turn):
        pl.semaphore_wait(told.at[turn], 1)
        if turn + 1 < len(reaches):
            tell(turn + 1)


    eye = iota((cams, cams), 0) == iota((cams, cams), 1)

    def column(line):
        wide = jnp.broadcast_to(line, (cams, cams))
        return jnp.sum(jnp.where(eye, wide, jnp.zeros_like(wide)), axis=1, keepdims=True)

    def line(wide):
        return jnp.sum(jnp.where(eye, wide[:, :cams], 0.0), axis=0, keepdims=True)

    loads["obs_count"].wait()
    loads["obs_point"].wait()
    used_count = column(obs_count[...].astype(F32)).astype(I32)
    used = iota((cams, slots), 1) < used_count

    ids = obs_point[...]
    group_of[...] = jnp.where(used, lax.shift_right_logical(ids, 7) & (GROUP - 1), -1)
    lane_of[...] = (ids & (LANES - 1)) + jnp.where(ids < points, 0, LANES)

    columns = jnp.transpose(lane_of[...].astype(F32)).astype(I32)
    lane_numbers = [
        (iota((slots, LANES), 1) + part * LANES).astype(jnp.int16) for part in range(halves)
    ]
    tall_unit = jnp.ones((slots, LANES), BF16)
    tall_nil = jnp.zeros((slots, LANES), BF16)
    pair_rows = [
        (iota((2 * GROUP, slots), 0) + first).astype(jnp.int16)
        for first in range(0, WIDE, 2 * GROUP)
    ]
    unit = jnp.ones((2 * GROUP, slots), BF16)
    nil = jnp.zeros((2 * GROUP, slots), BF16)
    group_row = iota((GROUP, slots), 0)

    def scatter(source, count, cam):
        mask = group_row == group_of[cam : cam + 1]
        blocks = [
            jnp.where(mask, jnp.broadcast_to(source[index, cam : cam + 1], (GROUP, slots)), 0.0)
            for index in range(SPLITS * count)
        ]
        lanes = jnp.broadcast_to(lane_of[cam : cam + 1], (2 * GROUP, slots)).astype(jnp.int16)
        hot = jnp.concatenate(
            [jnp.where(row == lanes, unit, nil) for row in pair_rows], axis=0
        )
        return dot_nt(jnp.concatenate(blocks, axis=0).astype(BF16), hot)

    def first_scatter(cam):
        mask = group_row == group_of[cam : cam + 1]
        blocks = [
            jnp.where(
                mask, jnp.broadcast_to(first_terms[index, cam : cam + 1], (GROUP, slots)), 0.0
            )
            for index in range(SPLITS * 9)
        ]
        wide = jnp.broadcast_to(columns[:, cam : cam + 1], (slots, LANES)).astype(jnp.int16)
        hot = [jnp.where(lanes == wide, tall_unit, tall_nil) for lanes in lane_numbers]
        return jnp.dot(
            jnp.concatenate(blocks, axis=0).astype(BF16),
            jnp.concatenate(hot, axis=1),
            preferred_element_type=F32,
        )

    def joined(sums, index):
        whole = sums[(SPLITS * index + SPLITS - 1) * GROUP : (SPLITS * index + SPLITS) * GROUP]
        for step in reversed(range(SPLITS - 1)):
            first = (SPLITS * index + step) * GROUP
            whole = whole + sums[first : first + GROUP]
        return whole

    def neighbour(where, turn, size):
        spot = FIRST_ROWS[turn]
        if where == "next":
            return pltpu.make_async_remote_copy(
                src_ref=to_next.at[pl.ds(spot, size)],
                dst_ref=from_prev.at[pl.ds(spot, size)],
                send_sem=next_send.at[turn],
                recv_sem=next_recv.at[turn],
                device_id=(lax.rem(me + 1, n),),
                device_id_type=MESH,
            )
        return pltpu.make_async_remote_copy(
            src_ref=to_prev.at[pl.ds(spot, size)],
            dst_ref=from_next.at[pl.ds(spot, size)],
            send_sem=prev_send.at[turn],
            recv_sem=prev_recv.at[turn],
            device_id=(lax.rem(me + n - 1, n),),
            device_id_type=MESH,
        )

    row_of = iota((GROUP, LANES), 0)
    low_row = row_of < edge

    def looked_up(tile, rows, tile_row, tile_lane, start):
        for row in range(rows):
            wide = jnp.broadcast_to(tile[row : row + 1], tile_lane.shape)
            found = jnp.take_along_axis(wide, tile_lane, axis=1, mode="promise_in_bounds")
            start = jnp.where(tile_row == row, found, start)
        return start

    def start_pair(turn, size):
        @pl.when(has_next)
        def _():
            neighbour("next", turn, size).start()

        @pl.when(has_prev)
        def _():
            neighbour("prev", turn, size).start()

    def send(sums, turn):
        spot = FIRST_ROWS[turn]
        for index, member in enumerate(sums):
            to_next[spot + index] = member[:, :LANES]
            to_prev[spot + index] = member[:, LANES:]
        start_pair(turn, len(sums))

    edge_row = iota((GROUP, LANES), 0) < 2 * edge

    def receive(sums, turn):
        spot = FIRST_ROWS[turn]
        @pl.when(has_next)
        def _():
            copy = neighbour("next", turn, len(sums))
            copy.wait_send()
            neighbour("prev", turn, len(sums)).wait_recv()

        @pl.when(has_prev)
        def _():
            copy = neighbour("prev", turn, len(sums))
            copy.wait_send()
            neighbour("next", turn, len(sums)).wait_recv()

        return [
            jnp.concatenate(
                [
                    member[:, :LANES] + jnp.where(edge_row, from_next[spot + index], 0.0),
                    member[:, LANES:] + jnp.where(edge_row, from_prev[spot + index], 0.0),
                ],
                axis=1,
            )
            for index, member in enumerate(sums)
        ]

    def pjac(index):
        return point_jac[index].astype(F32)

    def spread_out(col):
        return jnp.broadcast_to(col, (cams, LANES))

    def point_product(vector):
        for entry in range(9):
            vector_rows[entry] = vector[entry]
        running = [[None] * halves for index in range(3)]
        for cam in range(cams):
            for entry in range(9):
                scale = jnp.broadcast_to(vector_rows[entry, cam : cam + 1], (GROUP, LANES))
                for index in range(3):
                    for part in range(halves):
                        block = coupling[
                            cam * 27 + index * 9 + entry, :, part * LANES : (part + 1) * LANES
                        ]
                        term = block * scale
                        before = running[index][part]
                        running[index][part] = term if before is None else before + term
        return [jnp.concatenate(parts, axis=1) for parts in running]

    def camera_product(values):
        for cam in range(cams):
            for entry in range(9):
                whole = None
                for index in range(3):
                    for part in range(halves):
                        lanes = slice(part * LANES, (part + 1) * LANES)
                        term = coupling[cam * 27 + index * 9 + entry, :, lanes] * values[index][:, lanes]
                        whole = term if whole is None else whole + term
                partial[entry, cam * GROUP : (cam + 1) * GROUP] = whole
        result = []
        for entry in range(9):
            whole = partial[entry, pl.ds(0, cams, stride=GROUP)]
            for row in range(1, GROUP):
                whole = whole + partial[entry, pl.ds(row, cams, stride=GROUP)]
            result.append(spread_out(jnp.sum(whole, axis=1, keepdims=True)))
        return result

    def square_product(vector):
        result = [None] * 9
        for index, (lead, tail) in enumerate(SQUARES):
            block = squares[index]
            for here, there in {(lead, tail), (tail, lead)}:
                term = block * vector[there]
                result[here] = term if result[here] is None else result[here] + term
        return result

    def dot_of(left, right):
        running = left[0] * right[0]
        for entry in range(1, 9):
            running = running + left[entry] * right[entry]
        return jnp.sum(running, axis=0, keepdims=True)

    dot_lane = iota((1, LANES), 1)
    part_row = iota((GROUP, WIDE), 0)
    part_left = iota((GROUP, WIDE), 1) < LANES
    own_row = jnp.where(part_left, part_row, part_row - edge)
    is_own = jnp.where(part_left, edge - 1 - own_row, own_row) >= 0
    is_own = is_own | (part_row >= 2 * edge)

    def point_dot(left, right):
        running = left[0] * right[0]
        for index in range(1, 3):
            running = running + left[index] * right[index]
        running = jnp.where(is_own, running, 0.0)
        running = running[:, :LANES] + running[:, LANES:]
        running = jnp.sum(running, axis=0, keepdims=True)
        return jnp.broadcast_to(jnp.sum(running, axis=1, keepdims=True), (1, LANES))

    def dots_copy(offset):
        return pltpu.make_async_remote_copy(
            src_ref=dots_out,
            dst_ref=dots_in.at[offset - 1],
            send_sem=dots_send,
            recv_sem=dots_recv,
            device_id=(lax.rem(me + offset, n),),
            device_id_type=MESH,
        )

    def start_dots(offset, carry):
        dots_copy(offset).start()
        return carry

    for name in LOAD_ORDER[2:]:
        loads[name].wait()
    start_col = [column(start_guess[entry : entry + 1]) for entry in range(9)]
    listed = [back_list, front_list]
    listed = [
        member[:, part * LANES : (part + 1) * LANES] for member in listed for part in range(edge)
    ]
    listed = jnp.concatenate(
        listed + [jnp.full((GROUP - 2 * edge, LANES), -1, I32)], axis=0
    )
    list_row = lax.shift_right_arithmetic(listed, 7)
    list_lane = listed & (LANES - 1)

    errors = []
    for side in range(2):
        running = cam_jac[9 * side].astype(F32) * start_col[0]
        for entry in range(1, 9):
            running = running + cam_jac[9 * side + entry].astype(F32) * start_col[entry]
        errors.append(running)
    blocks = [
        pjac(lead) * pjac(tail) + pjac(3 + lead) * pjac(3 + tail) for lead, tail in ENTRY_PAIRS
    ]
    blocks = blocks + [
        errors[0] * pjac(entry) + errors[1] * pjac(3 + entry) for entry in range(3)
    ]
    for index, block in enumerate(blocks):
        for step, term in enumerate(splits_of(block)):
            first_terms[SPLITS * index + step] = term
    chains = [None, None]
    for cam in range(cams):
        tall = cam % 2 == 0 or cam % 8 == 3
        part = first_scatter(cam) if tall else scatter(first_terms, 9, cam)
        before = chains[0 if tall else 1]
        chains[0 if tall else 1] = part if before is None else before + part
    for index in range(9):
        coupling[index] = joined(chains[0], index)
    whole = chains[1]
    sums = [joined(whole, index) + coupling[index] for index in range(9)]

    moved = [point_damp[:, part * LANES : (part + 1) * LANES] for part in range(GROUP)]
    moved = jnp.concatenate(moved, axis=0)
    tiles = []
    for index, (member, pair) in enumerate(zip(sums, ENTRY_PAIRS + ((0, 1),) * 3)):
        own, side = member[:, :LANES], member[:, LANES:]
        if pair[0] == pair[1]:
            own = own + moved
        chosen = looked_up(own, GROUP, list_row, list_lane, jnp.zeros((GROUP, LANES), F32))
        tiles.append(
            (own, jnp.where(low_row, chosen, side), jnp.where(low_row, side, chosen))
        )
        to_next[index], to_prev[index] = tiles[-1][1], tiles[-1][2]

    pl.semaphore_wait(barrier, len(reaches) + jnp.where(has_prev, 1, 0))
    tell(0)
    start_pair(0, 9)

    for index in range(18):
        wide_jac[index] = jnp.where(used, cam_jac[index].astype(F32), 0.0)
    damp = column(cam_damp[...])
    right = [spread_out(column(right_side[entry : entry + 1])) for entry in range(9)]
    start = [spread_out(member) for member in start_col]

    flat = jnp.concatenate([back_list[...], front_list[...]], axis=1)
    place = iota((1, 2 * border), 1)
    code_row = iota((2 * GROUP, 2 * border), 0)
    code = jnp.where(
        code_row < GROUP, lax.shift_right_logical(place, 7) + 1, place & (LANES - 1)
    )
    code = jnp.where(lax.shift_right_logical(flat, 7) == (code_row & (GROUP - 1)), code, 0)
    hot = jnp.where(iota((LANES, 2 * border), 0) == (flat & (LANES - 1)), 1.0, 0.0).astype(BF16)
    table = dot_nt(code.astype(F32).astype(BF16), hot).astype(I32)
    place_row = table[:GROUP] - 1
    place_lane = table[GROUP:]
    other = place_row < 0
    count = jnp.where(other, 1.0, 0.0)
    before = jnp.where(iota((LANES, LANES), 0) < iota((LANES, LANES), 1), 1.0, 0.0).astype(BF16)
    double = jnp.concatenate([count, jnp.zeros((GROUP, LANES), F32)], axis=0).astype(BF16)
    rank = jnp.dot(double, before, preferred_element_type=F32)[:GROUP]
    total = jnp.sum(count, axis=1, keepdims=True)
    for row in range(GROUP - 1):
        rank = rank + jnp.where(row_of > row, total[row : row + 1], 0.0)
    rank = rank.astype(I32)
    code_table = jnp.where(
        other,
        2 * edge * WIDE + rank,
        place_row * WIDE + place_lane + jnp.where(place_row < edge, 0, LANES),
    )
    aim = jnp.where(other, rank, -1)
    slot_row = iota((WIDE, LANES), 0)
    hot = [jnp.where(slot_row == aim[row : row + 1], 1.0, 0.0) for row in range(GROUP)]
    hot = jnp.concatenate(hot, axis=1).astype(BF16)
    code_row = iota((2 * GROUP, points), 0)
    place = iota((2 * GROUP, points), 1)
    code = jnp.where(
        code_row < GROUP, lax.shift_right_logical(place, 7) + 1, place & (LANES - 1)
    )
    table = dot_nt(code.astype(F32).astype(BF16), hot).astype(I32)

    def in_place(line):
        return jnp.where(
            row_of == 2 * edge,
            jnp.broadcast_to(line[:, :LANES], (GROUP, LANES)),
            jnp.broadcast_to(line[:, LANES:], (GROUP, LANES)),
        )

    rest_row = jnp.where(row_of < 2 * edge, -1, in_place(table[:1] - 1))
    rest_lane = jnp.where(row_of < 2 * edge, 0, in_place(table[GROUP : GROUP + 1]))
    sums = []
    for own, left, right_half in tiles:
        rest = looked_up(own, GROUP, rest_row, rest_lane, jnp.zeros((GROUP, LANES), F32))
        left = left + jnp.where(row_of == 2 * edge, rest, 0.0)
        moved = pltpu.roll(rest, GROUP - 1, 0)
        right_half = right_half + jnp.where(row_of == 2 * edge, moved, 0.0)
        sums.append(jnp.concatenate([left, right_half], axis=1))

    for top in range(0, cams, GROUP):
        for left in range(0, slots, LANES):
            spot = (slice(top, top + GROUP), slice(left, left + LANES))
            ids = obs_point[spot]
            back_slot = ids - points
            front_slot = back_slot - border
            in_back = ids < points + border
            side = jnp.where(
                in_back,
                lax.shift_right_logical(back_slot, 7) * WIDE + LANES + (back_slot & (LANES - 1)),
                (edge + lax.shift_right_logical(front_slot, 7)) * WIDE + (front_slot & (LANES - 1)),
            )
            id_row = lax.shift_right_logical(ids, 7)
            side = looked_up(code_table, GROUP, id_row, ids & (LANES - 1), side)
            group_of[spot] = jnp.where(used[spot], lax.shift_right_logical(side, 8), -1)
            lane_of[spot] = side & (WIDE - 1)

    for top in range(0, cams, GROUP):
        for left in range(0, slots, LANES):
            spot = (slice(top, top + GROUP), slice(left, left + LANES))
            camera = [wide_jac[(index, *spot)] for index in range(18)]
            for index in range(3):
                one = point_jac[(index, slice(None), spot[1])].astype(F32)[spot[0]]
                two = point_jac[(3 + index, slice(None), spot[1])].astype(F32)[spot[0]]
                for entry in range(9):
                    product = one * camera[entry] + two * camera[9 + entry]
                    for step, term in enumerate(splits_of(product)):
                        terms[(SPLITS * (index * 9 + entry) + step, *spot)] = term
    for cam in range(cams):
        whole = scatter(terms, 27, cam)
        for index in range(27):
            coupling[cam * 27 + index] = joined(whole, index)

    precond = []
    for index, (lead, tail) in enumerate(SQUARES):
        running = None
        for left in range(0, slots, LANES):
            lanes = slice(left, left + LANES)
            term = (
                wide_jac[lead, :, lanes] * wide_jac[tail, :, lanes]
                + wide_jac[9 + lead, :, lanes] * wide_jac[9 + tail, :, lanes]
            )
            running = term if running is None else running + term
        total = jnp.sum(running, axis=1, keepdims=True)
        if lead == tail:
            total = total + damp
            precond.append(spread_out(1.0 / total))
        squares[index] = spread_out(total)
    image = square_product(start)

    hear(0)
    sums = receive(sums, 0)
    inverse = symmetric_inverse(sums[:6])
    back = camera_product(apply_inverse(inverse, sums[6:]))
    residual = [right[entry] - (image[entry] - back[entry]) for entry in range(9)]
    direction = [precond[entry] * residual[entry] for entry in range(9)]

    sums = point_product(direction)
    send(sums, 1)
    hear(1)
    square_direction = square_product(direction)
    hear(2)
    sums = receive(sums, 1)
    values = apply_inverse(inverse, sums)
    back = camera_product(values)
    image = [square_direction[entry] - back[entry] for entry in range(9)]
    ahead = [precond[entry] * image[entry] for entry in range(9)]

    sums_ahead = point_product(ahead)
    send(sums_ahead, 2)
    hear(3)
    square_ahead = square_product(ahead)
    inner = dot_of(residual, direction)
    curve = dot_of(direction, image)
    weight = dot_of(image, ahead)
    shift = dot_of(residual, ahead) / jnp.where(weight > 0.0, weight, 1.0)
    shift = jnp.clip(shift, -1e6, 1e6)
    rest = [direction[entry] - shift * ahead[entry] for entry in range(9)]
    left_over = [residual[entry] - shift * image[entry] for entry in range(9)]
    square_rest = [square_direction[entry] - shift * square_ahead[entry] for entry in range(9)]
    members = [
        inner,
        curve,
        dot_of(left_over, rest),
        dot_of(rest, square_rest),
        dot_of(rest, image),
        2.0 * dot_of(left_over, ahead),
        2.0 * dot_of(rest, square_ahead),
        weight,
        weight,
        dot_of(ahead, square_ahead),
    ]
    packed = jnp.zeros((1, LANES), F32)
    for index, member in enumerate(members):
        packed = jnp.where(dot_lane == index, member, packed)
    dots_out[1] = shift
    for turn in range(4, len(reaches)):
        hear(turn)
    sums_ahead = receive(sums_ahead, 2)
    values_ahead = apply_inverse(inverse, sums_ahead)
    wide_shift = jnp.concatenate([shift] * halves, axis=1)
    sums_rest = [sums[index] - wide_shift * sums_ahead[index] for index in range(3)]
    values_rest = [values[index] - wide_shift * values_ahead[index] for index in range(3)]
    packed = packed - jnp.where(dot_lane == 3, point_dot(sums_rest, values_rest), 0.0)
    packed = packed - jnp.where(dot_lane == 6, 2.0 * point_dot(sums_rest, values_ahead), 0.0)
    packed = packed - jnp.where(dot_lane == 9, point_dot(sums_ahead, values_ahead), 0.0)
    dots_out[0] = packed
    lax.fori_loop(1, n, start_dots, 0)

    back = camera_product(values_ahead)
    further = [square_ahead[entry] - back[entry] for entry in range(9)]

    pltpu.make_async_copy(dots_in, dots_in, dots_recv).wait()
    pltpu.make_async_copy(dots_in, dots_in, dots_send).wait()

    def picked(row, low, high):
        inside = (dot_lane >= low) & (dot_lane < high)
        return jnp.sum(jnp.where(inside, row, 0.0), axis=1, keepdims=True)

    whole = packed + jnp.sum(dots_in[:, 0], axis=0)
    inner = picked(whole, 0, 1)
    curve = picked(whole, 1, 2)
    step = inner / curve

    def moved_by(row, about):
        gap = about - step
        row = jnp.where(dot_lane >= 5, row * gap, row)
        return jnp.where(dot_lane >= 8, row * gap, row)

    whole = moved_by(packed, shift)
    for offset in range(1, n):
        whole = whole + moved_by(dots_in[offset - 1, 0], dots_in[offset - 1, 1])
    one = (dot_lane == 2) | (dot_lane == 5) | (dot_lane == 8)
    two = (dot_lane == 3) | (dot_lane == 6) | (dot_lane == 9)
    three = (dot_lane == 4) | (dot_lane == 7)
    inner_next = jnp.sum(jnp.where(one, whole, 0.0), axis=1, keepdims=True)
    own_curve = jnp.sum(jnp.where(two, whole, 0.0), axis=1, keepdims=True)
    cross = jnp.sum(jnp.where(three, whole, 0.0), axis=1, keepdims=True)
    ratio = inner_next / inner
    curve = own_curve + ratio * (2.0 * cross + ratio * curve)
    second = inner_next / curve
    for entry in range(9):
        scaled = direction[entry] - step * ahead[entry]
        fresh = scaled + ratio * direction[entry]
        seen = image[entry] - step * further[entry] + ratio * image[entry]
        solved = start[entry] + step * direction[entry] + second * fresh
        left = residual[entry] - step * image[entry] - second * seen
        packed_out[entry : entry + 1] = line(solved)
        packed_out[16 + entry : 17 + entry] = line(left)


def solution(mesh):
    n = mesh.shape["seg"]

    def shards(
        cam_jac,
        point_jac,
        obs_point,
        obs_count,
        back_list,
        front_list,
        point_damp,
        cam_damp,
        right_side,
        start_guess,
    ):
        cams, slots = obs_point.shape
        operands = (
            cam_jac,
            point_jac,
            obs_point,
            obs_count.reshape(1, -1),
            back_list,
            front_list,
            point_damp.reshape(1, -1),
            cam_damp.reshape(1, -1),
            right_side,
            start_guess,
        )
        vector = jax.ShapeDtypeStruct(right_side.shape, F32)
        found = pl.pallas_call(
            functools.partial(kernel, n),
            out_shape=pltpu.VMEM((32, right_side.shape[1]), F32),
            in_specs=[pl.BlockSpec(memory_space=pltpu.HBM)] * 10,
            out_specs=pl.BlockSpec(memory_space=pltpu.VMEM),
            scratch_shapes=[
                pltpu.VMEM((cams, slots), I32),
                pltpu.VMEM((cams, slots), I32),
                pltpu.VMEM((18, cams, slots), F32),
                pltpu.VMEM((SPLITS * 9, cams, slots), F32),
                pltpu.VMEM((SPLITS * 27, cams, slots), F32),
                pltpu.VMEM((cams * 27, GROUP, WIDE), F32),
                pltpu.VMEM((9, cams * GROUP, LANES), F32),
                pltpu.VMEM((9, cams, LANES), F32),
                pltpu.VMEM((len(SQUARES), cams, LANES), F32),
                pltpu.VMEM((15, GROUP, LANES), F32),
                pltpu.VMEM((15, GROUP, LANES), F32),
                pltpu.VMEM((15, GROUP, LANES), F32),
                pltpu.VMEM((15, GROUP, LANES), F32),
                pltpu.VMEM((2, 1, LANES), F32),
                pltpu.VMEM((n - 1, 2, 1, LANES), F32),
                pltpu.SemaphoreType.DMA((3,)),
                pltpu.SemaphoreType.DMA((3,)),
                pltpu.SemaphoreType.DMA((3,)),
                pltpu.SemaphoreType.DMA((3,)),
                pltpu.SemaphoreType.DMA,
                pltpu.SemaphoreType.DMA,
                pltpu.SemaphoreType.REGULAR((max(1, (n - 1).bit_length()),)),
                *[pltpu.VMEM(member.shape, member.dtype) for member in operands],
                pltpu.SemaphoreType.DMA((len(operands),)),
            ],
            compiler_params=pltpu.CompilerParams(
                collective_id=0, has_side_effects=True, vmem_limit_bytes=56 * 1024 * 1024
            ),
            name="schur_cg",
        )(*operands)
        return found[:9], found[16:25]

    return jax.shard_map(
        shards,
        mesh=mesh,
        in_specs=(
            P(None, "seg", None),
            P(None, "seg", None),
            P("seg", None),
            P("seg"),
            P("seg", None),
            P("seg", None),
            P("seg"),
            P("seg"),
            P(None, "seg"),
            P(None, "seg"),
        ),
        out_specs=(P(None, "seg"), P(None, "seg")),
        check_vma=False,
    )
```

```python
import functools

import jax
import jax.numpy as jnp
from jax import lax
from jax.experimental import pallas as pl
from jax.experimental.pallas import tpu as pltpu
from jax.sharding import PartitionSpec as P

ENTRY_PAIRS = ((0, 0), (0, 1), (0, 2), (1, 1), (1, 2), (2, 2))
F32, BF16, I32 = jnp.float32, jnp.bfloat16, jnp.int32
MESH = pl.DeviceIdType.MESH
LANES = 128
WIDE = 256
GROUP = 8
SPLITS = 2
SIZES = (9, 3, 3)
SQUARES = tuple((lead, tail) for lead in range(9) for tail in range(lead, 9))
LOAD_ORDER = (
    "obs_count",
    "obs_point",
    "start_guess",
    "point_jac",
    "cam_jac",
    "back_list",
    "front_list",
    "point_damp",
    "cam_damp",
    "right_side",
)


def splits_of(value):
    terms = []
    for step in range(SPLITS):
        term = value.astype(BF16).astype(F32)
        terms.append(term)
        value = value - term
    return terms


def iota(shape, dim):
    return lax.broadcasted_iota(I32, shape, dim)


def dot_nt(left, right):
    return lax.dot_general(left, right, (((1,), (1,)), ((), ())), preferred_element_type=F32)


def symmetric_inverse(entries):
    cofactors = [
        entries[3] * entries[5] - entries[4] * entries[4],
        entries[2] * entries[4] - entries[1] * entries[5],
        entries[1] * entries[4] - entries[2] * entries[3],
        entries[0] * entries[5] - entries[2] * entries[2],
        entries[1] * entries[2] - entries[0] * entries[4],
        entries[0] * entries[3] - entries[1] * entries[1],
    ]
    determinant = entries[0] * cofactors[0] + entries[1] * cofactors[1] + entries[2] * cofactors[2]
    determinant = jnp.where(determinant > 0.0, determinant, 1.0)
    return [member / determinant for member in cofactors]


def apply_inverse(inverse, sums):
    return [
        inverse[0] * sums[0] + inverse[1] * sums[1] + inverse[2] * sums[2],
        inverse[1] * sums[0] + inverse[3] * sums[1] + inverse[4] * sums[2],
        inverse[2] * sums[0] + inverse[4] * sums[1] + inverse[5] * sums[2],
    ]


def kernel(
    n,
    cam_jac_hbm,
    point_jac_hbm,
    obs_point_hbm,
    obs_count_hbm,
    back_list_hbm,
    front_list_hbm,
    point_damp_hbm,
    cam_damp_hbm,
    right_side_hbm,
    start_guess_hbm,
    packed_out,
    group_of,
    lane_of,
    wide_jac,
    first_terms,
    terms,
    coupling,
    partial,
    vector_rows,
    squares,
    to_next,
    to_prev,
    from_prev,
    from_next,
    dots_out,
    dots_in,
    next_send,
    next_recv,
    prev_send,
    prev_recv,
    dots_send,
    dots_recv,
    told,
    cam_jac,
    point_jac,
    obs_point,
    obs_count,
    back_list,
    front_list,
    point_damp,
    cam_damp,
    right_side,
    start_guess,
    load_sem,
):
    cams, slots = obs_point.shape
    points = point_damp.shape[1]
    border = back_list.shape[1]
    edge = border // LANES
    halves = WIDE // LANES
    me = lax.axis_index("seg")

    loads = {
        "cam_jac": pltpu.make_async_copy(cam_jac_hbm, cam_jac, load_sem.at[0]),
        "point_jac": pltpu.make_async_copy(point_jac_hbm, point_jac, load_sem.at[1]),
        "obs_point": pltpu.make_async_copy(obs_point_hbm, obs_point, load_sem.at[2]),
        "obs_count": pltpu.make_async_copy(obs_count_hbm, obs_count, load_sem.at[3]),
        "back_list": pltpu.make_async_copy(back_list_hbm, back_list, load_sem.at[4]),
        "front_list": pltpu.make_async_copy(front_list_hbm, front_list, load_sem.at[5]),
        "point_damp": pltpu.make_async_copy(point_damp_hbm, point_damp, load_sem.at[6]),
        "cam_damp": pltpu.make_async_copy(cam_damp_hbm, cam_damp, load_sem.at[7]),
        "right_side": pltpu.make_async_copy(right_side_hbm, right_side, load_sem.at[8]),
        "start_guess": pltpu.make_async_copy(start_guess_hbm, start_guess, load_sem.at[9]),
    }
    for name in LOAD_ORDER:
        loads[name].start()

    barrier = pltpu.get_barrier_semaphore()

    kept = 2 * edge
    heights = (kept, GROUP, GROUP)
    lengths = [-(-count * height // GROUP) * GROUP for count, height in zip(SIZES, heights)]
    spots = [sum(lengths[:turn]) for turn in range(3)]

    for landing in (from_prev, from_next):
        landing[...] = jnp.zeros_like(landing)
    for leaving in (to_next, to_prev):
        leaving[lengths[0] - GROUP : lengths[0]] = jnp.zeros((GROUP, LANES), F32)

    reaches = []
    while 2 ** len(reaches) < n:
        reaches.insert(0, 2 ** len(reaches))
    has_next = me < n - 1
    has_prev = me > 0
    for reach in reaches:
        pl.semaphore_signal(
            barrier, inc=1, device_id=(lax.rem(me + n - reach, n),), device_id_type=MESH
        )

    @pl.when(has_next)
    def _():
        pl.semaphore_signal(barrier, inc=1, device_id=(me + 1,), device_id_type=MESH)

    def tell(turn):
        pl.semaphore_signal(
            told.at[turn],
            inc=1,
            device_id=(lax.rem(me + reaches[turn], n),),
            device_id_type=MESH,
        )

    def hear(turn):
        pl.semaphore_wait(told.at[turn], 1)
        if turn + 1 < len(reaches):
            tell(turn + 1)


    eye = iota((cams, cams), 0) == iota((cams, cams), 1)

    def column(line):
        wide = jnp.broadcast_to(line, (cams, cams))
        return jnp.sum(jnp.where(eye, wide, jnp.zeros_like(wide)), axis=1, keepdims=True)

    def line(wide):
        return jnp.sum(jnp.where(eye, wide[:, :cams], 0.0), axis=0, keepdims=True)

    loads["obs_count"].wait()
    loads["obs_point"].wait()
    loads["start_guess"].wait()
    start_col = [column(start_guess[entry : entry + 1]) for entry in range(9)]
    used_count = column(obs_count[...].astype(F32)).astype(I32)
    used = iota((cams, slots), 1) < used_count

    ids = obs_point[...]
    group_of[...] = jnp.where(used, lax.shift_right_logical(ids, 7) & (GROUP - 1), -1)
    lane_of[...] = (ids & (LANES - 1)) + jnp.where(ids < points, 0, LANES)

    columns = jnp.transpose(lane_of[...].astype(F32)).astype(I32)
    lane_numbers = [
        (iota((slots, LANES), 1) + part * LANES).astype(jnp.int16) for part in range(halves)
    ]
    tall_unit = jnp.ones((slots, LANES), BF16)
    tall_nil = jnp.zeros((slots, LANES), BF16)
    pair_rows = [
        (iota((2 * GROUP, slots), 0) + first).astype(jnp.int16)
        for first in range(0, WIDE, 2 * GROUP)
    ]
    unit = jnp.ones((2 * GROUP, slots), BF16)
    nil = jnp.zeros((2 * GROUP, slots), BF16)
    group_row = iota((GROUP, slots), 0)

    def scatter(source, count, cam):
        mask = group_row == group_of[cam : cam + 1]
        blocks = [
            jnp.where(mask, jnp.broadcast_to(source[index, cam : cam + 1], (GROUP, slots)), 0.0)
            for index in range(SPLITS * count)
        ]
        lanes = jnp.broadcast_to(lane_of[cam : cam + 1], (2 * GROUP, slots)).astype(jnp.int16)
        hot = jnp.concatenate(
            [jnp.where(row == lanes, unit, nil) for row in pair_rows], axis=0
        )
        return dot_nt(jnp.concatenate(blocks, axis=0).astype(BF16), hot)

    def first_scatter(cam):
        mask = group_row == group_of[cam : cam + 1]
        blocks = [
            jnp.where(
                mask, jnp.broadcast_to(first_terms[index, cam : cam + 1], (GROUP, slots)), 0.0
            )
            for index in range(SPLITS * 9)
        ]
        wide = jnp.broadcast_to(columns[:, cam : cam + 1], (slots, LANES)).astype(jnp.int16)
        hot = [jnp.where(lanes == wide, tall_unit, tall_nil) for lanes in lane_numbers]
        return jnp.dot(
            jnp.concatenate(blocks, axis=0).astype(BF16),
            jnp.concatenate(hot, axis=1),
            preferred_element_type=F32,
        )

    def joined(sums, index):
        whole = sums[(SPLITS * index + SPLITS - 1) * GROUP : (SPLITS * index + SPLITS) * GROUP]
        for step in reversed(range(SPLITS - 1)):
            first = (SPLITS * index + step) * GROUP
            whole = whole + sums[first : first + GROUP]
        return whole

    def neighbour(where, turn):
        spot, size = spots[turn], lengths[turn]
        if where == "next":
            return pltpu.make_async_remote_copy(
                src_ref=to_next.at[pl.ds(spot, size)],
                dst_ref=from_prev.at[pl.ds(spot, size)],
                send_sem=next_send.at[turn],
                recv_sem=next_recv.at[turn],
                device_id=(lax.rem(me + 1, n),),
                device_id_type=MESH,
            )
        return pltpu.make_async_remote_copy(
            src_ref=to_prev.at[pl.ds(spot, size)],
            dst_ref=from_next.at[pl.ds(spot, size)],
            send_sem=prev_send.at[turn],
            recv_sem=prev_recv.at[turn],
            device_id=(lax.rem(me + n - 1, n),),
            device_id_type=MESH,
        )

    row_of = iota((GROUP, LANES), 0)
    low_row = row_of < edge

    def looked_up(tile, rows, tile_row, tile_lane, start):
        for row in range(rows):
            wide = jnp.broadcast_to(tile[row : row + 1], tile_lane.shape)
            found = jnp.take_along_axis(wide, tile_lane, axis=1, mode="promise_in_bounds")
            start = jnp.where(tile_row == row, found, start)
        return start

    def start_pair(turn):
        @pl.when(has_next)
        def _():
            neighbour("next", turn).start()

        @pl.when(has_prev)
        def _():
            neighbour("prev", turn).start()

    def send(sums, turn):
        for index, member in enumerate(sums):
            spot = spots[turn] + index * GROUP
            to_next[spot : spot + GROUP] = member[:, :LANES]
            to_prev[spot : spot + GROUP] = member[:, LANES:]
        start_pair(turn)

    edge_row = iota((GROUP, LANES), 0) < 2 * edge

    def receive(sums, turn):
        @pl.when(has_next)
        def _():
            copy = neighbour("next", turn)
            copy.wait_send()
            neighbour("prev", turn).wait_recv()

        @pl.when(has_prev)
        def _():
            copy = neighbour("prev", turn)
            copy.wait_send()
            neighbour("next", turn).wait_recv()

        whole = []
        for index, member in enumerate(sums):
            spot = spots[turn] + index * heights[turn]
            rows = slice(spot, spot + GROUP)
            left = member[:, :LANES] + jnp.where(edge_row, from_next[rows], 0.0)
            below = member[:, LANES:] + jnp.where(edge_row, from_prev[rows], 0.0)
            whole.append(jnp.concatenate([left, below], axis=1))
        return whole

    def pjac(index):
        return point_jac[index].astype(F32)

    def spread_out(col):
        return jnp.broadcast_to(col, (cams, LANES))

    def point_terms(running, entry, vector):
        vector_rows[entry] = vector
        for cam in range(cams):
            scale = jnp.broadcast_to(vector_rows[entry, cam : cam + 1], (GROUP, LANES))
            for index in range(3):
                for part in range(halves):
                    block = coupling[
                        cam * 27 + index * 9 + entry, :, part * LANES : (part + 1) * LANES
                    ]
                    term = block * scale
                    before = running[index][part]
                    running[index][part] = term if before is None else before + term

    def camera_entry(values, entry):
        for cam in range(cams):
            whole = None
            for index in range(3):
                for part in range(halves):
                    lanes = slice(part * LANES, (part + 1) * LANES)
                    term = coupling[cam * 27 + index * 9 + entry, :, lanes] * values[index][:, lanes]
                    whole = term if whole is None else whole + term
            partial[entry, cam * GROUP : (cam + 1) * GROUP] = whole
        whole = partial[entry, pl.ds(0, cams, stride=GROUP)]
        for row in range(1, GROUP):
            whole = whole + partial[entry, pl.ds(row, cams, stride=GROUP)]
        return spread_out(jnp.sum(whole, axis=1, keepdims=True))

    def there_and_back(values, use):
        running = [[None] * halves for index in range(3)]
        for entry in range(9):
            point_terms(running, entry, use(entry, camera_entry(values, entry)))
        return [jnp.concatenate(parts, axis=1) for parts in running]

    def square_product(vector):
        result = [None] * 9
        for index, (lead, tail) in enumerate(SQUARES):
            block = squares[index]
            for here, there in {(lead, tail), (tail, lead)}:
                term = block * vector[there]
                result[here] = term if result[here] is None else result[here] + term
        return result

    def dot_of(left, right):
        running = left[0] * right[0]
        for entry in range(1, 9):
            running = running + left[entry] * right[entry]
        return jnp.sum(running, axis=0, keepdims=True)

    dot_lane = iota((1, LANES), 1)
    part_row = iota((GROUP, WIDE), 0)
    part_left = iota((GROUP, WIDE), 1) < LANES
    own_row = jnp.where(part_left, part_row, part_row - edge)
    is_own = jnp.where(part_left, edge - 1 - own_row, own_row) >= 0
    is_own = is_own | (part_row >= 2 * edge)

    def point_dot(left, right):
        running = left[0] * right[0]
        for index in range(1, 3):
            running = running + left[index] * right[index]
        running = jnp.where(is_own, running, 0.0)
        running = running[:, :LANES] + running[:, LANES:]
        running = jnp.sum(running, axis=0, keepdims=True)
        return jnp.broadcast_to(jnp.sum(running, axis=1, keepdims=True), (1, LANES))

    def dots_copy(offset):
        return pltpu.make_async_remote_copy(
            src_ref=dots_out,
            dst_ref=dots_in.at[offset - 1],
            send_sem=dots_send,
            recv_sem=dots_recv,
            device_id=(lax.rem(me + offset, n),),
            device_id_type=MESH,
        )

    def start_dots(offset, carry):
        dots_copy(offset).start()
        return carry

    for name in LOAD_ORDER[3:]:
        loads[name].wait()
    listed = [back_list, front_list]
    listed = [
        member[:, part * LANES : (part + 1) * LANES] for member in listed for part in range(edge)
    ]
    listed = jnp.concatenate(
        listed + [jnp.full((GROUP - 2 * edge, LANES), -1, I32)], axis=0
    )
    list_row = lax.shift_right_arithmetic(listed, 7)
    list_lane = listed & (LANES - 1)

    chains = [None, None]
    for top in range(0, cams, GROUP):
        near = slice(top, top + GROUP)

        def upper(ref, index):
            return ref[index].astype(F32)[near]

        errors = []
        for side in range(2):
            running = upper(cam_jac, 9 * side) * start_col[0][near]
            for entry in range(1, 9):
                running = running + upper(cam_jac, 9 * side + entry) * start_col[entry][near]
            errors.append(running)
        ours = [upper(point_jac, index) for index in range(6)]
        blocks = [ours[lead] * ours[tail] + ours[3 + lead] * ours[3 + tail] for lead, tail in ENTRY_PAIRS]
        blocks = blocks + [
            errors[0] * ours[entry] + errors[1] * ours[3 + entry] for entry in range(3)
        ]
        for index, block in enumerate(blocks):
            for step, term in enumerate(splits_of(block)):
                first_terms[SPLITS * index + step, near] = term
        for cam in range(top, top + GROUP):
            side = 0 if cam % 2 == 0 or cam % 8 == 3 else 1
            if side == 0 and cam not in (0, 2):
                part = first_scatter(cam)
            else:
                part = scatter(first_terms, 9, cam)
            before = chains[side]
            chains[side] = part if before is None else before + part
    for index in range(9):
        coupling[index] = joined(chains[0], index)
    whole = chains[1]
    sums = [joined(whole, index) + coupling[index] for index in range(9)]

    moved = [point_damp[:, part * LANES : (part + 1) * LANES] for part in range(GROUP)]
    moved = jnp.concatenate(moved, axis=0)
    tiles = []
    for index, (member, pair) in enumerate(zip(sums, ENTRY_PAIRS + ((0, 1),) * 3)):
        own, side = member[:, :LANES], member[:, LANES:]
        if pair[0] == pair[1]:
            own = own + moved
        chosen = looked_up(own, GROUP, list_row, list_lane, jnp.zeros((GROUP, LANES), F32))
        tiles.append(
            (own, jnp.where(low_row, chosen, side), jnp.where(low_row, side, chosen))
        )
        rows = slice(index * kept, (index + 1) * kept)
        to_next[rows], to_prev[rows] = tiles[-1][1][:kept], tiles[-1][2][:kept]

    pl.semaphore_wait(barrier, len(reaches) + jnp.where(has_prev, 1, 0))
    tell(0)
    start_pair(0)

    for index in range(18):
        wide_jac[index] = jnp.where(used, cam_jac[index].astype(F32), 0.0)
    damp = column(cam_damp[...])
    right = [spread_out(column(right_side[entry : entry + 1])) for entry in range(9)]
    start = [spread_out(member) for member in start_col]

    flat = jnp.concatenate([back_list[...], front_list[...]], axis=1)
    place = iota((1, 2 * border), 1)
    code_row = iota((2 * GROUP, 2 * border), 0)
    code = jnp.where(
        code_row < GROUP, lax.shift_right_logical(place, 7) + 1, place & (LANES - 1)
    )
    code = jnp.where(lax.shift_right_logical(flat, 7) == (code_row & (GROUP - 1)), code, 0)
    hot = jnp.where(iota((LANES, 2 * border), 0) == (flat & (LANES - 1)), 1.0, 0.0).astype(BF16)
    table = dot_nt(code.astype(F32).astype(BF16), hot).astype(I32)
    place_row = table[:GROUP] - 1
    place_lane = table[GROUP:]
    other = place_row < 0
    count = jnp.where(other, 1.0, 0.0)
    before = jnp.where(iota((LANES, LANES), 0) < iota((LANES, LANES), 1), 1.0, 0.0).astype(BF16)
    double = jnp.concatenate([count, jnp.zeros((GROUP, LANES), F32)], axis=0).astype(BF16)
    rank = jnp.dot(double, before, preferred_element_type=F32)[:GROUP]
    total = jnp.sum(count, axis=1, keepdims=True)
    for row in range(GROUP - 1):
        rank = rank + jnp.where(row_of > row, total[row : row + 1], 0.0)
    rank = rank.astype(I32)
    code_table = jnp.where(
        other,
        2 * edge * WIDE + rank,
        place_row * WIDE + place_lane + jnp.where(place_row < edge, 0, LANES),
    )
    aim = jnp.where(other, rank, -1)
    slot_row = iota((WIDE, LANES), 0)
    hot = [jnp.where(slot_row == aim[row : row + 1], 1.0, 0.0) for row in range(GROUP)]
    hot = jnp.concatenate(hot, axis=1).astype(BF16)
    code_row = iota((2 * GROUP, points), 0)
    place = iota((2 * GROUP, points), 1)
    code = jnp.where(
        code_row < GROUP, lax.shift_right_logical(place, 7) + 1, place & (LANES - 1)
    )
    table = dot_nt(code.astype(F32).astype(BF16), hot).astype(I32)

    def in_place(line):
        return jnp.where(
            row_of == 2 * edge,
            jnp.broadcast_to(line[:, :LANES], (GROUP, LANES)),
            jnp.broadcast_to(line[:, LANES:], (GROUP, LANES)),
        )

    rest_row = jnp.where(row_of < 2 * edge, -1, in_place(table[:1] - 1))
    rest_lane = jnp.where(row_of < 2 * edge, 0, in_place(table[GROUP : GROUP + 1]))
    sums = []
    for own, left, right_half in tiles:
        rest = looked_up(own, GROUP, rest_row, rest_lane, jnp.zeros((GROUP, LANES), F32))
        left = left + jnp.where(row_of == 2 * edge, rest, 0.0)
        moved = pltpu.roll(rest, GROUP - 1, 0)
        right_half = right_half + jnp.where(row_of == 2 * edge, moved, 0.0)
        sums.append(jnp.concatenate([left, right_half], axis=1))

    for top in range(0, cams, GROUP):
        for left in range(0, slots, LANES):
            spot = (slice(top, top + GROUP), slice(left, left + LANES))
            ids = obs_point[spot]
            back_slot = ids - points
            front_slot = back_slot - border
            in_back = ids < points + border
            side = jnp.where(
                in_back,
                lax.shift_right_logical(back_slot, 7) * WIDE + LANES + (back_slot & (LANES - 1)),
                (edge + lax.shift_right_logical(front_slot, 7)) * WIDE + (front_slot & (LANES - 1)),
            )
            id_row = lax.shift_right_logical(ids, 7)
            side = looked_up(code_table, GROUP, id_row, ids & (LANES - 1), side)
            group_of[spot] = jnp.where(used[spot], lax.shift_right_logical(side, 8), -1)
            lane_of[spot] = side & (WIDE - 1)

    for top in range(0, cams, GROUP):
        for left in range(0, slots, LANES):
            spot = (slice(top, top + GROUP), slice(left, left + LANES))
            camera = [wide_jac[(index, *spot)] for index in range(18)]
            for index in range(3):
                one = point_jac[(index, slice(None), spot[1])].astype(F32)[spot[0]]
                two = point_jac[(3 + index, slice(None), spot[1])].astype(F32)[spot[0]]
                for entry in range(9):
                    product = one * camera[entry] + two * camera[9 + entry]
                    for step, term in enumerate(splits_of(product)):
                        terms[(SPLITS * (index * 9 + entry) + step, *spot)] = term
    for cam in range(cams):
        whole = scatter(terms, 27, cam)
        for index in range(27):
            coupling[cam * 27 + index] = joined(whole, index)

    precond = []
    for index, (lead, tail) in enumerate(SQUARES):
        running = None
        for left in range(0, slots, LANES):
            lanes = slice(left, left + LANES)
            term = (
                wide_jac[lead, :, lanes] * wide_jac[tail, :, lanes]
                + wide_jac[9 + lead, :, lanes] * wide_jac[9 + tail, :, lanes]
            )
            running = term if running is None else running + term
        total = jnp.sum(running, axis=1, keepdims=True)
        if lead == tail:
            total = total + damp
            precond.append(spread_out(1.0 / total))
        squares[index] = spread_out(total)
    start_image = square_product(start)

    hear(0)
    sums = receive(sums, 0)
    inverse = symmetric_inverse(sums[:6])
    residual, direction = [], []

    def first_use(entry, back):
        residual.append(right[entry] - (start_image[entry] - back))
        direction.append(precond[entry] * residual[entry])
        return direction[entry]

    sums = there_and_back(apply_inverse(inverse, sums[6:]), first_use)
    send(sums, 1)
    hear(1)
    square_direction = square_product(direction)
    hear(2)
    sums = receive(sums, 1)
    values = apply_inverse(inverse, sums)
    image, ahead = [], []

    def second_use(entry, back):
        image.append(square_direction[entry] - back)
        ahead.append(precond[entry] * image[entry])
        return ahead[entry]

    sums_ahead = there_and_back(values, second_use)
    send(sums_ahead, 2)
    hear(3)
    square_ahead = square_product(ahead)
    inner = dot_of(residual, direction)
    curve = dot_of(direction, image)
    weight = dot_of(image, ahead)
    shift = dot_of(residual, ahead) / jnp.where(weight > 0.0, weight, 1.0)
    shift = jnp.clip(shift, -1e6, 1e6)
    rest = [direction[entry] - shift * ahead[entry] for entry in range(9)]
    left_over = [residual[entry] - shift * image[entry] for entry in range(9)]
    square_rest = [square_direction[entry] - shift * square_ahead[entry] for entry in range(9)]
    members = [
        inner,
        curve,
        dot_of(left_over, rest),
        dot_of(rest, square_rest),
        dot_of(rest, image),
        2.0 * dot_of(left_over, ahead),
        2.0 * dot_of(rest, square_ahead),
        weight,
        weight,
        dot_of(ahead, square_ahead),
    ]
    packed = jnp.zeros((1, LANES), F32)
    for index, member in enumerate(members):
        packed = jnp.where(dot_lane == index, member, packed)
    dots_out[1] = shift
    for turn in range(4, len(reaches)):
        hear(turn)
    sums_ahead = receive(sums_ahead, 2)
    values_ahead = apply_inverse(inverse, sums_ahead)
    wide_shift = jnp.concatenate([shift] * halves, axis=1)
    sums_rest = [sums[index] - wide_shift * sums_ahead[index] for index in range(3)]
    values_rest = [values[index] - wide_shift * values_ahead[index] for index in range(3)]
    packed = packed - jnp.where(dot_lane == 3, point_dot(sums_rest, values_rest), 0.0)
    packed = packed - jnp.where(dot_lane == 6, 2.0 * point_dot(sums_rest, values_ahead), 0.0)
    packed = packed - jnp.where(dot_lane == 9, point_dot(sums_ahead, values_ahead), 0.0)
    dots_out[0] = packed
    lax.fori_loop(1, n, start_dots, 0)

    further = [square_ahead[entry] - camera_entry(values_ahead, entry) for entry in range(9)]

    def lines(vector):
        return jnp.concatenate([line(member) for member in vector], axis=0)

    residual, direction, image, ahead, further = map(
        lines, (residual, direction, image, ahead, further)
    )

    pltpu.make_async_copy(dots_in, dots_in, dots_recv).wait()
    pltpu.make_async_copy(dots_in, dots_in, dots_send).wait()

    def picked(row, lane):
        wide = jnp.broadcast_to(row, (GROUP, LANES))
        spot = jnp.full((GROUP, LANES), lane, I32)
        return jnp.take_along_axis(wide, spot, axis=1, mode="promise_in_bounds")[:1]

    whole = packed + jnp.sum(dots_in[:, 0], axis=0)
    inner = picked(whole, 0)
    curve = picked(whole, 1)
    step = inner / curve

    def moved_by(row, about):
        gap = about - step
        row = jnp.where(dot_lane >= 5, row * gap, row)
        return jnp.where(dot_lane >= 8, row * gap, row)

    whole = moved_by(packed, shift)
    for offset in range(1, n):
        whole = whole + moved_by(dots_in[offset - 1, 0], dots_in[offset - 1, 1])
    inner_next = picked(whole, 2) + picked(whole, 5) + picked(whole, 8)
    own_curve = picked(whole, 3) + picked(whole, 6) + picked(whole, 9)
    cross = picked(whole, 4) + picked(whole, 7)
    ratio = inner_next / inner
    curve = own_curve + ratio * (2.0 * cross + ratio * curve)
    second = inner_next / curve
    step, ratio, second = step[:, :cams], ratio[:, :cams], second[:, :cams]
    fresh = direction - step * ahead + ratio * direction
    seen = image - step * further + ratio * image
    packed_out[:9] = start_guess[...] + step * direction + second * fresh
    packed_out[16:25] = residual - step * image - second * seen


def solution(mesh):
    n = mesh.shape["seg"]

    def shards(
        cam_jac,
        point_jac,
        obs_point,
        obs_count,
        back_list,
        front_list,
        point_damp,
        cam_damp,
        right_side,
        start_guess,
    ):
        cams, slots = obs_point.shape
        kept = 2 * (back_list.shape[1] // LANES)
        link_rows = -(-SIZES[0] * kept // GROUP) * GROUP + sum(SIZES[1:]) * GROUP
        operands = (
            cam_jac,
            point_jac,
            obs_point,
            obs_count.reshape(1, -1),
            back_list,
            front_list,
            point_damp.reshape(1, -1),
            cam_damp.reshape(1, -1),
            right_side,
            start_guess,
        )
        vector = jax.ShapeDtypeStruct(right_side.shape, F32)
        found = pl.pallas_call(
            functools.partial(kernel, n),
            out_shape=pltpu.VMEM((32, right_side.shape[1]), F32),
            in_specs=[pl.BlockSpec(memory_space=pltpu.HBM)] * 10,
            out_specs=pl.BlockSpec(memory_space=pltpu.VMEM),
            scratch_shapes=[
                pltpu.VMEM((cams, slots), I32),
                pltpu.VMEM((cams, slots), I32),
                pltpu.VMEM((18, cams, slots), F32),
                pltpu.VMEM((SPLITS * 9, cams, slots), F32),
                pltpu.VMEM((SPLITS * 27, cams, slots), F32),
                pltpu.VMEM((cams * 27, GROUP, WIDE), F32),
                pltpu.VMEM((9, cams * GROUP, LANES), F32),
                pltpu.VMEM((9, cams, LANES), F32),
                pltpu.VMEM((len(SQUARES), cams, LANES), F32),
                pltpu.VMEM((link_rows, LANES), F32),
                pltpu.VMEM((link_rows, LANES), F32),
                pltpu.VMEM((link_rows, LANES), F32),
                pltpu.VMEM((link_rows, LANES), F32),
                pltpu.VMEM((2, 1, LANES), F32),
                pltpu.VMEM((n - 1, 2, 1, LANES), F32),
                pltpu.SemaphoreType.DMA((3,)),
                pltpu.SemaphoreType.DMA((3,)),
                pltpu.SemaphoreType.DMA((3,)),
                pltpu.SemaphoreType.DMA((3,)),
                pltpu.SemaphoreType.DMA,
                pltpu.SemaphoreType.DMA,
                pltpu.SemaphoreType.REGULAR((max(1, (n - 1).bit_length()),)),
                *[pltpu.VMEM(member.shape, member.dtype) for member in operands],
                pltpu.SemaphoreType.DMA((len(operands),)),
            ],
            compiler_params=pltpu.CompilerParams(
                collective_id=0, has_side_effects=True, vmem_limit_bytes=56 * 1024 * 1024
            ),
            name="schur_cg",
        )(*operands)
        return found[:9], found[16:25]

    return jax.shard_map(
        shards,
        mesh=mesh,
        in_specs=(
            P(None, "seg", None),
            P(None, "seg", None),
            P("seg", None),
            P("seg"),
            P("seg", None),
            P("seg", None),
            P("seg"),
            P("seg"),
            P(None, "seg"),
            P(None, "seg"),
        ),
        out_specs=(P(None, "seg"), P(None, "seg")),
        check_vma=False,
    )
```

```python
import functools

import jax
import jax.numpy as jnp
from jax import lax
from jax.experimental import pallas as pl
from jax.experimental.pallas import tpu as pltpu
from jax.sharding import PartitionSpec as P

ENTRY_PAIRS = ((0, 0), (0, 1), (0, 2), (1, 1), (1, 2), (2, 2))
F32, BF16, I32 = jnp.float32, jnp.bfloat16, jnp.int32
MESH = pl.DeviceIdType.MESH
LANES = 128
WIDE = 256
GROUP = 8
SPLITS = 2
SIZES = (9, 3, 3)
SQUARES = tuple((lead, tail) for lead in range(9) for tail in range(lead, 9))
LOAD_ORDER = (
    "obs_count",
    "obs_point",
    "start_guess",
    "point_jac",
    "cam_jac",
    "back_list",
    "front_list",
    "point_damp",
    "cam_damp",
    "right_side",
)


def splits_of(value):
    terms = []
    for step in range(SPLITS):
        term = value.astype(BF16).astype(F32)
        terms.append(term)
        value = value - term
    return terms


def iota(shape, dim):
    return lax.broadcasted_iota(I32, shape, dim)


def dot_nt(left, right):
    return lax.dot_general(left, right, (((1,), (1,)), ((), ())), preferred_element_type=F32)


def symmetric_inverse(entries):
    cofactors = [
        entries[3] * entries[5] - entries[4] * entries[4],
        entries[2] * entries[4] - entries[1] * entries[5],
        entries[1] * entries[4] - entries[2] * entries[3],
        entries[0] * entries[5] - entries[2] * entries[2],
        entries[1] * entries[2] - entries[0] * entries[4],
        entries[0] * entries[3] - entries[1] * entries[1],
    ]
    determinant = entries[0] * cofactors[0] + entries[1] * cofactors[1] + entries[2] * cofactors[2]
    determinant = jnp.where(determinant > 0.0, determinant, 1.0)
    return [member / determinant for member in cofactors]


def apply_inverse(inverse, sums):
    return [
        inverse[0] * sums[0] + inverse[1] * sums[1] + inverse[2] * sums[2],
        inverse[1] * sums[0] + inverse[3] * sums[1] + inverse[4] * sums[2],
        inverse[2] * sums[0] + inverse[4] * sums[1] + inverse[5] * sums[2],
    ]


def kernel(
    n,
    cam_jac_hbm,
    point_jac_hbm,
    obs_point_hbm,
    obs_count_hbm,
    back_list_hbm,
    front_list_hbm,
    point_damp_hbm,
    cam_damp_hbm,
    right_side_hbm,
    start_guess_hbm,
    packed_out,
    group_of,
    lane_of,
    wide_jac,
    first_terms,
    terms,
    coupling,
    partial,
    vector_rows,
    squares,
    leaving,
    landing,
    dots_out,
    dots_in,
    next_send,
    next_recv,
    prev_send,
    prev_recv,
    dots_send,
    dots_recv,
    told,
    cam_jac,
    point_jac,
    obs_point,
    obs_count,
    back_list,
    front_list,
    point_damp,
    cam_damp,
    right_side,
    start_guess,
    load_sem,
):
    cams, slots = obs_point.shape
    points = point_damp.shape[1]
    border = back_list.shape[1]
    edge = border // LANES
    halves = WIDE // LANES
    me = lax.axis_index("seg")

    loads = {
        "cam_jac": pltpu.make_async_copy(cam_jac_hbm, cam_jac, load_sem.at[0]),
        "point_jac": pltpu.make_async_copy(point_jac_hbm, point_jac, load_sem.at[1]),
        "obs_point": pltpu.make_async_copy(obs_point_hbm, obs_point, load_sem.at[2]),
        "obs_count": pltpu.make_async_copy(obs_count_hbm, obs_count, load_sem.at[3]),
        "back_list": pltpu.make_async_copy(back_list_hbm, back_list, load_sem.at[4]),
        "front_list": pltpu.make_async_copy(front_list_hbm, front_list, load_sem.at[5]),
        "point_damp": pltpu.make_async_copy(point_damp_hbm, point_damp, load_sem.at[6]),
        "cam_damp": pltpu.make_async_copy(cam_damp_hbm, cam_damp, load_sem.at[7]),
        "right_side": pltpu.make_async_copy(right_side_hbm, right_side, load_sem.at[8]),
        "start_guess": pltpu.make_async_copy(start_guess_hbm, start_guess, load_sem.at[9]),
    }
    for name in LOAD_ORDER:
        loads[name].start()

    barrier = pltpu.get_barrier_semaphore()

    kept = 2 * edge
    heights = (kept, GROUP, GROUP)
    lengths = [-(-count * height // GROUP) * GROUP for count, height in zip(SIZES, heights)]
    spots = [sum(lengths[:turn]) for turn in range(3)]

    landing[...] = jnp.zeros_like(landing)
    for side in range(2):
        leaving[side, lengths[0] - GROUP : lengths[0]] = jnp.zeros((GROUP, LANES), F32)

    reaches = []
    while 2 ** len(reaches) < n:
        reaches.insert(0, 2 ** len(reaches))
    has_next = me < n - 1
    has_prev = me > 0
    for reach in reaches:
        pl.semaphore_signal(
            barrier, inc=1, device_id=(lax.rem(me + n - reach, n),), device_id_type=MESH
        )

    @pl.when(has_next)
    def _():
        pl.semaphore_signal(barrier, inc=1, device_id=(me + 1,), device_id_type=MESH)

    def tell(turn):
        pl.semaphore_signal(
            told.at[turn],
            inc=1,
            device_id=(lax.rem(me + reaches[turn], n),),
            device_id_type=MESH,
        )

    def hear(turn):
        pl.semaphore_wait(told.at[turn], 1)
        if turn + 1 < len(reaches):
            tell(turn + 1)


    eye = iota((cams, cams), 0) == iota((cams, cams), 1)

    def column(line):
        wide = jnp.broadcast_to(line, (cams, cams))
        return jnp.sum(jnp.where(eye, wide, jnp.zeros_like(wide)), axis=1, keepdims=True)

    def line(wide):
        return jnp.sum(jnp.where(eye, wide[:, :cams], 0.0), axis=0, keepdims=True)

    loads["obs_count"].wait()
    loads["obs_point"].wait()
    loads["start_guess"].wait()
    start_col = [column(start_guess[entry : entry + 1]) for entry in range(9)]
    used_count = column(obs_count[...].astype(F32)).astype(I32)
    used = iota((cams, slots), 1) < used_count

    ids = obs_point[...]
    group_of[...] = jnp.where(used, lax.shift_right_logical(ids, 7) & (GROUP - 1), -1)
    lane_of[...] = (ids & (LANES - 1)) + jnp.where(ids < points, 0, LANES)

    columns = jnp.transpose(lane_of[...].astype(F32)).astype(I32)
    lane_numbers = [
        (iota((slots, LANES), 1) + part * LANES).astype(jnp.int16) for part in range(halves)
    ]
    tall_unit = jnp.ones((slots, LANES), BF16)
    tall_nil = jnp.zeros((slots, LANES), BF16)
    pair_rows = [
        (iota((2 * GROUP, slots), 0) + first).astype(jnp.int16)
        for first in range(0, WIDE, 2 * GROUP)
    ]
    unit = jnp.ones((2 * GROUP, slots), BF16)
    nil = jnp.zeros((2 * GROUP, slots), BF16)
    group_row = iota((GROUP, slots), 0)

    def scatter(source, count, cam):
        mask = group_row == group_of[cam : cam + 1]
        blocks = [
            jnp.where(mask, jnp.broadcast_to(source[index, cam : cam + 1], (GROUP, slots)), 0.0)
            for index in range(SPLITS * count)
        ]
        lanes = jnp.broadcast_to(lane_of[cam : cam + 1], (2 * GROUP, slots)).astype(jnp.int16)
        hot = jnp.concatenate(
            [jnp.where(row == lanes, unit, nil) for row in pair_rows], axis=0
        )
        return dot_nt(jnp.concatenate(blocks, axis=0).astype(BF16), hot)

    def first_scatter(cam):
        mask = group_row == group_of[cam : cam + 1]
        blocks = [
            jnp.where(
                mask, jnp.broadcast_to(first_terms[index, cam : cam + 1], (GROUP, slots)), 0.0
            )
            for index in range(SPLITS * 9)
        ]
        wide = jnp.broadcast_to(columns[:, cam : cam + 1], (slots, LANES)).astype(jnp.int16)
        hot = [jnp.where(lanes == wide, tall_unit, tall_nil) for lanes in lane_numbers]
        return jnp.dot(
            jnp.concatenate(blocks, axis=0).astype(BF16),
            jnp.concatenate(hot, axis=1),
            preferred_element_type=F32,
        )

    def joined(sums, index):
        whole = sums[(SPLITS * index + SPLITS - 1) * GROUP : (SPLITS * index + SPLITS) * GROUP]
        for step in reversed(range(SPLITS - 1)):
            first = (SPLITS * index + step) * GROUP
            whole = whole + sums[first : first + GROUP]
        return whole

    def neighbour(where, turn):
        spot, size = spots[turn], lengths[turn]
        if where == "next":
            return pltpu.make_async_remote_copy(
                src_ref=leaving.at[0, pl.ds(spot, size)],
                dst_ref=landing.at[1, pl.ds(spot, size)],
                send_sem=next_send.at[turn],
                recv_sem=next_recv.at[turn],
                device_id=(lax.rem(me + 1, n),),
                device_id_type=MESH,
            )
        return pltpu.make_async_remote_copy(
            src_ref=leaving.at[1, pl.ds(spot, size)],
            dst_ref=landing.at[0, pl.ds(spot, size)],
            send_sem=prev_send.at[turn],
            recv_sem=prev_recv.at[turn],
            device_id=(lax.rem(me + n - 1, n),),
            device_id_type=MESH,
        )

    row_of = iota((GROUP, LANES), 0)
    low_row = row_of < edge

    def looked_up(tile, rows, tile_row, tile_lane, start):
        for row in range(rows):
            wide = jnp.broadcast_to(tile[row : row + 1], tile_lane.shape)
            found = jnp.take_along_axis(wide, tile_lane, axis=1, mode="promise_in_bounds")
            start = jnp.where(tile_row == row, found, start)
        return start

    def start_pair(turn):
        @pl.when(has_next)
        def _():
            neighbour("next", turn).start()

        @pl.when(has_prev)
        def _():
            neighbour("prev", turn).start()

    even = (me & 1) == 0
    near = me & 1
    far = 1 - near
    edge_row = row_of < 2 * edge

    def send(sums, turn):
        for index, member in enumerate(sums):
            rows = slice(spots[turn] + index * GROUP, spots[turn] + (index + 1) * GROUP)
            leaving[near, rows] = member[0]
            leaving[far, rows] = member[1]
        start_pair(turn)

    def wait_next(turn, when):
        @pl.when(jnp.logical_and(has_next, when))
        def _():
            neighbour("next", turn).wait_send()
            neighbour("prev", turn).wait_recv()

    def wait_prev(turn, when):
        @pl.when(jnp.logical_and(has_prev, when))
        def _():
            neighbour("prev", turn).wait_send()
            neighbour("next", turn).wait_recv()

    def arrived(sums, turn, side):
        odd = jnp.logical_not(even)
        wait_next(turn, odd if side else even)
        wait_prev(turn, even if side else odd)
        whole = []
        for index, member in enumerate(sums):
            spot = spots[turn] + index * heights[turn]
            came = landing[(near, far)[side], spot : spot + GROUP]
            whole.append(member[side] + jnp.where(edge_row, came, 0.0))
        return whole

    def pjac(index):
        return point_jac[index].astype(F32)

    def spread_out(col):
        return jnp.broadcast_to(col, (cams, LANES))

    def point_terms(running, entry, vector):
        vector_rows[entry] = vector
        for cam in range(cams):
            scale = jnp.broadcast_to(vector_rows[entry, cam : cam + 1], (GROUP, LANES))
            for index in range(3):
                for side, half in enumerate((near, far)):
                    term = coupling[half, cam * 27 + index * 9 + entry] * scale
                    before = running[index][side]
                    running[index][side] = term if before is None else before + term

    def near_products(values):
        for entry in range(9):
            for cam in range(cams):
                whole = coupling[near, cam * 27 + entry] * values[0]
                for index in range(1, 3):
                    whole = whole + coupling[near, cam * 27 + index * 9 + entry] * values[index]
                partial[entry, cam * GROUP : (cam + 1) * GROUP] = whole

    def camera_entry(values, entry):
        for cam in range(cams):
            rows = slice(cam * GROUP, (cam + 1) * GROUP)
            whole = partial[entry, rows]
            for index in range(3):
                whole = whole + coupling[far, cam * 27 + index * 9 + entry] * values[index]
            partial[entry, rows] = whole
        whole = partial[entry, pl.ds(0, cams, stride=GROUP)]
        for row in range(1, GROUP):
            whole = whole + partial[entry, pl.ds(row, cams, stride=GROUP)]
        return spread_out(jnp.sum(whole, axis=1, keepdims=True))

    def there_and_back(values, use):
        running = [[None] * halves for index in range(3)]
        for entry in range(9):
            point_terms(running, entry, use(entry, camera_entry(values, entry)))
        return running

    def square_product(vector):
        result = [None] * 9
        for index, (lead, tail) in enumerate(SQUARES):
            block = squares[index]
            for here, there in {(lead, tail), (tail, lead)}:
                term = block * vector[there]
                result[here] = term if result[here] is None else result[here] + term
        return result

    def dot_of(left, right):
        running = left[0] * right[0]
        for entry in range(1, 9):
            running = running + left[entry] * right[entry]
        return jnp.sum(running, axis=0, keepdims=True)

    dot_lane = iota((1, LANES), 1)
    left_own = jnp.where(low_row | (row_of >= 2 * edge), 1.0, 0.0)
    right_own = jnp.where(low_row, 0.0, 1.0)
    owned = (jnp.where(even, left_own, right_own), jnp.where(even, right_own, left_own))

    def point_part(left, right, side):
        running = left[0] * right[0]
        for index in range(1, 3):
            running = running + left[index] * right[index]
        return running * owned[side]

    def summed(tile):
        running = jnp.sum(tile, axis=0, keepdims=True)
        return jnp.broadcast_to(jnp.sum(running, axis=1, keepdims=True), (1, LANES))

    def dots_copy(offset):
        return pltpu.make_async_remote_copy(
            src_ref=dots_out,
            dst_ref=dots_in.at[offset - 1],
            send_sem=dots_send,
            recv_sem=dots_recv,
            device_id=(lax.rem(me + offset, n),),
            device_id_type=MESH,
        )

    def start_dots(offset, carry):
        dots_copy(offset).start()
        return carry

    for name in LOAD_ORDER[3:]:
        loads[name].wait()
    listed = [back_list, front_list]
    listed = [
        member[:, part * LANES : (part + 1) * LANES] for member in listed for part in range(edge)
    ]
    listed = jnp.concatenate(
        listed + [jnp.full((GROUP - 2 * edge, LANES), -1, I32)], axis=0
    )
    list_row = lax.shift_right_arithmetic(listed, 7)
    list_lane = listed & (LANES - 1)

    chains = [None, None]
    for top in range(0, cams, GROUP):
        eight = slice(top, top + GROUP)

        def upper(ref, index):
            return ref[index].astype(F32)[eight]

        errors = []
        for side in range(2):
            running = upper(cam_jac, 9 * side) * start_col[0][eight]
            for entry in range(1, 9):
                running = running + upper(cam_jac, 9 * side + entry) * start_col[entry][eight]
            errors.append(running)
        ours = [upper(point_jac, index) for index in range(6)]
        blocks = [ours[lead] * ours[tail] + ours[3 + lead] * ours[3 + tail] for lead, tail in ENTRY_PAIRS]
        blocks = blocks + [
            errors[0] * ours[entry] + errors[1] * ours[3 + entry] for entry in range(3)
        ]
        for index, block in enumerate(blocks):
            for step, term in enumerate(splits_of(block)):
                first_terms[SPLITS * index + step, eight] = term
        for cam in range(top, top + GROUP):
            side = 0 if cam % 2 == 0 or cam % 8 == 3 else 1
            if side == 0 and cam not in (0, 2):
                part = first_scatter(cam)
            else:
                part = scatter(first_terms, 9, cam)
            before = chains[side]
            chains[side] = part if before is None else before + part
    for index in range(9):
        half_sum = joined(chains[0], index)
        coupling[0, index], coupling[1, index] = half_sum[:, :LANES], half_sum[:, LANES:]
    whole = chains[1]
    sums = [
        joined(whole, index)
        + jnp.concatenate([coupling[0, index], coupling[1, index]], axis=1)
        for index in range(9)
    ]

    moved = [point_damp[:, part * LANES : (part + 1) * LANES] for part in range(GROUP)]
    moved = jnp.concatenate(moved, axis=0)
    tiles = []
    for index, (member, pair) in enumerate(zip(sums, ENTRY_PAIRS + ((0, 1),) * 3)):
        own, side = member[:, :LANES], member[:, LANES:]
        if pair[0] == pair[1]:
            own = own + moved
        chosen = looked_up(own, GROUP, list_row, list_lane, jnp.zeros((GROUP, LANES), F32))
        tiles.append(
            (own, jnp.where(low_row, chosen, side), jnp.where(low_row, side, chosen))
        )
        rows = slice(index * kept, (index + 1) * kept)
        leaving[0, rows], leaving[1, rows] = tiles[-1][1][:kept], tiles[-1][2][:kept]

    pl.semaphore_wait(barrier, len(reaches) + jnp.where(has_prev, 1, 0))
    tell(0)
    start_pair(0)

    for index in range(18):
        wide_jac[index] = jnp.where(used, cam_jac[index].astype(F32), 0.0)
    damp = column(cam_damp[...])
    right = [spread_out(column(right_side[entry : entry + 1])) for entry in range(9)]
    start = [spread_out(member) for member in start_col]

    flat = jnp.concatenate([back_list[...], front_list[...]], axis=1)
    place = iota((1, 2 * border), 1)
    code_row = iota((2 * GROUP, 2 * border), 0)
    code = jnp.where(
        code_row < GROUP, lax.shift_right_logical(place, 7) + 1, place & (LANES - 1)
    )
    code = jnp.where(lax.shift_right_logical(flat, 7) == (code_row & (GROUP - 1)), code, 0)
    hot = jnp.where(iota((LANES, 2 * border), 0) == (flat & (LANES - 1)), 1.0, 0.0).astype(BF16)
    table = dot_nt(code.astype(F32).astype(BF16), hot).astype(I32)
    place_row = table[:GROUP] - 1
    place_lane = table[GROUP:]
    other = place_row < 0
    count = jnp.where(other, 1.0, 0.0)
    before = jnp.where(iota((LANES, LANES), 0) < iota((LANES, LANES), 1), 1.0, 0.0).astype(BF16)
    double = jnp.concatenate([count, jnp.zeros((GROUP, LANES), F32)], axis=0).astype(BF16)
    rank = jnp.dot(double, before, preferred_element_type=F32)[:GROUP]
    total = jnp.sum(count, axis=1, keepdims=True)
    for row in range(GROUP - 1):
        rank = rank + jnp.where(row_of > row, total[row : row + 1], 0.0)
    rank = rank.astype(I32)
    code_table = jnp.where(
        other,
        2 * edge * WIDE + rank,
        place_row * WIDE + place_lane + jnp.where(place_row < edge, 0, LANES),
    )
    aim = jnp.where(other, rank, -1)
    slot_row = iota((WIDE, LANES), 0)
    hot = [jnp.where(slot_row == aim[row : row + 1], 1.0, 0.0) for row in range(GROUP)]
    hot = jnp.concatenate(hot, axis=1).astype(BF16)
    code_row = iota((2 * GROUP, points), 0)
    place = iota((2 * GROUP, points), 1)
    code = jnp.where(
        code_row < GROUP, lax.shift_right_logical(place, 7) + 1, place & (LANES - 1)
    )
    table = dot_nt(code.astype(F32).astype(BF16), hot).astype(I32)

    def in_place(line):
        return jnp.where(
            row_of == 2 * edge,
            jnp.broadcast_to(line[:, :LANES], (GROUP, LANES)),
            jnp.broadcast_to(line[:, LANES:], (GROUP, LANES)),
        )

    rest_row = jnp.where(row_of < 2 * edge, -1, in_place(table[:1] - 1))
    rest_lane = jnp.where(row_of < 2 * edge, 0, in_place(table[GROUP : GROUP + 1]))
    sums = []
    for own, left, right_half in tiles:
        rest = looked_up(own, GROUP, rest_row, rest_lane, jnp.zeros((GROUP, LANES), F32))
        left = left + jnp.where(row_of == 2 * edge, rest, 0.0)
        moved = pltpu.roll(rest, GROUP - 1, 0)
        right_half = right_half + jnp.where(row_of == 2 * edge, moved, 0.0)
        sums.append((jnp.where(even, left, right_half), jnp.where(even, right_half, left)))

    for top in range(0, cams, GROUP):
        for left in range(0, slots, LANES):
            spot = (slice(top, top + GROUP), slice(left, left + LANES))
            ids = obs_point[spot]
            back_slot = ids - points
            front_slot = back_slot - border
            in_back = ids < points + border
            side = jnp.where(
                in_back,
                lax.shift_right_logical(back_slot, 7) * WIDE + LANES + (back_slot & (LANES - 1)),
                (edge + lax.shift_right_logical(front_slot, 7)) * WIDE + (front_slot & (LANES - 1)),
            )
            id_row = lax.shift_right_logical(ids, 7)
            side = looked_up(code_table, GROUP, id_row, ids & (LANES - 1), side)
            group_of[spot] = jnp.where(used[spot], lax.shift_right_logical(side, 8), -1)
            lane_of[spot] = side & (WIDE - 1)

    for top in range(0, cams, GROUP):
        for left in range(0, slots, LANES):
            spot = (slice(top, top + GROUP), slice(left, left + LANES))
            camera = [wide_jac[(index, *spot)] for index in range(18)]
            for index in range(3):
                one = point_jac[(index, slice(None), spot[1])].astype(F32)[spot[0]]
                two = point_jac[(3 + index, slice(None), spot[1])].astype(F32)[spot[0]]
                for entry in range(9):
                    product = one * camera[entry] + two * camera[9 + entry]
                    for step, term in enumerate(splits_of(product)):
                        terms[(SPLITS * (index * 9 + entry) + step, *spot)] = term
    for cam in range(cams):
        whole = scatter(terms, 27, cam)
        for index in range(27):
            both = joined(whole, index)
            coupling[0, cam * 27 + index] = both[:, :LANES]
            coupling[1, cam * 27 + index] = both[:, LANES:]

    precond = []
    for index, (lead, tail) in enumerate(SQUARES):
        running = None
        for left in range(0, slots, LANES):
            lanes = slice(left, left + LANES)
            term = (
                wide_jac[lead, :, lanes] * wide_jac[tail, :, lanes]
                + wide_jac[9 + lead, :, lanes] * wide_jac[9 + tail, :, lanes]
            )
            running = term if running is None else running + term
        total = jnp.sum(running, axis=1, keepdims=True)
        if lead == tail:
            total = total + damp
            precond.append(spread_out(1.0 / total))
        squares[index] = spread_out(total)
    start_image = square_product(start)

    hear(0)
    inverse = []
    for side in range(2):
        whole = arrived(sums, 0, side)
        inverse.append(symmetric_inverse(whole[:6]))
        values = apply_inverse(inverse[side], whole[6:])
        if side == 0:
            near_products(values)
    residual, direction = [], []

    def first_use(entry, back):
        residual.append(right[entry] - (start_image[entry] - back))
        direction.append(precond[entry] * residual[entry])
        return direction[entry]

    sums = there_and_back(values, first_use)
    send(sums, 1)
    hear(1)
    square_direction = square_product(direction)
    points_now = [arrived(sums, 1, 0)]
    values = [apply_inverse(inverse[0], points_now[0])]
    near_products(values[0])
    hear(2)
    points_now.append(arrived(sums, 1, 1))
    values.append(apply_inverse(inverse[1], points_now[1]))
    image, ahead = [], []

    def second_use(entry, back):
        image.append(square_direction[entry] - back)
        ahead.append(precond[entry] * image[entry])
        return ahead[entry]

    sums_ahead = there_and_back(values[1], second_use)
    send(sums_ahead, 2)
    hear(3)
    square_ahead = square_product(ahead)
    inner = dot_of(residual, direction)
    curve = dot_of(direction, image)
    weight = dot_of(image, ahead)
    shift = dot_of(residual, ahead) / jnp.where(weight > 0.0, weight, 1.0)
    shift = jnp.clip(shift, -1e6, 1e6)
    rest = [direction[entry] - shift * ahead[entry] for entry in range(9)]
    left_over = [residual[entry] - shift * image[entry] for entry in range(9)]
    square_rest = [square_direction[entry] - shift * square_ahead[entry] for entry in range(9)]
    members = [
        inner,
        curve,
        dot_of(left_over, rest),
        dot_of(rest, square_rest),
        dot_of(rest, image),
        2.0 * dot_of(left_over, ahead),
        2.0 * dot_of(rest, square_ahead),
        weight,
        weight,
        dot_of(ahead, square_ahead),
    ]
    packed = jnp.zeros((1, LANES), F32)
    for index, member in enumerate(members):
        packed = jnp.where(dot_lane == index, member, packed)
    dots_out[1] = shift
    for turn in range(4, len(reaches)):
        hear(turn)
    values_ahead, tiles = [], [[], [], []]
    for side in range(2):
        points_ahead = arrived(sums_ahead, 2, side)
        values_ahead.append(apply_inverse(inverse[side], points_ahead))
        points_rest = [points_now[side][index] - shift * points_ahead[index] for index in range(3)]
        values_rest = [values[side][index] - shift * values_ahead[side][index] for index in range(3)]
        tiles[0].append(point_part(points_rest, values_rest, side))
        tiles[1].append(point_part(points_rest, values_ahead[side], side))
        tiles[2].append(point_part(points_ahead, values_ahead[side], side))
    for lane, factor, pair in zip((3, 6, 9), (1.0, 2.0, 1.0), tiles):
        packed = packed - jnp.where(dot_lane == lane, factor * summed(pair[0] + pair[1]), 0.0)
    dots_out[0] = packed
    lax.fori_loop(1, n, start_dots, 0)

    near_products(values_ahead[0])
    further = [square_ahead[entry] - camera_entry(values_ahead[1], entry) for entry in range(9)]

    def lines(vector):
        return jnp.concatenate([line(member) for member in vector], axis=0)

    residual, direction, image, ahead, further = map(
        lines, (residual, direction, image, ahead, further)
    )

    pltpu.make_async_copy(dots_in, dots_in, dots_recv).wait()
    pltpu.make_async_copy(dots_in, dots_in, dots_send).wait()

    def picked(row, lane):
        wide = jnp.broadcast_to(row, (GROUP, LANES))
        spot = jnp.full((GROUP, LANES), lane, I32)
        return jnp.take_along_axis(wide, spot, axis=1, mode="promise_in_bounds")[:1]

    whole = packed + jnp.sum(dots_in[:, 0], axis=0)
    inner = picked(whole, 0)
    curve = picked(whole, 1)
    step = inner / curve

    def moved_by(row, about):
        gap = about - step
        row = jnp.where(dot_lane >= 5, row * gap, row)
        return jnp.where(dot_lane >= 8, row * gap, row)

    whole = moved_by(packed, shift)
    for offset in range(1, n):
        whole = whole + moved_by(dots_in[offset - 1, 0], dots_in[offset - 1, 1])
    inner_next = picked(whole, 2) + picked(whole, 5) + picked(whole, 8)
    own_curve = picked(whole, 3) + picked(whole, 6) + picked(whole, 9)
    cross = picked(whole, 4) + picked(whole, 7)
    ratio = inner_next / inner
    curve = own_curve + ratio * (2.0 * cross + ratio * curve)
    second = inner_next / curve
    step, ratio, second = step[:, :cams], ratio[:, :cams], second[:, :cams]
    fresh = direction - step * ahead + ratio * direction
    seen = image - step * further + ratio * image
    packed_out[:9] = start_guess[...] + step * direction + second * fresh
    packed_out[16:25] = residual - step * image - second * seen


def solution(mesh):
    n = mesh.shape["seg"]

    def shards(
        cam_jac,
        point_jac,
        obs_point,
        obs_count,
        back_list,
        front_list,
        point_damp,
        cam_damp,
        right_side,
        start_guess,
    ):
        cams, slots = obs_point.shape
        kept = 2 * (back_list.shape[1] // LANES)
        link_rows = -(-SIZES[0] * kept // GROUP) * GROUP + sum(SIZES[1:]) * GROUP
        operands = (
            cam_jac,
            point_jac,
            obs_point,
            obs_count.reshape(1, -1),
            back_list,
            front_list,
            point_damp.reshape(1, -1),
            cam_damp.reshape(1, -1),
            right_side,
            start_guess,
        )
        vector = jax.ShapeDtypeStruct(right_side.shape, F32)
        found = pl.pallas_call(
            functools.partial(kernel, n),
            out_shape=pltpu.VMEM((32, right_side.shape[1]), F32),
            in_specs=[pl.BlockSpec(memory_space=pltpu.HBM)] * 10,
            out_specs=pl.BlockSpec(memory_space=pltpu.VMEM),
            scratch_shapes=[
                pltpu.VMEM((cams, slots), I32),
                pltpu.VMEM((cams, slots), I32),
                pltpu.VMEM((18, cams, slots), F32),
                pltpu.VMEM((SPLITS * 9, cams, slots), F32),
                pltpu.VMEM((SPLITS * 27, cams, slots), F32),
                pltpu.VMEM((2, cams * 27, GROUP, LANES), F32),
                pltpu.VMEM((9, cams * GROUP, LANES), F32),
                pltpu.VMEM((9, cams, LANES), F32),
                pltpu.VMEM((len(SQUARES), cams, LANES), F32),
                pltpu.VMEM((2, link_rows, LANES), F32),
                pltpu.VMEM((2, link_rows, LANES), F32),
                pltpu.VMEM((2, 1, LANES), F32),
                pltpu.VMEM((n - 1, 2, 1, LANES), F32),
                pltpu.SemaphoreType.DMA((3,)),
                pltpu.SemaphoreType.DMA((3,)),
                pltpu.SemaphoreType.DMA((3,)),
                pltpu.SemaphoreType.DMA((3,)),
                pltpu.SemaphoreType.DMA,
                pltpu.SemaphoreType.DMA,
                pltpu.SemaphoreType.REGULAR((max(1, (n - 1).bit_length()),)),
                *[pltpu.VMEM(member.shape, member.dtype) for member in operands],
                pltpu.SemaphoreType.DMA((len(operands),)),
            ],
            compiler_params=pltpu.CompilerParams(
                collective_id=0, has_side_effects=True, vmem_limit_bytes=56 * 1024 * 1024
            ),
            name="schur_cg",
        )(*operands)
        return found[:9], found[16:25]

    return jax.shard_map(
        shards,
        mesh=mesh,
        in_specs=(
            P(None, "seg", None),
            P(None, "seg", None),
            P("seg", None),
            P("seg"),
            P("seg", None),
            P("seg", None),
            P("seg"),
            P("seg"),
            P(None, "seg"),
            P(None, "seg"),
        ),
        out_specs=(P(None, "seg"), P(None, "seg")),
        check_vma=False,
    )
```

```python
import functools

import jax
import jax.numpy as jnp
from jax import lax
from jax.experimental import pallas as pl
from jax.experimental.pallas import tpu as pltpu
from jax.sharding import PartitionSpec as P

ENTRY_PAIRS = ((0, 0), (0, 1), (0, 2), (1, 1), (1, 2), (2, 2))
F32, BF16, I32 = jnp.float32, jnp.bfloat16, jnp.int32
MESH = pl.DeviceIdType.MESH
LANES = 128
WIDE = 256
GROUP = 8
SPLITS = 2
SIZES = (9, 3, 3)
SQUARES = tuple((lead, tail) for lead in range(9) for tail in range(lead, 9))
LOAD_ORDER = (
    "obs_count",
    "obs_point",
    "start_guess",
    "point_jac",
    "cam_jac",
    "back_list",
    "front_list",
    "point_damp",
    "cam_damp",
    "right_side",
)


def splits_of(value):
    terms = []
    for step in range(SPLITS):
        term = value.astype(BF16).astype(F32)
        terms.append(term)
        value = value - term
    return terms


def iota(shape, dim):
    return lax.broadcasted_iota(I32, shape, dim)


def dot_nt(left, right):
    return lax.dot_general(left, right, (((1,), (1,)), ((), ())), preferred_element_type=F32)


def symmetric_inverse(entries):
    cofactors = [
        entries[3] * entries[5] - entries[4] * entries[4],
        entries[2] * entries[4] - entries[1] * entries[5],
        entries[1] * entries[4] - entries[2] * entries[3],
        entries[0] * entries[5] - entries[2] * entries[2],
        entries[1] * entries[2] - entries[0] * entries[4],
        entries[0] * entries[3] - entries[1] * entries[1],
    ]
    determinant = entries[0] * cofactors[0] + entries[1] * cofactors[1] + entries[2] * cofactors[2]
    determinant = jnp.where(determinant > 0.0, determinant, 1.0)
    return [member / determinant for member in cofactors]


def apply_inverse(inverse, sums):
    return [
        inverse[0] * sums[0] + inverse[1] * sums[1] + inverse[2] * sums[2],
        inverse[1] * sums[0] + inverse[3] * sums[1] + inverse[4] * sums[2],
        inverse[2] * sums[0] + inverse[4] * sums[1] + inverse[5] * sums[2],
    ]


def kernel(
    n,
    cam_jac_hbm,
    point_jac_hbm,
    obs_point_hbm,
    obs_count_hbm,
    back_list_hbm,
    front_list_hbm,
    point_damp_hbm,
    cam_damp_hbm,
    right_side_hbm,
    start_guess_hbm,
    packed_out,
    group_of,
    lane_of,
    wide_jac,
    first_terms,
    terms,
    coupling,
    partial,
    vector_rows,
    squares,
    leaving,
    landing,
    dots_out,
    dots_in,
    next_send,
    next_recv,
    prev_send,
    prev_recv,
    dots_send,
    dots_recv,
    told,
    cam_jac,
    point_jac,
    obs_point,
    obs_count,
    back_list,
    front_list,
    point_damp,
    cam_damp,
    right_side,
    start_guess,
    load_sem,
):
    cams, slots = obs_point.shape
    points = point_damp.shape[1]
    border = back_list.shape[1]
    edge = border // LANES
    halves = WIDE // LANES
    me = lax.axis_index("seg")

    loads = {
        "cam_jac": pltpu.make_async_copy(cam_jac_hbm, cam_jac, load_sem.at[0]),
        "point_jac": pltpu.make_async_copy(point_jac_hbm, point_jac, load_sem.at[1]),
        "obs_point": pltpu.make_async_copy(obs_point_hbm, obs_point, load_sem.at[2]),
        "obs_count": pltpu.make_async_copy(obs_count_hbm, obs_count, load_sem.at[3]),
        "back_list": pltpu.make_async_copy(back_list_hbm, back_list, load_sem.at[4]),
        "front_list": pltpu.make_async_copy(front_list_hbm, front_list, load_sem.at[5]),
        "point_damp": pltpu.make_async_copy(point_damp_hbm, point_damp, load_sem.at[6]),
        "cam_damp": pltpu.make_async_copy(cam_damp_hbm, cam_damp, load_sem.at[7]),
        "right_side": pltpu.make_async_copy(right_side_hbm, right_side, load_sem.at[8]),
        "start_guess": pltpu.make_async_copy(start_guess_hbm, start_guess, load_sem.at[9]),
    }
    for name in LOAD_ORDER:
        loads[name].start()

    barrier = pltpu.get_barrier_semaphore()

    kept = 2 * edge
    heights = (kept, GROUP, GROUP)
    lengths = [-(-count * height // GROUP) * GROUP for count, height in zip(SIZES, heights)]
    spots = [sum(lengths[:turn]) for turn in range(3)]

    landing[...] = jnp.zeros_like(landing)
    for side in range(2):
        leaving[side, lengths[0] - GROUP : lengths[0]] = jnp.zeros((GROUP, LANES), F32)

    reaches = []
    while 2 ** len(reaches) < n:
        reaches.insert(0, 2 ** len(reaches))
    has_next = me < n - 1
    has_prev = me > 0
    for reach in reaches:
        pl.semaphore_signal(
            barrier, inc=1, device_id=(lax.rem(me + n - reach, n),), device_id_type=MESH
        )

    @pl.when(has_next)
    def _():
        pl.semaphore_signal(barrier, inc=1, device_id=(me + 1,), device_id_type=MESH)

    def tell(turn):
        pl.semaphore_signal(
            told.at[turn],
            inc=1,
            device_id=(lax.rem(me + reaches[turn], n),),
            device_id_type=MESH,
        )

    def hear(turn):
        pl.semaphore_wait(told.at[turn], 1)
        if turn + 1 < len(reaches):
            tell(turn + 1)


    eye = iota((cams, cams), 0) == iota((cams, cams), 1)

    def column(line):
        wide = jnp.broadcast_to(line, (cams, cams))
        return jnp.sum(jnp.where(eye, wide, jnp.zeros_like(wide)), axis=1, keepdims=True)

    def line(wide):
        return jnp.sum(jnp.where(eye, wide[:, :cams], 0.0), axis=0, keepdims=True)

    loads["obs_count"].wait()
    loads["obs_point"].wait()
    loads["start_guess"].wait()
    start_col = [column(start_guess[entry : entry + 1]) for entry in range(9)]
    used_count = column(obs_count[...].astype(F32)).astype(I32)
    used = iota((cams, slots), 1) < used_count

    ids = obs_point[...]
    group_of[...] = jnp.where(used, lax.shift_right_logical(ids, 7) & (GROUP - 1), -1)
    lane_of[...] = (ids & (LANES - 1)) + jnp.where(ids < points, 0, LANES)

    columns = jnp.transpose(lane_of[...].astype(F32)).astype(I32)
    lane_numbers = [
        (iota((slots, LANES), 1) + part * LANES).astype(jnp.int16) for part in range(halves)
    ]
    tall_unit = jnp.ones((slots, LANES), BF16)
    tall_nil = jnp.zeros((slots, LANES), BF16)
    pair_rows = [
        (iota((2 * GROUP, slots), 0) + first).astype(jnp.int16)
        for first in range(0, WIDE, 2 * GROUP)
    ]
    unit = jnp.ones((2 * GROUP, slots), BF16)
    nil = jnp.zeros((2 * GROUP, slots), BF16)
    group_row = iota((GROUP, slots), 0)

    def scatter(source, count, cam):
        mask = group_row == group_of[cam : cam + 1]
        blocks = [
            jnp.where(mask, jnp.broadcast_to(source[index, cam : cam + 1], (GROUP, slots)), 0.0)
            for index in range(SPLITS * count)
        ]
        lanes = jnp.broadcast_to(lane_of[cam : cam + 1], (2 * GROUP, slots)).astype(jnp.int16)
        hot = jnp.concatenate(
            [jnp.where(row == lanes, unit, nil) for row in pair_rows], axis=0
        )
        return dot_nt(jnp.concatenate(blocks, axis=0).astype(BF16), hot)

    def first_scatter(cam):
        mask = group_row == group_of[cam : cam + 1]
        blocks = [
            jnp.where(
                mask, jnp.broadcast_to(first_terms[index, cam : cam + 1], (GROUP, slots)), 0.0
            )
            for index in range(SPLITS * 9)
        ]
        wide = jnp.broadcast_to(columns[:, cam : cam + 1], (slots, LANES)).astype(jnp.int16)
        hot = [jnp.where(lanes == wide, tall_unit, tall_nil) for lanes in lane_numbers]
        return jnp.dot(
            jnp.concatenate(blocks, axis=0).astype(BF16),
            jnp.concatenate(hot, axis=1),
            preferred_element_type=F32,
        )

    def joined(sums, index):
        whole = sums[(SPLITS * index + SPLITS - 1) * GROUP : (SPLITS * index + SPLITS) * GROUP]
        for step in reversed(range(SPLITS - 1)):
            first = (SPLITS * index + step) * GROUP
            whole = whole + sums[first : first + GROUP]
        return whole

    def neighbour(where, turn):
        spot, size = spots[turn], lengths[turn]
        if where == "next":
            return pltpu.make_async_remote_copy(
                src_ref=leaving.at[0, pl.ds(spot, size)],
                dst_ref=landing.at[1, pl.ds(spot, size)],
                send_sem=next_send.at[turn],
                recv_sem=next_recv.at[turn],
                device_id=(lax.rem(me + 1, n),),
                device_id_type=MESH,
            )
        return pltpu.make_async_remote_copy(
            src_ref=leaving.at[1, pl.ds(spot, size)],
            dst_ref=landing.at[0, pl.ds(spot, size)],
            send_sem=prev_send.at[turn],
            recv_sem=prev_recv.at[turn],
            device_id=(lax.rem(me + n - 1, n),),
            device_id_type=MESH,
        )

    row_of = iota((GROUP, LANES), 0)
    low_row = row_of < edge

    def looked_up(tile, rows, tile_row, tile_lane, start):
        for row in range(rows):
            wide = jnp.broadcast_to(tile[row : row + 1], tile_lane.shape)
            found = jnp.take_along_axis(wide, tile_lane, axis=1, mode="promise_in_bounds")
            start = jnp.where(tile_row == row, found, start)
        return start

    def start_pair(turn):
        @pl.when(has_next)
        def _():
            neighbour("next", turn).start()

        @pl.when(has_prev)
        def _():
            neighbour("prev", turn).start()

    even = (me & 1) == 0
    near = me & 1
    far = 1 - near
    edge_row = row_of < 2 * edge

    def start_next(turn, when):
        @pl.when(jnp.logical_and(has_next, when))
        def _():
            neighbour("next", turn).start()

    def start_prev(turn, when):
        @pl.when(jnp.logical_and(has_prev, when))
        def _():
            neighbour("prev", turn).start()

    def store_half(half, tiles, turn):
        for index, tile in enumerate(tiles):
            rows = slice(spots[turn] + index * GROUP, spots[turn] + (index + 1) * GROUP)
            leaving[half, rows] = tile

    def send_far(tiles, turn):
        store_half(far, tiles, turn)
        start_next(turn, jnp.logical_not(even))
        start_prev(turn, even)

    def send_near(tiles, turn):
        store_half(near, tiles, turn)
        start_next(turn, even)
        start_prev(turn, jnp.logical_not(even))

    def wait_next(turn, when):
        @pl.when(jnp.logical_and(has_next, when))
        def _():
            neighbour("next", turn).wait_send()
            neighbour("prev", turn).wait_recv()

    def wait_prev(turn, when):
        @pl.when(jnp.logical_and(has_prev, when))
        def _():
            neighbour("prev", turn).wait_send()
            neighbour("next", turn).wait_recv()

    def arrived(sums, turn, side):
        odd = jnp.logical_not(even)
        wait_next(turn, odd if side else even)
        wait_prev(turn, even if side else odd)
        whole = []
        for index, member in enumerate(sums):
            spot = spots[turn] + index * heights[turn]
            came = landing[(near, far)[side], spot : spot + GROUP]
            whole.append(member[side] + jnp.where(edge_row, came, 0.0))
        return whole

    def pjac(index):
        return point_jac[index].astype(F32)

    def spread_out(col):
        return jnp.broadcast_to(col, (cams, LANES))

    def point_half(half):
        running = [None] * 3
        for entry in range(9):
            for cam in range(cams):
                scale = jnp.broadcast_to(vector_rows[entry, cam : cam + 1], (GROUP, LANES))
                for index in range(3):
                    term = coupling[half, cam * 27 + index * 9 + entry] * scale
                    running[index] = term if running[index] is None else running[index] + term
        return running

    def near_products(values):
        for entry in range(9):
            for cam in range(cams):
                whole = coupling[near, cam * 27 + entry] * values[0]
                for index in range(1, 3):
                    whole = whole + coupling[near, cam * 27 + index * 9 + entry] * values[index]
                partial[entry, cam * GROUP : (cam + 1) * GROUP] = whole

    def camera_entry(values, entry):
        for cam in range(cams):
            rows = slice(cam * GROUP, (cam + 1) * GROUP)
            whole = partial[entry, rows]
            for index in range(3):
                whole = whole + coupling[far, cam * 27 + index * 9 + entry] * values[index]
            partial[entry, rows] = whole
        whole = partial[entry, pl.ds(0, cams, stride=GROUP)]
        for row in range(1, GROUP):
            whole = whole + partial[entry, pl.ds(row, cams, stride=GROUP)]
        return spread_out(jnp.sum(whole, axis=1, keepdims=True))

    def there_and_back(values, use, turn):
        for entry in range(9):
            vector_rows[entry] = use(entry, camera_entry(values, entry))
        beyond = point_half(far)
        send_far(beyond, turn)
        inside = point_half(near)
        send_near(inside, turn)
        return list(zip(inside, beyond))

    def square_product(vector):
        result = [None] * 9
        for index, (lead, tail) in enumerate(SQUARES):
            block = squares[index]
            for here, there in {(lead, tail), (tail, lead)}:
                term = block * vector[there]
                result[here] = term if result[here] is None else result[here] + term
        return result

    def dot_of(left, right):
        running = left[0] * right[0]
        for entry in range(1, 9):
            running = running + left[entry] * right[entry]
        return jnp.sum(running, axis=0, keepdims=True)

    dot_lane = iota((1, LANES), 1)
    left_own = jnp.where(low_row | (row_of >= 2 * edge), 1.0, 0.0)
    right_own = jnp.where(low_row, 0.0, 1.0)
    owned = (jnp.where(even, left_own, right_own), jnp.where(even, right_own, left_own))

    def point_part(left, right, side):
        running = left[0] * right[0]
        for index in range(1, 3):
            running = running + left[index] * right[index]
        return running * owned[side]

    def summed(tile):
        running = jnp.sum(tile, axis=0, keepdims=True)
        return jnp.broadcast_to(jnp.sum(running, axis=1, keepdims=True), (1, LANES))

    def dots_copy(offset):
        return pltpu.make_async_remote_copy(
            src_ref=dots_out,
            dst_ref=dots_in.at[offset - 1],
            send_sem=dots_send,
            recv_sem=dots_recv,
            device_id=(lax.rem(me + offset, n),),
            device_id_type=MESH,
        )

    def start_dots(offset, carry):
        dots_copy(offset).start()
        return carry

    for name in LOAD_ORDER[3:]:
        loads[name].wait()
    listed = [back_list, front_list]
    listed = [
        member[:, part * LANES : (part + 1) * LANES] for member in listed for part in range(edge)
    ]
    listed = jnp.concatenate(
        listed + [jnp.full((GROUP - 2 * edge, LANES), -1, I32)], axis=0
    )
    list_row = lax.shift_right_arithmetic(listed, 7)
    list_lane = listed & (LANES - 1)

    chains = [None, None]
    for top in range(0, cams, GROUP):
        eight = slice(top, top + GROUP)

        def upper(ref, index):
            return ref[index].astype(F32)[eight]

        errors = []
        for side in range(2):
            running = upper(cam_jac, 9 * side) * start_col[0][eight]
            for entry in range(1, 9):
                running = running + upper(cam_jac, 9 * side + entry) * start_col[entry][eight]
            errors.append(running)
        ours = [upper(point_jac, index) for index in range(6)]
        blocks = [ours[lead] * ours[tail] + ours[3 + lead] * ours[3 + tail] for lead, tail in ENTRY_PAIRS]
        blocks = blocks + [
            errors[0] * ours[entry] + errors[1] * ours[3 + entry] for entry in range(3)
        ]
        for index, block in enumerate(blocks):
            for step, term in enumerate(splits_of(block)):
                first_terms[SPLITS * index + step, eight] = term
        for cam in range(top, top + GROUP):
            side = 0 if cam % 2 == 0 or cam % 8 == 3 else 1
            if side == 0 and cam not in (0, 2):
                part = first_scatter(cam)
            else:
                part = scatter(first_terms, 9, cam)
            before = chains[side]
            chains[side] = part if before is None else before + part
    for index in range(9):
        half_sum = joined(chains[0], index)
        coupling[0, index], coupling[1, index] = half_sum[:, :LANES], half_sum[:, LANES:]
    whole = chains[1]
    sums = [
        joined(whole, index)
        + jnp.concatenate([coupling[0, index], coupling[1, index]], axis=1)
        for index in range(9)
    ]

    moved = [point_damp[:, part * LANES : (part + 1) * LANES] for part in range(GROUP)]
    moved = jnp.concatenate(moved, axis=0)
    tiles = []
    for index, (member, pair) in enumerate(zip(sums, ENTRY_PAIRS + ((0, 1),) * 3)):
        own, side = member[:, :LANES], member[:, LANES:]
        if pair[0] == pair[1]:
            own = own + moved
        chosen = looked_up(own, GROUP, list_row, list_lane, jnp.zeros((GROUP, LANES), F32))
        tiles.append(
            (own, jnp.where(low_row, chosen, side), jnp.where(low_row, side, chosen))
        )
        rows = slice(index * kept, (index + 1) * kept)
        leaving[0, rows], leaving[1, rows] = tiles[-1][1][:kept], tiles[-1][2][:kept]

    pl.semaphore_wait(barrier, len(reaches) + jnp.where(has_prev, 1, 0))
    tell(0)
    start_pair(0)

    for index in range(18):
        wide_jac[index] = jnp.where(used, cam_jac[index].astype(F32), 0.0)
    damp = column(cam_damp[...])
    right = [spread_out(column(right_side[entry : entry + 1])) for entry in range(9)]
    start = [spread_out(member) for member in start_col]

    flat = jnp.concatenate([back_list[...], front_list[...]], axis=1)
    place = iota((1, 2 * border), 1)
    code_row = iota((2 * GROUP, 2 * border), 0)
    code = jnp.where(
        code_row < GROUP, lax.shift_right_logical(place, 7) + 1, place & (LANES - 1)
    )
    code = jnp.where(lax.shift_right_logical(flat, 7) == (code_row & (GROUP - 1)), code, 0)
    hot = jnp.where(iota((LANES, 2 * border), 0) == (flat & (LANES - 1)), 1.0, 0.0).astype(BF16)
    table = dot_nt(code.astype(F32).astype(BF16), hot).astype(I32)
    place_row = table[:GROUP] - 1
    place_lane = table[GROUP:]
    other = place_row < 0
    count = jnp.where(other, 1.0, 0.0)
    before = jnp.where(iota((LANES, LANES), 0) < iota((LANES, LANES), 1), 1.0, 0.0).astype(BF16)
    double = jnp.concatenate([count, jnp.zeros((GROUP, LANES), F32)], axis=0).astype(BF16)
    rank = jnp.dot(double, before, preferred_element_type=F32)[:GROUP]
    total = jnp.sum(count, axis=1, keepdims=True)
    for row in range(GROUP - 1):
        rank = rank + jnp.where(row_of > row, total[row : row + 1], 0.0)
    rank = rank.astype(I32)
    code_table = jnp.where(
        other,
        2 * edge * WIDE + rank,
        place_row * WIDE + place_lane + jnp.where(place_row < edge, 0, LANES),
    )
    aim = jnp.where(other, rank, -1)
    slot_row = iota((WIDE, LANES), 0)
    hot = [jnp.where(slot_row == aim[row : row + 1], 1.0, 0.0) for row in range(GROUP)]
    hot = jnp.concatenate(hot, axis=1).astype(BF16)
    code_row = iota((2 * GROUP, points), 0)
    place = iota((2 * GROUP, points), 1)
    code = jnp.where(
        code_row < GROUP, lax.shift_right_logical(place, 7) + 1, place & (LANES - 1)
    )
    table = dot_nt(code.astype(F32).astype(BF16), hot).astype(I32)

    def in_place(line):
        return jnp.where(
            row_of == 2 * edge,
            jnp.broadcast_to(line[:, :LANES], (GROUP, LANES)),
            jnp.broadcast_to(line[:, LANES:], (GROUP, LANES)),
        )

    rest_row = jnp.where(row_of < 2 * edge, -1, in_place(table[:1] - 1))
    rest_lane = jnp.where(row_of < 2 * edge, 0, in_place(table[GROUP : GROUP + 1]))
    sums = []
    for own, left, right_half in tiles:
        rest = looked_up(own, GROUP, rest_row, rest_lane, jnp.zeros((GROUP, LANES), F32))
        left = left + jnp.where(row_of == 2 * edge, rest, 0.0)
        moved = pltpu.roll(rest, GROUP - 1, 0)
        right_half = right_half + jnp.where(row_of == 2 * edge, moved, 0.0)
        sums.append((jnp.where(even, left, right_half), jnp.where(even, right_half, left)))

    for top in range(0, cams, GROUP):
        for left in range(0, slots, LANES):
            spot = (slice(top, top + GROUP), slice(left, left + LANES))
            ids = obs_point[spot]
            back_slot = ids - points
            front_slot = back_slot - border
            in_back = ids < points + border
            side = jnp.where(
                in_back,
                lax.shift_right_logical(back_slot, 7) * WIDE + LANES + (back_slot & (LANES - 1)),
                (edge + lax.shift_right_logical(front_slot, 7)) * WIDE + (front_slot & (LANES - 1)),
            )
            id_row = lax.shift_right_logical(ids, 7)
            side = looked_up(code_table, GROUP, id_row, ids & (LANES - 1), side)
            group_of[spot] = jnp.where(used[spot], lax.shift_right_logical(side, 8), -1)
            lane_of[spot] = side & (WIDE - 1)

    for top in range(0, cams, GROUP):
        for left in range(0, slots, LANES):
            spot = (slice(top, top + GROUP), slice(left, left + LANES))
            camera = [wide_jac[(index, *spot)] for index in range(18)]
            for index in range(3):
                one = point_jac[(index, slice(None), spot[1])].astype(F32)[spot[0]]
                two = point_jac[(3 + index, slice(None), spot[1])].astype(F32)[spot[0]]
                for entry in range(9):
                    product = one * camera[entry] + two * camera[9 + entry]
                    for step, term in enumerate(splits_of(product)):
                        terms[(SPLITS * (index * 9 + entry) + step, *spot)] = term
    for cam in range(cams):
        whole = scatter(terms, 27, cam)
        for index in range(27):
            both = joined(whole, index)
            coupling[0, cam * 27 + index] = both[:, :LANES]
            coupling[1, cam * 27 + index] = both[:, LANES:]

    precond = []
    for index, (lead, tail) in enumerate(SQUARES):
        running = None
        for left in range(0, slots, LANES):
            lanes = slice(left, left + LANES)
            term = (
                wide_jac[lead, :, lanes] * wide_jac[tail, :, lanes]
                + wide_jac[9 + lead, :, lanes] * wide_jac[9 + tail, :, lanes]
            )
            running = term if running is None else running + term
        total = jnp.sum(running, axis=1, keepdims=True)
        if lead == tail:
            total = total + damp
            precond.append(spread_out(1.0 / total))
        squares[index] = spread_out(total)
    start_image = square_product(start)

    hear(0)
    inverse = []
    for side in range(2):
        whole = arrived(sums, 0, side)
        inverse.append(symmetric_inverse(whole[:6]))
        values = apply_inverse(inverse[side], whole[6:])
        if side == 0:
            near_products(values)
    residual, direction = [], []

    def first_use(entry, back):
        residual.append(right[entry] - (start_image[entry] - back))
        direction.append(precond[entry] * residual[entry])
        return direction[entry]

    sums = there_and_back(values, first_use, 1)
    hear(1)
    square_direction = square_product(direction)
    points_now = [arrived(sums, 1, 0)]
    values = [apply_inverse(inverse[0], points_now[0])]
    near_products(values[0])
    hear(2)
    points_now.append(arrived(sums, 1, 1))
    values.append(apply_inverse(inverse[1], points_now[1]))
    image, ahead = [], []

    def second_use(entry, back):
        image.append(square_direction[entry] - back)
        ahead.append(precond[entry] * image[entry])
        return ahead[entry]

    sums_ahead = there_and_back(values[1], second_use, 2)
    hear(3)
    square_ahead = square_product(ahead)
    inner = dot_of(residual, direction)
    curve = dot_of(direction, image)
    weight = dot_of(image, ahead)
    shift = dot_of(residual, ahead) / jnp.where(weight > 0.0, weight, 1.0)
    shift = jnp.clip(shift, -1e6, 1e6)
    rest = [direction[entry] - shift * ahead[entry] for entry in range(9)]
    left_over = [residual[entry] - shift * image[entry] for entry in range(9)]
    square_rest = [square_direction[entry] - shift * square_ahead[entry] for entry in range(9)]
    members = [
        inner,
        curve,
        dot_of(left_over, rest),
        dot_of(rest, square_rest),
        dot_of(rest, image),
        2.0 * dot_of(left_over, ahead),
        2.0 * dot_of(rest, square_ahead),
        weight,
        weight,
        dot_of(ahead, square_ahead),
    ]
    packed = jnp.zeros((1, LANES), F32)
    for index, member in enumerate(members):
        packed = jnp.where(dot_lane == index, member, packed)
    dots_out[1] = shift
    for turn in range(4, len(reaches)):
        hear(turn)
    values_ahead, tiles = [], [[], [], []]
    for side in range(2):
        points_ahead = arrived(sums_ahead, 2, side)
        values_ahead.append(apply_inverse(inverse[side], points_ahead))
        points_rest = [points_now[side][index] - shift * points_ahead[index] for index in range(3)]
        values_rest = [values[side][index] - shift * values_ahead[side][index] for index in range(3)]
        tiles[0].append(point_part(points_rest, values_rest, side))
        tiles[1].append(point_part(points_rest, values_ahead[side], side))
        tiles[2].append(point_part(points_ahead, values_ahead[side], side))
    for lane, factor, pair in zip((3, 6, 9), (1.0, 2.0, 1.0), tiles):
        packed = packed - jnp.where(dot_lane == lane, factor * summed(pair[0] + pair[1]), 0.0)
    dots_out[0] = packed
    lax.fori_loop(1, n, start_dots, 0)

    near_products(values_ahead[0])
    further = [square_ahead[entry] - camera_entry(values_ahead[1], entry) for entry in range(9)]

    def lines(vector):
        return jnp.concatenate([line(member) for member in vector], axis=0)

    residual, direction, image, ahead, further = map(
        lines, (residual, direction, image, ahead, further)
    )

    pltpu.make_async_copy(dots_in, dots_in, dots_recv).wait()
    pltpu.make_async_copy(dots_in, dots_in, dots_send).wait()

    def picked(row, lane):
        wide = jnp.broadcast_to(row, (GROUP, LANES))
        spot = jnp.full((GROUP, LANES), lane, I32)
        return jnp.take_along_axis(wide, spot, axis=1, mode="promise_in_bounds")[:1]

    whole = packed + jnp.sum(dots_in[:, 0], axis=0)
    inner = picked(whole, 0)
    curve = picked(whole, 1)
    step = inner / curve

    def moved_by(row, about):
        gap = about - step
        row = jnp.where(dot_lane >= 5, row * gap, row)
        return jnp.where(dot_lane >= 8, row * gap, row)

    whole = moved_by(packed, shift)
    for offset in range(1, n):
        whole = whole + moved_by(dots_in[offset - 1, 0], dots_in[offset - 1, 1])
    inner_next = picked(whole, 2) + picked(whole, 5) + picked(whole, 8)
    own_curve = picked(whole, 3) + picked(whole, 6) + picked(whole, 9)
    cross = picked(whole, 4) + picked(whole, 7)
    ratio = inner_next / inner
    curve = own_curve + ratio * (2.0 * cross + ratio * curve)
    second = inner_next / curve
    step, ratio, second = step[:, :cams], ratio[:, :cams], second[:, :cams]
    fresh = direction - step * ahead + ratio * direction
    seen = image - step * further + ratio * image
    packed_out[:9] = start_guess[...] + step * direction + second * fresh
    packed_out[16:25] = residual - step * image - second * seen


def solution(mesh):
    n = mesh.shape["seg"]

    def shards(
        cam_jac,
        point_jac,
        obs_point,
        obs_count,
        back_list,
        front_list,
        point_damp,
        cam_damp,
        right_side,
        start_guess,
    ):
        cams, slots = obs_point.shape
        kept = 2 * (back_list.shape[1] // LANES)
        link_rows = -(-SIZES[0] * kept // GROUP) * GROUP + sum(SIZES[1:]) * GROUP
        operands = (
            cam_jac,
            point_jac,
            obs_point,
            obs_count.reshape(1, -1),
            back_list,
            front_list,
            point_damp.reshape(1, -1),
            cam_damp.reshape(1, -1),
            right_side,
            start_guess,
        )
        vector = jax.ShapeDtypeStruct(right_side.shape, F32)
        found = pl.pallas_call(
            functools.partial(kernel, n),
            out_shape=pltpu.VMEM((32, right_side.shape[1]), F32),
            in_specs=[pl.BlockSpec(memory_space=pltpu.HBM)] * 10,
            out_specs=pl.BlockSpec(memory_space=pltpu.VMEM),
            scratch_shapes=[
                pltpu.VMEM((cams, slots), I32),
                pltpu.VMEM((cams, slots), I32),
                pltpu.VMEM((18, cams, slots), F32),
                pltpu.VMEM((SPLITS * 9, cams, slots), F32),
                pltpu.VMEM((SPLITS * 27, cams, slots), F32),
                pltpu.VMEM((2, cams * 27, GROUP, LANES), F32),
                pltpu.VMEM((9, cams * GROUP, LANES), F32),
                pltpu.VMEM((9, cams, LANES), F32),
                pltpu.VMEM((len(SQUARES), cams, LANES), F32),
                pltpu.VMEM((2, link_rows, LANES), F32),
                pltpu.VMEM((2, link_rows, LANES), F32),
                pltpu.VMEM((2, 1, LANES), F32),
                pltpu.VMEM((n - 1, 2, 1, LANES), F32),
                pltpu.SemaphoreType.DMA((3,)),
                pltpu.SemaphoreType.DMA((3,)),
                pltpu.SemaphoreType.DMA((3,)),
                pltpu.SemaphoreType.DMA((3,)),
                pltpu.SemaphoreType.DMA,
                pltpu.SemaphoreType.DMA,
                pltpu.SemaphoreType.REGULAR((max(1, (n - 1).bit_length()),)),
                *[pltpu.VMEM(member.shape, member.dtype) for member in operands],
                pltpu.SemaphoreType.DMA((len(operands),)),
            ],
            compiler_params=pltpu.CompilerParams(
                collective_id=0, has_side_effects=True, vmem_limit_bytes=56 * 1024 * 1024
            ),
            name="schur_cg",
        )(*operands)
        return found[:9], found[16:25]

    return jax.shard_map(
        shards,
        mesh=mesh,
        in_specs=(
            P(None, "seg", None),
            P(None, "seg", None),
            P("seg", None),
            P("seg"),
            P("seg", None),
            P("seg", None),
            P("seg"),
            P("seg"),
            P(None, "seg"),
            P(None, "seg"),
        ),
        out_specs=(P(None, "seg"), P(None, "seg")),
        check_vma=False,
    )
```

```python
import functools

import jax
import jax.numpy as jnp
from jax import lax
from jax.experimental import pallas as pl
from jax.experimental.pallas import tpu as pltpu
from jax.sharding import PartitionSpec as P

ENTRY_PAIRS = ((0, 0), (0, 1), (0, 2), (1, 1), (1, 2), (2, 2))
F32, BF16, I32 = jnp.float32, jnp.bfloat16, jnp.int32
MESH = pl.DeviceIdType.MESH
LANES = 128
WIDE = 256
GROUP = 8
SPLITS = 2
SIZES = (9, 3, 3)
SQUARES = tuple((lead, tail) for lead in range(9) for tail in range(lead, 9))
LOAD_ORDER = (
    "obs_count",
    "obs_point",
    "start_guess",
    "point_jac",
    "cam_jac",
    "back_list",
    "front_list",
    "point_damp",
    "cam_damp",
    "right_side",
)


def splits_of(value):
    terms = []
    for step in range(SPLITS):
        term = value.astype(BF16).astype(F32)
        terms.append(term)
        value = value - term
    return terms


def iota(shape, dim):
    return lax.broadcasted_iota(I32, shape, dim)


def dot_nt(left, right):
    return lax.dot_general(left, right, (((1,), (1,)), ((), ())), preferred_element_type=F32)


def symmetric_inverse(entries):
    cofactors = [
        entries[3] * entries[5] - entries[4] * entries[4],
        entries[2] * entries[4] - entries[1] * entries[5],
        entries[1] * entries[4] - entries[2] * entries[3],
        entries[0] * entries[5] - entries[2] * entries[2],
        entries[1] * entries[2] - entries[0] * entries[4],
        entries[0] * entries[3] - entries[1] * entries[1],
    ]
    determinant = entries[0] * cofactors[0] + entries[1] * cofactors[1] + entries[2] * cofactors[2]
    determinant = jnp.where(determinant > 0.0, determinant, 1.0)
    return [member / determinant for member in cofactors]


def apply_inverse(inverse, sums):
    return [
        inverse[0] * sums[0] + inverse[1] * sums[1] + inverse[2] * sums[2],
        inverse[1] * sums[0] + inverse[3] * sums[1] + inverse[4] * sums[2],
        inverse[2] * sums[0] + inverse[4] * sums[1] + inverse[5] * sums[2],
    ]


def kernel(
    n,
    cam_jac_hbm,
    point_jac_hbm,
    obs_point_hbm,
    obs_count_hbm,
    back_list_hbm,
    front_list_hbm,
    point_damp_hbm,
    cam_damp_hbm,
    right_side_hbm,
    start_guess_hbm,
    packed_out,
    group_of,
    lane_of,
    wide_jac,
    first_terms,
    terms,
    coupling,
    partial,
    vector_rows,
    squares,
    leaving,
    landing,
    dots_out,
    dots_in,
    next_recv,
    prev_recv,
    dots_recv,
    told,
    cam_jac,
    point_jac,
    obs_point,
    obs_count,
    back_list,
    front_list,
    point_damp,
    cam_damp,
    right_side,
    start_guess,
    load_sem,
):
    cams, slots = obs_point.shape
    points = point_damp.shape[1]
    border = back_list.shape[1]
    edge = border // LANES
    halves = WIDE // LANES
    me = lax.axis_index("seg")

    loads = {
        "cam_jac": pltpu.make_async_copy(cam_jac_hbm, cam_jac, load_sem.at[0]),
        "point_jac": pltpu.make_async_copy(point_jac_hbm, point_jac, load_sem.at[1]),
        "obs_point": pltpu.make_async_copy(obs_point_hbm, obs_point, load_sem.at[2]),
        "obs_count": pltpu.make_async_copy(obs_count_hbm, obs_count, load_sem.at[3]),
        "back_list": pltpu.make_async_copy(back_list_hbm, back_list, load_sem.at[4]),
        "front_list": pltpu.make_async_copy(front_list_hbm, front_list, load_sem.at[5]),
        "point_damp": pltpu.make_async_copy(point_damp_hbm, point_damp, load_sem.at[6]),
        "cam_damp": pltpu.make_async_copy(cam_damp_hbm, cam_damp, load_sem.at[7]),
        "right_side": pltpu.make_async_copy(right_side_hbm, right_side, load_sem.at[8]),
        "start_guess": pltpu.make_async_copy(start_guess_hbm, start_guess, load_sem.at[9]),
    }
    for name in LOAD_ORDER:
        loads[name].start()

    barrier = pltpu.get_barrier_semaphore()

    kept = 2 * edge
    heights = (kept, GROUP, GROUP)
    lengths = [-(-count * height // GROUP) * GROUP for count, height in zip(SIZES, heights)]
    spots = [sum(lengths[:turn]) for turn in range(3)]

    landing[...] = jnp.zeros_like(landing)
    for side in range(2):
        leaving[side, lengths[0] - GROUP : lengths[0]] = jnp.zeros((GROUP, LANES), F32)

    reaches = []
    while 2 ** len(reaches) < n:
        reaches.insert(0, 2 ** len(reaches))
    has_next = me < n - 1
    has_prev = me > 0
    for reach in reaches:
        pl.semaphore_signal(
            barrier, inc=1, device_id=(lax.rem(me + n - reach, n),), device_id_type=MESH
        )

    @pl.when(has_next)
    def _():
        pl.semaphore_signal(barrier, inc=1, device_id=(me + 1,), device_id_type=MESH)

    def tell(turn):
        pl.semaphore_signal(
            told.at[turn],
            inc=1,
            device_id=(lax.rem(me + reaches[turn], n),),
            device_id_type=MESH,
        )

    def hear(turn):
        pl.semaphore_wait(told.at[turn], 1)
        if turn + 1 < len(reaches):
            tell(turn + 1)


    eye = iota((cams, cams), 0) == iota((cams, cams), 1)

    def column(line):
        wide = jnp.broadcast_to(line, (cams, cams))
        return jnp.sum(jnp.where(eye, wide, jnp.zeros_like(wide)), axis=1, keepdims=True)

    def line(wide):
        return jnp.sum(jnp.where(eye, wide[:, :cams], 0.0), axis=0, keepdims=True)

    loads["obs_count"].wait()
    loads["obs_point"].wait()
    loads["start_guess"].wait()
    start_col = [column(start_guess[entry : entry + 1]) for entry in range(9)]
    used_count = column(obs_count[...].astype(F32)).astype(I32)
    used = iota((cams, slots), 1) < used_count

    ids = obs_point[...]
    group_of[...] = jnp.where(used, lax.shift_right_logical(ids, 7) & (GROUP - 1), -1)
    lane_of[...] = (ids & (LANES - 1)) + jnp.where(ids < points, 0, LANES)

    columns = jnp.transpose(lane_of[...].astype(F32)).astype(I32)
    lane_numbers = [
        (iota((slots, LANES), 1) + part * LANES).astype(jnp.int16) for part in range(halves)
    ]
    tall_unit = jnp.ones((slots, LANES), BF16)
    tall_nil = jnp.zeros((slots, LANES), BF16)
    pair_rows = [
        (iota((2 * GROUP, slots), 0) + first).astype(jnp.int16)
        for first in range(0, WIDE, 2 * GROUP)
    ]
    unit = jnp.ones((2 * GROUP, slots), BF16)
    nil = jnp.zeros((2 * GROUP, slots), BF16)
    group_row = iota((GROUP, slots), 0)

    def scatter(source, count, cam):
        mask = group_row == group_of[cam : cam + 1]
        blocks = [
            jnp.where(mask, jnp.broadcast_to(source[index, cam : cam + 1], (GROUP, slots)), 0.0)
            for index in range(SPLITS * count)
        ]
        lanes = jnp.broadcast_to(lane_of[cam : cam + 1], (2 * GROUP, slots)).astype(jnp.int16)
        hot = jnp.concatenate(
            [jnp.where(row == lanes, unit, nil) for row in pair_rows], axis=0
        )
        return dot_nt(jnp.concatenate(blocks, axis=0).astype(BF16), hot)

    def first_scatter(cam):
        mask = group_row == group_of[cam : cam + 1]
        blocks = [
            jnp.where(
                mask, jnp.broadcast_to(first_terms[index, cam : cam + 1], (GROUP, slots)), 0.0
            )
            for index in range(SPLITS * 9)
        ]
        wide = jnp.broadcast_to(columns[:, cam : cam + 1], (slots, LANES)).astype(jnp.int16)
        hot = [jnp.where(lanes == wide, tall_unit, tall_nil) for lanes in lane_numbers]
        return jnp.dot(
            jnp.concatenate(blocks, axis=0).astype(BF16),
            jnp.concatenate(hot, axis=1),
            preferred_element_type=F32,
        )

    def joined(sums, index):
        whole = sums[(SPLITS * index + SPLITS - 1) * GROUP : (SPLITS * index + SPLITS) * GROUP]
        for step in reversed(range(SPLITS - 1)):
            first = (SPLITS * index + step) * GROUP
            whole = whole + sums[first : first + GROUP]
        return whole

    def neighbour(where, turn):
        spot, size = spots[turn], lengths[turn]
        if where == "next":
            return pltpu.make_async_remote_copy(
                src_ref=leaving.at[0, pl.ds(spot, size)],
                dst_ref=landing.at[1, pl.ds(spot, size)],
                send_sem=load_sem.at[turn],
                recv_sem=next_recv.at[turn],
                device_id=(lax.rem(me + 1, n),),
                device_id_type=MESH,
            )
        return pltpu.make_async_remote_copy(
            src_ref=leaving.at[1, pl.ds(spot, size)],
            dst_ref=landing.at[0, pl.ds(spot, size)],
            send_sem=load_sem.at[3 + turn],
            recv_sem=prev_recv.at[turn],
            device_id=(lax.rem(me + n - 1, n),),
            device_id_type=MESH,
        )

    row_of = iota((GROUP, LANES), 0)
    low_row = row_of < edge

    def looked_up(tile, rows, tile_row, tile_lane, start):
        for row in range(rows):
            wide = jnp.broadcast_to(tile[row : row + 1], tile_lane.shape)
            found = jnp.take_along_axis(wide, tile_lane, axis=1, mode="promise_in_bounds")
            start = jnp.where(tile_row == row, found, start)
        return start

    even = (me & 1) == 0
    near = me & 1
    far = 1 - near
    edge_row = row_of < 2 * edge

    def start_next(turn, when):
        @pl.when(jnp.logical_and(has_next, when))
        def _():
            neighbour("next", turn).start()

    def start_prev(turn, when):
        @pl.when(jnp.logical_and(has_prev, when))
        def _():
            neighbour("prev", turn).start()

    def start_far(turn):
        start_next(turn, jnp.logical_not(even))
        start_prev(turn, even)

    def start_near(turn):
        start_next(turn, even)
        start_prev(turn, jnp.logical_not(even))

    def store_half(half, tiles, turn):
        for index, tile in enumerate(tiles):
            rows = slice(spots[turn] + index * GROUP, spots[turn] + (index + 1) * GROUP)
            leaving[half, rows] = tile

    def send_far(tiles, turn):
        store_half(far, tiles, turn)
        start_far(turn)

    def send_near(tiles, turn):
        store_half(near, tiles, turn)
        start_near(turn)

    def wait_next(turn, when):
        @pl.when(jnp.logical_and(has_next, when))
        def _():
            neighbour("next", turn).wait_send()
            neighbour("prev", turn).wait_recv()

    def wait_prev(turn, when):
        @pl.when(jnp.logical_and(has_prev, when))
        def _():
            neighbour("prev", turn).wait_send()
            neighbour("next", turn).wait_recv()

    def arrived(sums, turn, side):
        odd = jnp.logical_not(even)
        wait_next(turn, odd if side else even)
        wait_prev(turn, even if side else odd)
        whole = []
        for index, member in enumerate(sums):
            spot = spots[turn] + index * heights[turn]
            came = landing[(near, far)[side], spot : spot + GROUP]
            whole.append(member[side] + jnp.where(edge_row, came, 0.0))
        return whole

    def pjac(index):
        return point_jac[index].astype(F32)

    def spread_out(col):
        return jnp.broadcast_to(col, (cams, LANES))

    def point_half(half):
        running = [None] * 3
        for entry in range(9):
            for cam in range(cams):
                scale = jnp.broadcast_to(vector_rows[entry, cam : cam + 1], (GROUP, LANES))
                for index in range(3):
                    term = coupling[half, cam * 27 + index * 9 + entry] * scale
                    running[index] = term if running[index] is None else running[index] + term
        return running

    def near_products(values):
        for entry in range(9):
            for cam in range(cams):
                whole = coupling[near, cam * 27 + entry] * values[0]
                for index in range(1, 3):
                    whole = whole + coupling[near, cam * 27 + index * 9 + entry] * values[index]
                partial[entry, cam * GROUP : (cam + 1) * GROUP] = whole

    def camera_entry(values, entry):
        for cam in range(cams):
            rows = slice(cam * GROUP, (cam + 1) * GROUP)
            whole = partial[entry, rows]
            for index in range(3):
                whole = whole + coupling[far, cam * 27 + index * 9 + entry] * values[index]
            partial[entry, rows] = whole
        whole = partial[entry, pl.ds(0, cams, stride=GROUP)]
        for row in range(1, GROUP):
            whole = whole + partial[entry, pl.ds(row, cams, stride=GROUP)]
        return spread_out(jnp.sum(whole, axis=1, keepdims=True))

    def there_and_back(values, use, turn):
        for entry in range(9):
            vector_rows[entry] = use(entry, camera_entry(values, entry))
        beyond = point_half(far)
        send_far(beyond, turn)
        inside = point_half(near)
        send_near(inside, turn)
        return list(zip(inside, beyond))

    def square_product(vector):
        result = [None] * 9
        for index, (lead, tail) in enumerate(SQUARES):
            block = squares[index]
            for here, there in {(lead, tail), (tail, lead)}:
                term = block * vector[there]
                result[here] = term if result[here] is None else result[here] + term
        return result

    def dot_of(left, right):
        running = left[0] * right[0]
        for entry in range(1, 9):
            running = running + left[entry] * right[entry]
        return jnp.sum(running, axis=0, keepdims=True)

    dot_lane = iota((1, LANES), 1)
    left_own = jnp.where(low_row | (row_of >= 2 * edge), 1.0, 0.0)
    right_own = jnp.where(low_row, 0.0, 1.0)
    owned = (jnp.where(even, left_own, right_own), jnp.where(even, right_own, left_own))

    def point_part(left, right, side):
        running = left[0] * right[0]
        for index in range(1, 3):
            running = running + left[index] * right[index]
        return running * owned[side]

    def summed(tile):
        running = jnp.sum(tile, axis=0, keepdims=True)
        return jnp.broadcast_to(jnp.sum(running, axis=1, keepdims=True), (1, LANES))

    def dots_copy(offset):
        return pltpu.make_async_remote_copy(
            src_ref=dots_out,
            dst_ref=dots_in.at[offset - 1],
            send_sem=load_sem.at[6],
            recv_sem=dots_recv,
            device_id=(lax.rem(me + offset, n),),
            device_id_type=MESH,
        )

    def start_dots(offset, carry):
        dots_copy(offset).start()
        return carry

    for name in LOAD_ORDER[3:]:
        loads[name].wait()
    listed = [back_list, front_list]
    listed = [
        member[:, part * LANES : (part + 1) * LANES] for member in listed for part in range(edge)
    ]
    listed = jnp.concatenate(
        listed + [jnp.full((GROUP - 2 * edge, LANES), -1, I32)], axis=0
    )
    list_row = lax.shift_right_arithmetic(listed, 7)
    list_lane = listed & (LANES - 1)

    chains = [None, None]
    for top in range(0, cams, GROUP):
        eight = slice(top, top + GROUP)

        def upper(ref, index):
            return ref[index].astype(F32)[eight]

        errors = []
        for side in range(2):
            running = upper(cam_jac, 9 * side) * start_col[0][eight]
            for entry in range(1, 9):
                running = running + upper(cam_jac, 9 * side + entry) * start_col[entry][eight]
            errors.append(running)
        ours = [upper(point_jac, index) for index in range(6)]
        blocks = [ours[lead] * ours[tail] + ours[3 + lead] * ours[3 + tail] for lead, tail in ENTRY_PAIRS]
        blocks = blocks + [
            errors[0] * ours[entry] + errors[1] * ours[3 + entry] for entry in range(3)
        ]
        for index, block in enumerate(blocks):
            for step, term in enumerate(splits_of(block)):
                first_terms[SPLITS * index + step, eight] = term
        for cam in range(top, top + GROUP):
            side = 0 if cam % 2 == 0 or cam % 8 == 3 else 1
            if side == 0 and cam not in (0, 2):
                part = first_scatter(cam)
            else:
                part = scatter(first_terms, 9, cam)
            before = chains[side]
            chains[side] = part if before is None else before + part
    for index in range(9):
        half_sum = joined(chains[0], index)
        coupling[0, index], coupling[1, index] = half_sum[:, :LANES], half_sum[:, LANES:]
    whole = chains[1]
    sums = [
        joined(whole, index)
        + jnp.concatenate([coupling[0, index], coupling[1, index]], axis=1)
        for index in range(9)
    ]

    moved = [point_damp[:, part * LANES : (part + 1) * LANES] for part in range(GROUP)]
    moved = jnp.concatenate(moved, axis=0)
    tiles = []
    for index, (member, pair) in enumerate(zip(sums, ENTRY_PAIRS + ((0, 1),) * 3)):
        own, side = member[:, :LANES], member[:, LANES:]
        if pair[0] == pair[1]:
            own = own + moved
        chosen = looked_up(own, GROUP, list_row, list_lane, jnp.zeros((GROUP, LANES), F32))
        tiles.append(
            (own, jnp.where(low_row, chosen, side), jnp.where(low_row, side, chosen))
        )

    pl.semaphore_wait(barrier, len(reaches) + jnp.where(has_prev, 1, 0))
    tell(0)
    for half, begin in ((far, start_far), (near, start_near)):
        for index, (own, left, right_half) in enumerate(tiles):
            first, other = (right_half, left) if half is far else (left, right_half)
            tile = jnp.where(even, first, other)
            leaving[half, index * kept : (index + 1) * kept] = tile[:kept]
        begin(0)

    for index in range(18):
        wide_jac[index] = jnp.where(used, cam_jac[index].astype(F32), 0.0)
    damp = column(cam_damp[...])
    right = [spread_out(column(right_side[entry : entry + 1])) for entry in range(9)]
    start = [spread_out(member) for member in start_col]

    flat = jnp.concatenate([back_list[...], front_list[...]], axis=1)
    place = iota((1, 2 * border), 1)
    code_row = iota((2 * GROUP, 2 * border), 0)
    code = jnp.where(
        code_row < GROUP, lax.shift_right_logical(place, 7) + 1, place & (LANES - 1)
    )
    code = jnp.where(lax.shift_right_logical(flat, 7) == (code_row & (GROUP - 1)), code, 0)
    hot = jnp.where(iota((LANES, 2 * border), 0) == (flat & (LANES - 1)), 1.0, 0.0).astype(BF16)
    table = dot_nt(code.astype(F32).astype(BF16), hot).astype(I32)
    place_row = table[:GROUP] - 1
    place_lane = table[GROUP:]
    other = place_row < 0
    count = jnp.where(other, 1.0, 0.0)
    before = jnp.where(iota((LANES, LANES), 0) < iota((LANES, LANES), 1), 1.0, 0.0).astype(BF16)
    double = jnp.concatenate([count, jnp.zeros((GROUP, LANES), F32)], axis=0).astype(BF16)
    rank = jnp.dot(double, before, preferred_element_type=F32)[:GROUP]
    total = jnp.sum(count, axis=1, keepdims=True)
    for row in range(GROUP - 1):
        rank = rank + jnp.where(row_of > row, total[row : row + 1], 0.0)
    rank = rank.astype(I32)
    code_table = jnp.where(
        other,
        2 * edge * WIDE + rank,
        place_row * WIDE + place_lane + jnp.where(place_row < edge, 0, LANES),
    )
    aim = jnp.where(other, rank, -1)
    slot_row = iota((WIDE, LANES), 0)
    hot = [jnp.where(slot_row == aim[row : row + 1], 1.0, 0.0) for row in range(GROUP)]
    hot = jnp.concatenate(hot, axis=1).astype(BF16)
    code_row = iota((2 * GROUP, points), 0)
    place = iota((2 * GROUP, points), 1)
    code = jnp.where(
        code_row < GROUP, lax.shift_right_logical(place, 7) + 1, place & (LANES - 1)
    )
    table = dot_nt(code.astype(F32).astype(BF16), hot).astype(I32)

    def in_place(line):
        return jnp.where(
            row_of == 2 * edge,
            jnp.broadcast_to(line[:, :LANES], (GROUP, LANES)),
            jnp.broadcast_to(line[:, LANES:], (GROUP, LANES)),
        )

    rest_row = jnp.where(row_of < 2 * edge, -1, in_place(table[:1] - 1))
    rest_lane = jnp.where(row_of < 2 * edge, 0, in_place(table[GROUP : GROUP + 1]))
    sums = []
    for own, left, right_half in tiles:
        rest = looked_up(own, GROUP, rest_row, rest_lane, jnp.zeros((GROUP, LANES), F32))
        left = left + jnp.where(row_of == 2 * edge, rest, 0.0)
        moved = pltpu.roll(rest, GROUP - 1, 0)
        right_half = right_half + jnp.where(row_of == 2 * edge, moved, 0.0)
        sums.append((jnp.where(even, left, right_half), jnp.where(even, right_half, left)))

    for top in range(0, cams, GROUP):
        for left in range(0, slots, LANES):
            spot = (slice(top, top + GROUP), slice(left, left + LANES))
            ids = obs_point[spot]
            back_slot = ids - points
            front_slot = back_slot - border
            in_back = ids < points + border
            side = jnp.where(
                in_back,
                lax.shift_right_logical(back_slot, 7) * WIDE + LANES + (back_slot & (LANES - 1)),
                (edge + lax.shift_right_logical(front_slot, 7)) * WIDE + (front_slot & (LANES - 1)),
            )
            id_row = lax.shift_right_logical(ids, 7)
            side = looked_up(code_table, GROUP, id_row, ids & (LANES - 1), side)
            group_of[spot] = jnp.where(used[spot], lax.shift_right_logical(side, 8), -1)
            lane_of[spot] = side & (WIDE - 1)

    for top in range(0, cams, GROUP):
        for left in range(0, slots, LANES):
            spot = (slice(top, top + GROUP), slice(left, left + LANES))
            camera = [wide_jac[(index, *spot)] for index in range(18)]
            for index in range(3):
                one = point_jac[(index, slice(None), spot[1])].astype(F32)[spot[0]]
                two = point_jac[(3 + index, slice(None), spot[1])].astype(F32)[spot[0]]
                for entry in range(9):
                    product = one * camera[entry] + two * camera[9 + entry]
                    for step, term in enumerate(splits_of(product)):
                        terms[(SPLITS * (index * 9 + entry) + step, *spot)] = term
    for cam in range(cams):
        whole = scatter(terms, 27, cam)
        for index in range(27):
            both = joined(whole, index)
            coupling[0, cam * 27 + index] = both[:, :LANES]
            coupling[1, cam * 27 + index] = both[:, LANES:]

    precond = []
    for index, (lead, tail) in enumerate(SQUARES):
        running = None
        for left in range(0, slots, LANES):
            lanes = slice(left, left + LANES)
            term = (
                wide_jac[lead, :, lanes] * wide_jac[tail, :, lanes]
                + wide_jac[9 + lead, :, lanes] * wide_jac[9 + tail, :, lanes]
            )
            running = term if running is None else running + term
        total = jnp.sum(running, axis=1, keepdims=True)
        if lead == tail:
            total = total + damp
            precond.append(spread_out(1.0 / total))
        squares[index] = spread_out(total)
    start_image = square_product(start)

    hear(0)
    inverse = []
    for side in range(2):
        whole = arrived(sums, 0, side)
        inverse.append(symmetric_inverse(whole[:6]))
        values = apply_inverse(inverse[side], whole[6:])
        if side == 0:
            near_products(values)
    residual, direction = [], []

    def first_use(entry, back):
        residual.append(right[entry] - (start_image[entry] - back))
        direction.append(precond[entry] * residual[entry])
        return direction[entry]

    sums = there_and_back(values, first_use, 1)
    hear(1)
    square_direction = square_product(direction)
    points_now = [arrived(sums, 1, 0)]
    values = [apply_inverse(inverse[0], points_now[0])]
    near_products(values[0])
    hear(2)
    points_now.append(arrived(sums, 1, 1))
    values.append(apply_inverse(inverse[1], points_now[1]))
    image, ahead = [], []

    def second_use(entry, back):
        image.append(square_direction[entry] - back)
        ahead.append(precond[entry] * image[entry])
        return ahead[entry]

    sums_ahead = there_and_back(values[1], second_use, 2)
    hear(3)
    square_ahead = square_product(ahead)
    inner = dot_of(residual, direction)
    curve = dot_of(direction, image)
    weight = dot_of(image, ahead)
    shift = dot_of(residual, ahead) / jnp.where(weight > 0.0, weight, 1.0)
    shift = jnp.clip(shift, -1e6, 1e6)
    rest = [direction[entry] - shift * ahead[entry] for entry in range(9)]
    left_over = [residual[entry] - shift * image[entry] for entry in range(9)]
    square_rest = [square_direction[entry] - shift * square_ahead[entry] for entry in range(9)]
    members = [
        inner,
        curve,
        dot_of(left_over, rest),
        dot_of(rest, square_rest),
        dot_of(rest, image),
        2.0 * dot_of(left_over, ahead),
        2.0 * dot_of(rest, square_ahead),
        weight,
        weight,
        dot_of(ahead, square_ahead),
    ]
    packed = jnp.zeros((1, LANES), F32)
    for index, member in enumerate(members):
        packed = jnp.where(dot_lane == index, member, packed)
    dots_out[1] = shift
    for turn in range(4, len(reaches)):
        hear(turn)
    values_ahead, tiles = [], [[], [], []]
    for side in range(2):
        points_ahead = arrived(sums_ahead, 2, side)
        values_ahead.append(apply_inverse(inverse[side], points_ahead))
        points_rest = [points_now[side][index] - shift * points_ahead[index] for index in range(3)]
        values_rest = [values[side][index] - shift * values_ahead[side][index] for index in range(3)]
        tiles[0].append(point_part(points_rest, values_rest, side))
        tiles[1].append(point_part(points_rest, values_ahead[side], side))
        tiles[2].append(point_part(points_ahead, values_ahead[side], side))
    for lane, factor, pair in zip((3, 6, 9), (1.0, 2.0, 1.0), tiles):
        packed = packed - jnp.where(dot_lane == lane, factor * summed(pair[0] + pair[1]), 0.0)
    dots_out[0] = packed
    lax.fori_loop(1, n, start_dots, 0)

    near_products(values_ahead[0])
    further = [square_ahead[entry] - camera_entry(values_ahead[1], entry) for entry in range(9)]

    def lines(vector):
        return jnp.concatenate([line(member) for member in vector], axis=0)

    residual, direction, image, ahead, further = map(
        lines, (residual, direction, image, ahead, further)
    )

    pltpu.make_async_copy(dots_in, dots_in, dots_recv).wait()
    pltpu.make_async_copy(dots_in, dots_in, load_sem.at[6]).wait()

    def picked(row, lane):
        wide = jnp.broadcast_to(row, (GROUP, LANES))
        spot = jnp.full((GROUP, LANES), lane, I32)
        return jnp.take_along_axis(wide, spot, axis=1, mode="promise_in_bounds")[:1]

    whole = packed + jnp.sum(dots_in[:, 0], axis=0)
    inner = picked(whole, 0)
    curve = picked(whole, 1)
    step = inner / curve

    def moved_by(row, about):
        gap = about - step
        row = jnp.where(dot_lane >= 5, row * gap, row)
        return jnp.where(dot_lane >= 8, row * gap, row)

    whole = moved_by(packed, shift)
    for offset in range(1, n):
        whole = whole + moved_by(dots_in[offset - 1, 0], dots_in[offset - 1, 1])
    inner_next = picked(whole, 2) + picked(whole, 5) + picked(whole, 8)
    own_curve = picked(whole, 3) + picked(whole, 6) + picked(whole, 9)
    cross = picked(whole, 4) + picked(whole, 7)
    ratio = inner_next / inner
    curve = own_curve + ratio * (2.0 * cross + ratio * curve)
    second = inner_next / curve
    step, ratio, second = step[:, :cams], ratio[:, :cams], second[:, :cams]
    fresh = direction - step * ahead + ratio * direction
    seen = image - step * further + ratio * image
    packed_out[:9] = start_guess[...] + step * direction + second * fresh
    packed_out[16:25] = residual - step * image - second * seen


def solution(mesh):
    n = mesh.shape["seg"]

    def shards(
        cam_jac,
        point_jac,
        obs_point,
        obs_count,
        back_list,
        front_list,
        point_damp,
        cam_damp,
        right_side,
        start_guess,
    ):
        cams, slots = obs_point.shape
        kept = 2 * (back_list.shape[1] // LANES)
        link_rows = -(-SIZES[0] * kept // GROUP) * GROUP + sum(SIZES[1:]) * GROUP
        operands = (
            cam_jac,
            point_jac,
            obs_point,
            obs_count.reshape(1, -1),
            back_list,
            front_list,
            point_damp.reshape(1, -1),
            cam_damp.reshape(1, -1),
            right_side,
            start_guess,
        )
        vector = jax.ShapeDtypeStruct(right_side.shape, F32)
        found = pl.pallas_call(
            functools.partial(kernel, n),
            out_shape=pltpu.VMEM((32, right_side.shape[1]), F32),
            in_specs=[pl.BlockSpec(memory_space=pltpu.HBM)] * 10,
            out_specs=pl.BlockSpec(memory_space=pltpu.VMEM),
            scratch_shapes=[
                pltpu.VMEM((cams, slots), I32),
                pltpu.VMEM((cams, slots), I32),
                pltpu.VMEM((18, cams, slots), F32),
                pltpu.VMEM((SPLITS * 9, cams, slots), F32),
                pltpu.VMEM((SPLITS * 27, cams, slots), F32),
                pltpu.VMEM((2, cams * 27, GROUP, LANES), F32),
                pltpu.VMEM((9, cams * GROUP, LANES), F32),
                pltpu.VMEM((9, cams, LANES), F32),
                pltpu.VMEM((len(SQUARES), cams, LANES), F32),
                pltpu.VMEM((2, link_rows, LANES), F32),
                pltpu.VMEM((2, link_rows, LANES), F32),
                pltpu.VMEM((2, 1, LANES), F32),
                pltpu.VMEM((n - 1, 2, 1, LANES), F32),
                pltpu.SemaphoreType.DMA((3,)),
                pltpu.SemaphoreType.DMA((3,)),
                pltpu.SemaphoreType.DMA,
                pltpu.SemaphoreType.REGULAR((max(1, (n - 1).bit_length()),)),
                *[pltpu.VMEM(member.shape, member.dtype) for member in operands],
                pltpu.SemaphoreType.DMA((len(operands),)),
            ],
            compiler_params=pltpu.CompilerParams(
                collective_id=0, has_side_effects=True, vmem_limit_bytes=56 * 1024 * 1024
            ),
            name="schur_cg",
        )(*operands)
        return found[:9], found[16:25]

    return jax.shard_map(
        shards,
        mesh=mesh,
        in_specs=(
            P(None, "seg", None),
            P(None, "seg", None),
            P("seg", None),
            P("seg"),
            P("seg", None),
            P("seg", None),
            P("seg"),
            P("seg"),
            P(None, "seg"),
            P(None, "seg"),
        ),
        out_specs=(P(None, "seg"), P(None, "seg")),
        check_vma=False,
    )
```
